32 devices in a mesh: tok: 16 (over z, y, x), head: 2 (over core).
Axes of the slice: x: 2, y: 2, z: 4, core: 2. Of those that a mesh axis runs over, the one named last changes fastest.
Arguments:
- text_queries: bfloat16 [256, 8192], P('tok', 'head'), may hold values from -6 to 6
- text_grads: bfloat16 [256, 8192], P('tok', 'head'), may hold values from -6 to 6
- vision_keys: bfloat16 [8192, 1024], P('tok', 'head'), may hold values from -6 to 6
- video_value_rows: bfloat16 [8192, 1024], P('tok', 'head'), may hold values from -6 to 6
- vision: bfloat16 [8192, 4096], P('tok'), may hold values from -6 to 6
- lengths: int32 [8], replicated, may hold values from 16 to 48, as said below
- frame_range: int32 [8, 2], replicated, may hold values from 0 to 64, as said below
Outputs:
- query_grad: bfloat16 [256, 8192], P(None, 'head')
- key_weight_grad: float32 [4096, 1024], P('tok', 'head')
- value_weight_grad: float32 [4096, 1024], P('tok', 'head')
The draws below stay inside these ranges and needn't reach their ends.
Inputs may be any that keep to these rules, and one draw needn't show every extreme that they name: Each segment holds at least one row; the lengths sum to 256. `frame_range`: each segment's range covers 64 // 4 frames or more, first entry below the second.
All inputs are finite; a program needn't handle non-finite values.
Results may differ from the reference program's by a relative error of at most 0.0073.
Values may be sent and summed in bfloat16 or wider, within the bound.
A program may use at most 128 MiB of HBM per device.

```python
import jax
import jax.numpy as jnp
from jax import lax

QUERY_HEADS = 64
KEY_VALUE_HEADS = 8
HEAD_WIDTH = 128
DW = 4096
TQ = 256
TEXT_SEGMENTS = 8
FRAME_TOK = 128
FRAMES = 64
VIDEO_TOKENS = 8192


def layout(key):
    base_key = jax.random.fold_in(key, 7001)
    base_rows = TQ // TEXT_SEGMENTS
    spread = base_rows // 4
    shifts = jax.random.randint(jax.random.fold_in(base_key, 1), (TEXT_SEGMENTS,), -spread, spread + 1)
    segment_ids = jnp.arange(TEXT_SEGMENTS, dtype=jnp.int32)
    shifts = jnp.where(segment_ids <= 1, spread, shifts)
    shifts = jnp.where(segment_ids == 2, -spread, shifts)
    shifts = jnp.where(segment_ids == TEXT_SEGMENTS - 1, -spread, shifts)
    seg_rows = base_rows + shifts - jnp.roll(shifts, 1)
    fewest = FRAMES // 4
    first_frame = jax.random.randint(jax.random.fold_in(base_key, 2), (TEXT_SEGMENTS,), 0, FRAMES - fewest + 1)
    first_frame = jnp.where(segment_ids == 0, 0, first_frame)
    extension = jax.random.randint(jax.random.fold_in(base_key, 3), (TEXT_SEGMENTS,), 0, FRAMES - fewest - first_frame + 1)
    extension = jnp.where(segment_ids == 1, FRAMES - fewest - first_frame, extension)
    end_frame = first_frame + fewest + extension
    ranges = jnp.stack([first_frame, end_frame], axis=1)
    return (seg_rows.astype(jnp.int32), ranges.astype(jnp.int32))


def paired(key):
    paired_key = jax.random.fold_in(key, 7002)
    query_rows = jnp.clip(1.5 * jax.random.normal(jax.random.fold_in(paired_key, 5), (TQ, QUERY_HEADS * HEAD_WIDTH), jnp.float32), -5.5, 5.5)
    key_row_block = jnp.clip(1.5 * jax.random.normal(jax.random.fold_in(paired_key, 6), (VIDEO_TOKENS, KEY_VALUE_HEADS * HEAD_WIDTH), jnp.float32), -5.5, 5.5)
    return (query_rows, key_row_block)


def draw_lengths(key, part):
    return layout(key)[0]


def draw_frame_range(key, part):
    return layout(key)[1]


def draw_text_queries(key, part):
    return paired(key)[0].astype(jnp.bfloat16)


def draw_vision_keys(key, part):
    return paired(key)[1].astype(jnp.bfloat16)


def spiked(drawn, rng, source, target, parts, factor):
    owner, partner = [(jnp.arange(drawn.shape[dim]) // (drawn.shape[dim] // parts)).reshape([-1 if axis == dim else 1 for axis in range(drawn.ndim)]) for dim in (source, target)]
    chosen = jax.random.permutation(rng, parts)[partner]
    strong = (owner == chosen) | (owner == (partner + parts // 2) % parts)
    return jnp.where(strong, factor * drawn, drawn)


def steps_of(stream_key, dims, pieces, least, high):
    def one(dim, parts):
        heights = jax.random.uniform(jax.random.fold_in(jax.random.fold_in(stream_key, 6), dim), (parts,), jnp.float32, least / len(pieces), high / len(pieces))
        return jnp.repeat(jnp.exp(heights), dims[dim] // parts).reshape((-1,) + (1,) * (len(dims) - dim - 1))

    factor_of = one(*pieces[0])
    for cut in pieces[1:]:
        factor_of = factor_of * one(*cut)
    return factor_of


def noise(key, shape, scale, limit, shards=(), kind=jnp.bfloat16):
    factor_of = steps_of(key, shape, shards, -0.22, 0.18) if shards else 1.0
    drawn = jax.random.normal(key, shape, jnp.float32) * scale * factor_of
    return jnp.minimum(jnp.maximum(drawn, -limit), limit).astype(kind)


def noise_with(key, extent, scale, bound, shards, heavy, held_as=jnp.bfloat16):
    drawn = scale * jax.random.normal(key, extent, jnp.float32)
    if shards:
        drawn = drawn * steps_of(key, extent, shards, -0.22, 0.18)
    return jnp.clip(spiked(drawn, jax.random.fold_in(key, 3), *heavy), -bound, bound).astype(held_as)


def setup_inputs(seed: int = 0) -> dict:
    splits = jax.random.split(jax.random.key(seed), 8)
    return {
        "text_queries": draw_text_queries(jax.random.fold_in(splits[7], 71), 0),
        "text_grads": noise(splits[1], (TQ, QUERY_HEADS * HEAD_WIDTH), 1.0, 6.0, ((0, 16), (1, 2))),
        "vision_keys": draw_vision_keys(jax.random.fold_in(splits[7], 71), 0),
        "video_value_rows": noise(splits[3], (VIDEO_TOKENS, KEY_VALUE_HEADS * HEAD_WIDTH), 1.0, 6.0, ((0, 16), (1, 2))),
        "vision": noise_with(splits[4], (VIDEO_TOKENS, DW), 1.0, 6.0, ((0, 16),), (0, 1, 16, 2.0)),
        "lengths": draw_lengths(jax.random.fold_in(splits[7], 71), 0),
        "frame_range": draw_frame_range(jax.random.fold_in(splits[7], 71), 0),
    }


NEG_FILL = -1e30


def row_bounds(lengths, frame_range):
    row_ids = jnp.arange(TQ, dtype=jnp.int32)
    segment_ends = jnp.cumsum(lengths).astype(jnp.int32)
    segment = jnp.sum((row_ids[:, None] >= segment_ends[None, :]).astype(jnp.int32), axis=1)
    segment_pick = (segment[:, None] == jnp.arange(TEXT_SEGMENTS, dtype=jnp.int32)[None, :]).astype(jnp.int32)
    first_frame = jnp.sum(segment_pick * frame_range[None, :, 0], axis=1)
    end_frame = jnp.sum(segment_pick * frame_range[None, :, 1], axis=1)
    return first_frame, end_frame


def reference(text_queries, text_grads, vision_keys, video_value_rows, vision, lengths, frame_range):
    group_width = QUERY_HEADS // KEY_VALUE_HEADS
    score_scale = HEAD_WIDTH ** -0.5
    first_frame, end_frame = row_bounds(lengths, frame_range)
    frames = jnp.arange(VIDEO_TOKENS, dtype=jnp.int32) // FRAME_TOK
    allowed = (frames[None, :] >= first_frame[:, None]) & (frames[None, :] < end_frame[:, None])

    def head_gradient_list(kv_head):
        k_head = lax.dynamic_slice_in_dim(vision_keys, kv_head * HEAD_WIDTH, HEAD_WIDTH, 1)
        v_head = lax.dynamic_slice_in_dim(video_value_rows, kv_head * HEAD_WIDTH, HEAD_WIDTH, 1)

        def query_head(running, member):
            q_index = kv_head * group_width + member
            q_one = lax.dynamic_slice_in_dim(text_queries, q_index * HEAD_WIDTH, HEAD_WIDTH, 1)
            g_one = lax.dynamic_slice_in_dim(text_grads, q_index * HEAD_WIDTH, HEAD_WIDTH, 1)
            scores = jnp.dot(q_one, k_head.T, preferred_element_type=jnp.float32) * score_scale
            row_top = jnp.max(jnp.where(allowed, scores, NEG_FILL), axis=1, keepdims=True)
            exp_terms = jnp.where(allowed, jnp.exp(scores - row_top), 0.0)
            row_total = jnp.sum(exp_terms, axis=1, keepdims=True)
            attn_probs = exp_terms / row_total
            dprobs = jnp.dot(g_one, v_head.T, preferred_element_type=jnp.float32)
            row_delta = jnp.sum(attn_probs * dprobs, axis=1, keepdims=True)
            dscore = (attn_probs * (dprobs - row_delta)).astype(jnp.bfloat16)
            key_sum = running[0] + jnp.dot(dscore.T, q_one, preferred_element_type=jnp.float32)
            value_sum = running[1] + jnp.dot(attn_probs.astype(jnp.bfloat16).T, g_one, preferred_element_type=jnp.float32)
            dq_part = score_scale * jnp.dot(dscore, k_head, preferred_element_type=jnp.float32)
            return (key_sum, value_sum), dq_part

        zero_acc = jnp.zeros((VIDEO_TOKENS, HEAD_WIDTH), jnp.float32)
        sums, dq_parts = lax.scan(query_head, (zero_acc, zero_acc), jnp.arange(group_width, dtype=jnp.int32))
        return dq_parts, (score_scale * sums[0]).astype(jnp.bfloat16), sums[1].astype(jnp.bfloat16)

    query_gradient_total, key_gradient_total, value_gradient_total = lax.map(head_gradient_list, jnp.arange(KEY_VALUE_HEADS, dtype=jnp.int32))
    query_grad = query_gradient_total.transpose(2, 0, 1, 3).reshape(TQ, QUERY_HEADS * HEAD_WIDTH).astype(jnp.bfloat16)
    key_gradient_flat = key_gradient_total.transpose(1, 0, 2).reshape(VIDEO_TOKENS, KEY_VALUE_HEADS * HEAD_WIDTH)
    value_gradient_flat = value_gradient_total.transpose(1, 0, 2).reshape(VIDEO_TOKENS, KEY_VALUE_HEADS * HEAD_WIDTH)
    key_weight_grad = jnp.dot(vision.T, key_gradient_flat, preferred_element_type=jnp.float32)
    value_weight_grad = jnp.dot(vision.T, value_gradient_flat, preferred_element_type=jnp.float32)
    return query_grad, key_weight_grad, value_weight_grad
```

```python
import functools

import jax
import jax.numpy as jnp
from jax import lax
from jax.experimental import pallas as pl
from jax.experimental.pallas import tpu as pltpu
from jax.sharding import PartitionSpec as P

HEAD_WIDTH = 128
FRAME_DEV = 4
NEG_FILL = -1e30
NT = (((1,), (1,)), ((), ()))
TN = (((0,), (0,)), ((), ()))
F32 = jnp.float32
BF16 = jnp.bfloat16


def dot(a, b, dims=(((1,), (0,)), ((), ()))):
    return lax.dot_general(a, b, dims, preferred_element_type=F32)


def kernel(cfg, q_in, g_in, k_in, v_in, x_in, bounds, q_out, kw_out, vw_out,
           qb, gb, kb, vb, vis, ebuf, dpb, stat, stin, coef, kv, dqt, dqs, dqin, dqall, part, rsb,
           loc, qs, qr, gs, gr, ks, kr, vs, vr, xs, xr, ss, sr, kvs, kvr, ds, dr, as_, ar, ys, yr, rs, rr, fs, fr):
    T, G, NZ = cfg["T"], cfg["G"], cfg["NZ"]
    blk, rows, NK, NR, FR = cfg["blk"], cfg["rows"], cfg["NK"], cfg["NR"], cfg["FR"]
    W, NV, FB = cfg["W"], cfg["NV"], cfg["FB"]
    H = cfg["H"]
    RB = cfg["RB"]
    scale = HEAD_WIDTH ** (-0.5)
    me = lax.axis_index("tok")
    z, j0 = me // G, me % G

    def remote(src, dst, s, r, peer):
        return pltpu.make_async_remote_copy(
            src_ref=src, dst_ref=dst, send_sem=s, recv_sem=r,
            device_id={"tok": peer}, device_id_type=pl.DeviceIdType.MESH)

    def m128(i, n):
        return pl.ds(pl.multiple_of(i * n, n), n)

    barrier = pltpu.get_barrier_semaphore()
    for d in range(1, T):
        pl.semaphore_signal(barrier, inc=1, device_id={"tok": lax.rem(me + d, T)}, device_id_type=pl.DeviceIdType.MESH)
    twin = lax.axis_index("head")
    if H > 1:
        twin = 1 - twin
        pl.semaphore_signal(barrier, inc=1, device_id={"head": twin}, device_id_type=pl.DeviceIdType.MESH)
    pl.semaphore_wait(barrier, T - 1 + (H > 1))

    def tpeer(d):
        return lax.rem(me + d, T), lax.rem(me + T - d, T)

    def gpeer(d):
        a, b = (j0 ^ d, j0 ^ d) if G & (G - 1) == 0 else (lax.rem(j0 + d, G), lax.rem(j0 + G - d, G))
        return a, b, z * G + a, z * G + b

    def zpeer(d):
        a, b = lax.rem(z + d, NZ), lax.rem(z + NZ - d, NZ)
        return a, b, a * G + j0, b * G + j0

    sends = []

    def send(c):
        c.start()
        sends.append(c)

    def q_copy(t_to, t_from):
        return (remote(q_in.at[lax.rem(t_to, G)], qb.at[m128(t_from, blk)], qs.at[t_to], qr.at[t_from], t_to),
                remote(g_in.at[lax.rem(t_to, G)], gb.at[m128(t_from, blk)], gs.at[t_to], gr.at[t_from], t_to))

    def k_copy(j_to, j_from, peer):
        return (remote(k_in.at[:, m128(j_to, 128)], kb.at[m128(j_from, rows)], ks.at[j_to], kr.at[j_from], peer),
                remote(v_in.at[:, m128(j_to, 128)], vb.at[m128(j_from, rows)], vs.at[j_to], vr.at[j_from], peer))

    WH = W // H
    half = lax.axis_index("head") * WH if H > 1 else 0

    def x_copy(b, j_to, j_from, peer):
        cols = pl.ds(pl.multiple_of((b * G + j_to) * W + half, WH), WH)
        dst = vis.at[b, m128(j_from, rows), pl.ds(pl.multiple_of(half, WH), WH)]
        return remote(x_in.at[:, cols], dst, xs.at[j_to, b], xr.at[j_from, b], peer)

    def f_copy(b, j_from, mine):
        at = half if mine else WH - half
        here = vis.at[b, m128(j_from, rows), pl.ds(pl.multiple_of(at, WH), WH)]
        return pltpu.make_async_remote_copy(
            src_ref=here, dst_ref=here, send_sem=fs.at[j_from, b], recv_sem=fr.at[j_from, b],
            device_id={"head": twin}, device_id_type=pl.DeviceIdType.MESH)

    local = [
        pltpu.make_async_copy(q_in.at[j0], qb.at[m128(me, blk)], loc.at[0]),
        pltpu.make_async_copy(g_in.at[j0], gb.at[m128(me, blk)], loc.at[1]),
        pltpu.make_async_copy(k_in.at[:, m128(j0, 128)], kb.at[m128(j0, rows)], loc.at[2]),
        pltpu.make_async_copy(v_in.at[:, m128(j0, 128)], vb.at[m128(j0, rows)], loc.at[3]),
    ]
    local_x = [pltpu.make_async_copy(x_in.at[:, m128(b * G + j0, W)], vis.at[b, m128(j0, rows)], loc.at[4 + b]) for b in range(NV)]
    for c in local:
        c.start()
    def q_sends(zd):
        a, _, _, _ = zpeer(zd)
        for i in range(G):
            to = a * G + (lax.rem(j0 + i, G) if zd else gpeer(i)[0])
            if zd or i:
                for c in q_copy(to, me):
                    send(c)

    q_sends(0)
    for d in range(1, G):
        a, _, peer, _ = gpeer(d)
        for c in k_copy(a, j0, peer):
            send(c)
    for d in range(1, NZ):
        q_sends(d)
    for c in local_x:
        c.start()
    for c in local:
        c.wait()
    for d in range(1, G):
        _, b, _, _ = gpeer(d)
        for c in k_copy(j0, b, me):
            c.wait_recv()

    def q_wait(zd):
        _, b, _, _ = zpeer(zd)
        for i in range(G):
            if zd or i:
                frm = b * G + (i if zd else gpeer(i)[1])
                for c in q_copy(me, frm):
                    c.wait_recv()

    n_frames = NK // FR
    frame0 = z * n_frames
    stat[0:1, :] = jnp.full((1, NR), NEG_FILL, F32)
    stat[1:8, :] = jnp.zeros((7, NR), F32)

    def totals(cols, width):
        first, end = bounds[0:1, cols], bounds[1:2, cols]
        UN = 2 if n_frames % 2 == 0 else 1

        def scored(i, top):
            for u in range(UN):
                f = i * UN + u
                ok = (first <= frame0 + f) & (frame0 + f < end)
                s = jnp.where(ok, dot(kb[m128(f, FR), :], qb[cols, :], NT) * scale, NEG_FILL)
                ebuf[m128(f, FR), cols] = s
                top = jnp.maximum(top, jnp.max(s, axis=0, keepdims=True))
            return top

        top = lax.fori_loop(0, n_frames // UN, scored, jnp.full((1, width), NEG_FILL, F32))

        def summed(i, carry):
            total, dotted = carry
            for u in range(UN):
                f = i * UN + u
                dp = dot(vb[m128(f, FR), :], gb[cols, :], NT)
                e = jnp.exp(ebuf[m128(f, FR), cols] - top)
                ebuf[m128(f, FR), cols] = e
                dpb[m128(f, FR), cols] = dp
                total += jnp.sum(e, axis=0, keepdims=True)
                dotted += jnp.sum(e * dp, axis=0, keepdims=True)
            return total, dotted

        zero = jnp.zeros((1, width), F32)
        total, dotted = lax.fori_loop(0, n_frames // UN, summed, (zero, zero))
        stat[0:1, cols] = top
        stat[1:2, cols] = total
        stat[2:3, cols] = dotted

    def x_sends():
        for d in range(1, G):
            a, _, peer, _ = gpeer(d)
            for b in range(NV):
                send(x_copy(b, a, j0, peer))

    by_z = (NR // NZ) % 128 == 0
    for d in range(NZ):
        q_wait(d)
        if d == NZ - 1:
            x_sends()
        if by_z:
            totals(m128(zpeer(d)[1], NR // NZ), NR // NZ)
    if not by_z:
        for r in range(0, NR, RB):
            totals(pl.ds(r, RB), RB)

    def s_copy(z_to, z_from, peer):
        return remote(stat, stin.at[z_from], ss.at[z_to], sr.at[z_from], peer)

    for d in range(1, NZ):
        a, _, peer, _ = zpeer(d)
        send(s_copy(a, z, peer))
    stin[z] = stat[...]
    for d in range(1, NZ):
        _, b, _, _ = zpeer(d)
        s_copy(z, b, me).wait_recv()
    top = stat[0:1, :]
    for i in range(NZ):
        top = jnp.maximum(top, stin[i, 0:1, :])
    total = jnp.zeros((1, NR), F32)
    dotted = jnp.zeros((1, NR), F32)
    for i in range(NZ):
        w = jnp.exp(stin[i, 0:1, :] - top)
        total += w * stin[i, 1:2, :]
        dotted += w * stin[i, 2:3, :]
    coef[0:1, :] = jnp.exp(stat[0:1, :] - top) / total
    coef[1:2, :] = dotted / total
    dqt[...] = jnp.zeros_like(dqt)

    NC = cfg["NC"]
    CH = NK // NC

    def kv_copy(c, j_to, j_from, peer):
        here = kv.at[j_from, pl.ds(c * CH, CH)]
        return remote(here, here, kvs.at[j_to, c], kvr.at[j_from, c], peer)

    for c in range(NC):
        @pl.loop(c * (CH // FR), (c + 1) * (CH // FR))
        def _(f):
            kt = kb[m128(f, FR), :].astype(F32).T.astype(BF16)
            dk = jnp.zeros((FR, HEAD_WIDTH), F32)
            dv = jnp.zeros((FR, HEAD_WIDTH), F32)
            for r in range(0, NR, RB):
                cols = pl.ds(r, RB)
                p = ebuf[m128(f, FR), cols] * coef[0:1, cols]
                t = (p * (dpb[m128(f, FR), cols] - coef[1:2, cols])).astype(BF16)
                dv += dot(p.astype(BF16), gb[cols, :])
                dk += dot(t, qb[cols, :])
                dqt[:, cols] += dot(kt, t)
            kv[j0, m128(f, FR), 0:HEAD_WIDTH] = (scale * dk).astype(BF16)
            kv[j0, m128(f, FR), HEAD_WIDTH:2 * HEAD_WIDTH] = dv.astype(BF16)

        for d in range(1, G - 1):
            a, _, peer, _ = gpeer(d)
            kv_copy(c, a, j0, peer).start()
        if H > 1 and c == NC // 2:
            for d in range(1, G):
                _, b, _, _ = gpeer(d)
                for i in range(NV):
                    x_copy(i, j0, b, me).wait_recv()
                    send(f_copy(i, b, True))

    for r in range(0, NR, 128):
        dqs[pl.ds(r, 128), :] = (scale * dqt[:, pl.ds(r, 128)].T).astype(BF16)
    QR = NR // NZ

    def d_copy(z_to, z_from, peer):
        return remote(dqs.at[m128(z_to, QR)], dqin.at[z_from], ds.at[z_to], dr.at[z_from], peer)

    def a_copy(z_to, z_from, peer):
        here = dqall.at[j0, m128(z_from, QR)]
        return remote(here, here, as_.at[z_to], ar.at[z_from], peer)

    def y_copy(j_to, j_from, peer):
        here = dqall.at[j_from]
        return remote(here, here, ys.at[j_to], yr.at[j_from], peer)

    def r_copy(j, z_to, z_from, peer):
        return remote(part.at[j, m128(z_to, FB)], rsb.at[z_from, j], rs.at[j, z_to], rr.at[j, z_from], peer)

    for d in range(1, NZ):
        a, _, peer, _ = zpeer(d)
        send(d_copy(a, z, peer))
    for c in local_x:
        c.wait()
    for d in range(1, G):
        _, b, _, _ = gpeer(d)
        for i in range(NV):
            (f_copy(i, b, False) if H > 1 else x_copy(i, j0, b, me)).wait_recv()

    def weigh(j):
        @pl.loop(0, NV)
        def _(b):
            part[j, m128(b, W), :] = dot(vis[b], kv[j], TN).astype(BF16)
        for d in range(1, NZ):
            a, _, peer, _ = zpeer(d)
            send(r_copy(j, a, z, peer))

    weigh(j0)
    mine = dqs[m128(z, QR), :].astype(F32)
    for d in range(1, NZ):
        _, b, _, _ = zpeer(d)
        d_copy(z, b, me).wait_recv()
        mine += dqin[b].astype(F32)
    dqall[j0, m128(z, QR), :] = mine.astype(BF16)
    for d in range(1, NZ):
        a, _, peer, _ = zpeer(d)
        send(a_copy(a, z, peer))

    def spread():
        for d in range(1, NZ):
            _, b, _, _ = zpeer(d)
            a_copy(z, b, me).wait_recv()
        for d in range(1, G):
            a, _, peer, _ = gpeer(d)
            send(y_copy(a, j0, peer))

    for d in range(1, G - 1):
        a, _, peer, _ = gpeer(d)
        for c in range(NC):
            kv_copy(c, a, j0, peer).wait_send()
    if G > 1:
        a, _, peer, _ = gpeer(G - 1)
        for c in range(NC):
            send(kv_copy(c, a, j0, peer))
    if G == 1:
        spread()
    for d in range(1, G):
        _, b, _, _ = gpeer(d)
        for c in range(NC):
            kv_copy(c, j0, b, me).wait_recv()
        weigh(b)
        if d == min(2, G - 1):
            spread()
    for d in range(1, G):
        _, b, _, _ = gpeer(d)
        y_copy(j0, b, me).wait_recv()
    out_copy = pltpu.make_async_copy(dqall, q_out, loc.at[0])
    out_copy.start()

    for d in range(1, NZ):
        _, b, _, _ = zpeer(d)
        for j in range(G):
            r_copy(j, z, b, me).wait_recv()
    for j in range(G):
        acc = part[j, m128(z, FB), :].astype(F32)
        for d in range(1, NZ):
            _, b, _, _ = zpeer(d)
            acc += rsb[b, j].astype(F32)
        kw_out[:, pl.ds(j * HEAD_WIDTH, HEAD_WIDTH)] = acc[:, 0:HEAD_WIDTH]
        vw_out[:, pl.ds(j * HEAD_WIDTH, HEAD_WIDTH)] = acc[:, HEAD_WIDTH:]
    out_copy.wait()
    for c in sends:
        c.wait_send()


def shards(T, cores, text_queries, text_grads, vision_keys, video_value_rows, vision, lengths, frame_range):
    R, QW = text_queries.shape
    rows, kv_width = vision_keys.shape
    G = kv_width // HEAD_WIDTH
    if cores == 2 and G == 4 and T == G * G and vision.shape[1] % (T * 128) == 0 and HEAD_WIDTH % (G * R) == 0:
        return plane_shards(T, text_queries, text_grads, vision_keys, video_value_rows, vision, lengths, frame_range)
    M = QW // kv_width
    NZ = T // G
    DW = vision.shape[1]
    blk, NK, NR = M * R, G * rows, T * M * R
    FB = DW // T
    W = FB if FB % 128 == 0 else 256
    NV = DW // (G * W)
    FR = rows // FRAME_DEV
    NC = 4 if NK >= 16 * FR else 1
    cfg = dict(T=T, G=G, NZ=NZ, blk=blk, rows=rows, NK=NK, NR=NR, FR=FR, W=W, NV=NV, FB=FB, NC=NC, RB=min(NR, 512),
               H=2 if cores == 2 and G > 1 and W % 256 == 0 else 1)

    text_len = R * T
    row_ids = jnp.arange(text_len, dtype=jnp.int32)
    segment_ends = jnp.cumsum(lengths)
    segment = jnp.sum((row_ids[:, None] >= segment_ends[None, :]).astype(jnp.int32), axis=1)
    segment_pick = (
        segment[:, None] == jnp.arange(lengths.shape[0], dtype=jnp.int32)[None, :]
    ).astype(jnp.int32)
    bounds = jnp.sum(segment_pick[None] * frame_range.T[:, None, :], axis=2)
    bounds = jnp.broadcast_to(bounds.reshape(2, T, 1, R), (2, T, M, R)).reshape(2, NR)

    def split(a):
        return a.reshape(R, G, M, HEAD_WIDTH).transpose(1, 2, 0, 3).reshape(G, blk, HEAD_WIDTH)

    anyspec = pl.BlockSpec(memory_space=pl.ANY)
    vm = pl.BlockSpec(memory_space=pltpu.VMEM)
    V = pltpu.VMEM
    D = pltpu.SemaphoreType.DMA
    sem_pairs = []
    for shape in ((T,), (T,), (G,), (G,), (G, NV), (NZ,), (G, NC), (NZ,), (NZ,), (G,), (G, NZ), (G, NV)):
        sem_pairs += [D(shape), D(shape)]
    q_grad, kw, vw = pl.pallas_call(
        functools.partial(kernel, cfg),
        out_shape=(
            jax.ShapeDtypeStruct((G, NR, HEAD_WIDTH), BF16),
            jax.ShapeDtypeStruct((FB, kv_width), F32),
            jax.ShapeDtypeStruct((FB, kv_width), F32),
        ),
        in_specs=[anyspec] * 5 + [vm],
        out_specs=(anyspec, vm, vm),
        scratch_shapes=[
            V((NR, HEAD_WIDTH), BF16), V((NR, HEAD_WIDTH), BF16),
            V((NK, HEAD_WIDTH), BF16), V((NK, HEAD_WIDTH), BF16),
            V((NV, NK, W), BF16),
            V((NK, NR), F32), V((NK, NR), F32),
            V((8, NR), F32), V((NZ, 8, NR), F32), V((8, NR), F32),
            V((G, NK, 2 * HEAD_WIDTH), BF16),
            V((HEAD_WIDTH, NR), F32), V((NR, HEAD_WIDTH), BF16),
            V((NZ, NR // NZ, HEAD_WIDTH), BF16), V((G, NR, HEAD_WIDTH), BF16),
            V((G, DW // G, 2 * HEAD_WIDTH), BF16),
            V((NZ, G, FB, 2 * HEAD_WIDTH), BF16),
            D((4 + NV,)),
        ] + sem_pairs,
        compiler_params=pltpu.CompilerParams(
            collective_id=0, has_side_effects=True, vmem_limit_bytes=67043328
        ),
    )(split(text_queries), split(text_grads), vision_keys, video_value_rows, vision, bounds)
    q_grad = q_grad.reshape(G, T, M, R, HEAD_WIDTH).transpose(1, 3, 0, 2, 4).reshape(text_len, QW)
    return q_grad, kw, vw


def plane_kernel(cfg, q_in, g_in, k_in, v_in, x_in, lens, frames, q_out, kw_out, vw_out,
                 qraw, graw, qb, gb, kb, vb, vis, ebuf, dpb, stat, stin, coef, lim, kv, dqt, dqs, dqin, dqall,
                 gst, tmp, part, rin, ybs, ybr, loc, lx, qs, qr, zs, zr, ks, kr, xs, xr, fs, fr, ss, sr, kvs, kvr,
                 ds, dr, as_, ar, ys, yr, cs, cr, es, er):
    G, NZ, M, R, FR, NC = cfg["G"], cfg["NZ"], cfg["M"], cfg["R"], cfg["FR"], cfg["NC"]
    rows, NK, NR, JW, FB, RZ = cfg["rows"], cfg["NK"], cfg["NR"], cfg["JW"], cfg["FB"], cfg["RZ"]
    D = HEAD_WIDTH
    ZB = M * RZ
    scale = D ** (-0.5)
    me = lax.axis_index("tok")
    core = lax.axis_index("head")
    z, j = me // G, me % G
    y, x = j // 2, j % 2

    def m128(i, n):
        return pl.ds(pl.multiple_of(i * n, n), n)

    def remote(src, dst, s, r, peer):
        return pltpu.make_async_remote_copy(
            src_ref=src, dst_ref=dst, send_sem=s, recv_sem=r,
            device_id={"tok": peer}, device_id_type=pl.DeviceIdType.MESH)

    def near(d):
        return j ^ d, z * G + (j ^ d)

    def far(d):
        a, b = lax.rem(z + d, NZ), lax.rem(z + NZ - d, NZ)
        return a, b, a * G + j, b * G + j

    mirror = 2 * z > NZ - 1
    zz = jnp.where(mirror, NZ - 1 - z, z)

    def band(s):
        u = s - (NZ - 1 - 2 * zz)
        k, odd = u // 2, u % 2
        b = jnp.where(u < 0, NZ - 1 - s, k + odd * (2 * zz - 2 * k))
        return jnp.where(mirror, NZ - 1 - b, b)

    barrier = pltpu.get_barrier_semaphore()
    for d in range(1, G):
        pl.semaphore_signal(barrier, inc=1, device_id={"tok": near(d)[1]}, device_id_type=pl.DeviceIdType.MESH)
    for d in range(1, NZ):
        pl.semaphore_signal(barrier, inc=1, device_id={"tok": far(d)[2]}, device_id_type=pl.DeviceIdType.MESH)
    pl.semaphore_signal(barrier, inc=1, device_id={"head": 1 - core}, device_id_type=pl.DeviceIdType.MESH)
    pl.semaphore_wait(barrier, G + NZ - 1)

    sends = []

    def send(c):
        c.start()
        sends.append(c)

    def own_rows(t):
        return m128(t, R)

    def q_copy(d, t_from, peer, j_to):
        cols = m128(j_to, JW)
        return (remote(q_in.at[:, cols], qraw.at[own_rows(t_from)], qs.at[0, d], qr.at[0, d], peer),
                remote(g_in.at[:, cols], graw.at[own_rows(t_from)], qs.at[1, d], qr.at[1, d], peer))

    def zq_copy(z_to, z_from, peer):
        here = m128(z_from, RZ)
        return (remote(qraw.at[here], qraw.at[here], zs.at[0, z_to], zr.at[0, z_from], peer),
                remote(graw.at[here], graw.at[here], zs.at[1, z_to], zr.at[1, z_from], peer))

    def k_copy(d, j_to, j_from, peer):
        return (remote(k_in.at[:, m128(j_to, D)], kb.at[m128(j_from, rows)], ks.at[0, d], kr.at[0, d], peer),
                remote(v_in.at[:, m128(j_to, D)], vb.at[m128(j_from, rows)], ks.at[1, d], kr.at[1, d], peer))

    def lane_half(mine):
        return m128(core if mine else 1 - core, FB)

    def x_copy(kind, b, x_to, j_from, peer):
        cols = m128(b * G + core * 2 + x_to, FB)
        dst = vis.at[b, m128(j_from, rows), lane_half(True)]
        return remote(x_in.at[:, cols], dst, xs.at[kind, b], xr.at[kind, b], peer)

    def pass_copy(b, j_from, peer):
        here = vis.at[b, m128(j_from, rows), lane_half(True)]
        return remote(here, here, xs.at[2, b], xr.at[2, b], peer)

    def f_copy(kind, b, mine):
        here = vis.at[b, m128(j ^ (kind + 1), rows), lane_half(mine)]
        return pltpu.make_async_remote_copy(
            src_ref=here, dst_ref=here, send_sem=fs.at[kind, b], recv_sem=fr.at[kind, b],
            device_id={"head": 1 - core}, device_id_type=pl.DeviceIdType.MESH)

    local = [
        pltpu.make_async_copy(q_in.at[:, m128(j, JW)], qraw.at[own_rows(me)], loc.at[0]),
        pltpu.make_async_copy(g_in.at[:, m128(j, JW)], graw.at[own_rows(me)], loc.at[1]),
        pltpu.make_async_copy(k_in.at[:, m128(j, D)], kb.at[m128(j, rows)], loc.at[2]),
        pltpu.make_async_copy(v_in.at[:, m128(j, D)], vb.at[m128(j, rows)], loc.at[3]),
    ]
    for c in local:
        c.start()
    for d in range(G - 1, 0, -1):
        for c in q_copy(d, me, near(d)[1], near(d)[0]):
            send(c)
    for d in range(1, G):
        for c in k_copy(d, near(d)[0], j, near(d)[1]):
            send(c)
    local_x = []
    for b in range(NZ):
        for h in range(2):
            local_x.append(pltpu.make_async_copy(
                x_in.at[:, m128(b * G + 2 * h + x, FB)], vis.at[b, m128(j, rows), pl.ds(h * FB, FB)], lx.at[b, h]))

    col = lax.broadcasted_iota(jnp.int32, (1, NR), 1)
    text = (col // ZB) * RZ + col % RZ
    seg = jnp.zeros((1, NR), jnp.int32)
    end = jnp.int32(0)
    NS = cfg["NS"]
    for i in range(NS):
        end = end + lens[i]
        seg += (text >= end).astype(jnp.int32)
    first, last = jnp.zeros((1, NR), jnp.int32), jnp.zeros((1, NR), jnp.int32)
    for i in range(NS):
        first = jnp.where(seg == i, frames[0, i], first)
        last = jnp.where(seg == i, frames[1, i], last)
    lim[0:1, :] = first
    lim[1:2, :] = last
    stat[0:8, :] = jnp.zeros((8, NR), F32)

    for c in local[:2]:
        c.wait()
    for d in range(1, G):
        for c in q_copy(d, z * G + near(d)[0], me, j):
            c.wait_recv()
    for k in range(1, NZ):
        b = band(NZ - 1 - k)
        for c in zq_copy(b, z, b * G + j):
            send(c)
    for s in range(NZ):
        send(x_copy(0, band(s), 1 - x, j, near(1)[1]))
        send(x_copy(1, band(s), x, j, near(2)[1]))
    for c in local_x:
        c.start()
    for c in local[2:]:
        c.wait()

    n_frames = rows // FR

    def totals(g, zb):
        cols = m128(zb, ZB)
        lo, hi = lim[0:1, cols], lim[1:2, cols]
        base = z * G * n_frames + g * n_frames

        def tokens(f):
            return m128(g * n_frames + f, FR)

        top = jnp.full((1, ZB), NEG_FILL, F32)
        for f in range(n_frames):
            ok = (lo <= base + f) & (base + f < hi)
            sc = jnp.where(ok, dot(kb[tokens(f), :], qb[cols, :], NT) * scale, NEG_FILL)
            ebuf[tokens(f), cols] = sc
            top = jnp.maximum(top, jnp.max(sc, axis=0, keepdims=True))
        total = jnp.zeros((1, ZB), F32)
        dotted = jnp.zeros((1, ZB), F32)
        for f in range(n_frames):
            dp = dot(vb[tokens(f), :], gb[cols, :], NT)
            e = jnp.exp(ebuf[tokens(f), cols] - top)
            ebuf[tokens(f), cols] = e
            dpb[tokens(f), cols] = dp
            total += jnp.sum(e, axis=0, keepdims=True)
            dotted += jnp.sum(e * dp, axis=0, keepdims=True)
        gst[g, 0:1, cols] = top
        gst[g, 1:2, cols] = total
        gst[g, 2:3, cols] = dotted

    def s_copy(zb, z_to, z_from, peer):
        cols = m128(zb, ZB)
        return remote(stat.at[:, cols], stin.at[z_from, :, cols], ss.at[zb, z_to], sr.at[zb, z_from], peer)

    def plane_totals(zb):
        cols = m128(zb, ZB)
        top = gst[0, 0:1, cols]
        for g in range(1, G):
            top = jnp.maximum(top, gst[g, 0:1, cols])
        total = jnp.zeros((1, ZB), F32)
        dotted = jnp.zeros((1, ZB), F32)
        for g in range(G):
            w = jnp.exp(gst[g, 0:1, cols] - top)
            total += w * gst[g, 1:2, cols]
            dotted += w * gst[g, 2:3, cols]
        stat[0:1, cols] = top
        stat[1:2, cols] = total
        stat[2:3, cols] = dotted
        for d in range(1, NZ):
            send(s_copy(zb, far(d)[0], z, far(d)[2]))

    def landed(s):
        b = band(s)
        x_copy(0, b, x, near(1)[0], me).wait_recv()
        send(pass_copy(b, near(1)[0], near(2)[1]))
        send(f_copy(0, b, True))
        x_copy(1, b, x, near(2)[0], me).wait_recv()
        send(f_copy(1, b, True))

    have_g, have_z = {0}, set()

    def block(d, k):
        zb = band(NZ - 1 - k)
        if d not in have_g:
            have_g.add(d)
            for c in k_copy(d, j, near(d)[0], me):
                c.wait_recv()
        if k not in have_z:
            have_z.add(k)
            if k:
                for c in zq_copy(z, zb, me):
                    c.wait_recv()
            for raw, buf in ((qraw, qb), (graw, gb)):
                for m in range(M):
                    buf[m128(zb * M + m, RZ), :] = raw[m128(zb, RZ), m * D:(m + 1) * D]
        totals(j ^ d, zb)

    for d, k in ((0, 0), (1, 0), (2, 0), (0, 1), (1, 1), (2, 1), (3, 0)):
        block(d, k)
    plane_totals(band(NZ - 1))
    block(3, 1)
    plane_totals(band(NZ - 2))
    landed(0)
    for k in range(2, NZ):
        for d in range(G):
            block(d, k)
        plane_totals(band(NZ - 1 - k))
        landed(k - 1)

    stin[z] = stat[...]
    dqt[...] = jnp.zeros_like(dqt)
    for zb in range(NZ):
        for d in range(1, NZ):
            s_copy(zb, z, far(d)[1], me).wait_recv()
    top = stat[0:1, :]
    for i in range(NZ):
        top = jnp.maximum(top, stin[i, 0:1, :])
    total = jnp.zeros((1, NR), F32)
    dotted = jnp.zeros((1, NR), F32)
    for i in range(NZ):
        w = jnp.exp(stin[i, 0:1, :] - top)
        total += w * stin[i, 1:2, :]
        dotted += w * stin[i, 2:3, :]
    for g in range(G):
        coef[g:g + 1, :] = jnp.exp(gst[g, 0:1, :] - top) / total
    coef[G:G + 1, :] = dotted / total
    landed(NZ - 1)

    CH = NK // NC

    def kv_copy(c, peer):
        at = pl.ds(c * CH, CH)
        return remote(kv.at[0, at], kv.at[1, at], kvs.at[c], kvr.at[c], peer)

    for c in range(NC):
        @pl.loop(c * (CH // FR), (c + 1) * (CH // FR))
        def _(f):
            kt = kb[m128(f, FR), :].astype(F32).T.astype(BF16)
            dk = jnp.zeros((FR, D), F32)
            dv = jnp.zeros((FR, D), F32)
            for r in range(0, NR, ZB):
                cols = pl.ds(r, ZB)
                p = ebuf[m128(f, FR), cols] * coef[c:c + 1, cols]
                t = (p * (dpb[m128(f, FR), cols] - coef[G:G + 1, cols])).astype(BF16)
                dv += dot(p.astype(BF16), gb[cols, :])
                dk += dot(t, qb[cols, :])
                dqt[:, cols] += dot(kt, t)
            kv[0, m128(f, FR), 0:D] = (scale * dk).astype(BF16)
            kv[0, m128(f, FR), D:2 * D] = dv.astype(BF16)

        send(kv_copy(c, near(1)[1]))

    for zb in range(NZ):
        for i in range(ZB // D):
            t = (scale * dqt[:, pl.ds(zb * ZB + i * D, D)].T).astype(BF16)
            for k in range(D // RZ):
                m = i * (D // RZ) + k
                dqs[pl.ds(zb * RZ, RZ), pl.ds(m * D, D)] = t[k * RZ:(k + 1) * RZ, :]
    HW = JW // 2

    def half(u):
        return pl.ds(u * HW, HW)

    def d_copy(u, z_to, z_from, peer):
        return remote(dqs.at[m128(z_to, RZ), half(u)], dqin.at[z_from, :, half(u)], ds.at[u, z_to], dr.at[u, z_from], peer)

    def a_copy(u, z_to, z_from, peer):
        here = dqall.at[j, m128(z_from, RZ), half(u)]
        return remote(here, here, as_.at[u, z_to], ar.at[u, z_from], peer)

    def y_copy(u, d, j_from, peer, kind):
        here = dqall.at[j_from, :, half(u)]
        return remote(here, here, ys.at[kind, u], yr.at[kind, u], peer)

    for u in range(2):
        for d in range(1, NZ):
            send(d_copy(u, far(d)[0], z, far(d)[2]))
    for c in local_x:
        c.wait()

    def c_copy(side, b, h, peer):
        return remote(part.at[h, b], rin.at[side, b, h], cs.at[b, h], cr.at[side, b, h], peer)

    def weigh(b, h, slot):
        for i in range(2):
            tmp[slot, pl.ds(i * FB, FB), :] = dot(vis[b, :, i * FB:(i + 1) * FB], kv[h], TN)

    def gather(s):
        b = band(s)
        pass_copy(b, near(3)[0], me).wait_recv()
        send(f_copy(2, b, True))
        for kind in range(3):
            f_copy(kind, b, False).wait_recv()

    def onward(s, h, between=None):
        b = band(s)
        weigh(b, h, 0)
        side = (b < z).astype(jnp.int32)
        fed = jnp.where(b > z, z > 0, z < NZ - 1)
        out = c_copy(side, b, h, (z + 1 - 2 * side) * G + j)

        def pass_on(extra):
            part[h, b] = (tmp[0] + extra if extra is not None else tmp[0]).astype(BF16)
            out.start()

        @pl.when(jnp.logical_not(fed))
        def _():
            pass_on(None)
        if between is not None:
            between()

        @pl.when(fed)
        def _():
            c_copy(side, b, h, me).wait_recv()
            pass_on(rin[side, b, h].astype(F32))
        sends.append(out)

    def e_copy(h, peer):
        return remote(ybs.at[h], ybr.at[h], es.at[h], er.at[h], peer)

    def finish(h):
        @pl.when(z > 0)
        def _():
            c_copy(0, z, h, me).wait_recv()
            tmp[1 + h] += rin[0, z, h].astype(F32)

        @pl.when(z < NZ - 1)
        def _():
            c_copy(1, z, h, me).wait_recv()
            tmp[1 + h] += rin[1, z, h].astype(F32)
        ybs[h] = tmp[1 + h, m128(1 - y, FB), :].astype(BF16)
        send(e_copy(h, near(2)[1]))
        at = m128(j ^ h, D)
        kw_out[:, at] = tmp[1 + h, m128(y, FB), 0:D]
        vw_out[:, at] = tmp[1 + h, m128(y, FB), D:2 * D]

    def summed_dq(u):
        mine = dqs[m128(z, RZ), half(u)].astype(F32)
        for d in range(1, NZ):
            d_copy(u, z, far(d)[1], me).wait_recv()
            mine += dqin[far(d)[1], :, half(u)].astype(F32)
        dqall[j, m128(z, RZ), half(u)] = mine.astype(BF16)
        for d in range(1, NZ):
            send(a_copy(u, far(d)[0], z, far(d)[2]))

    def shared_dq(u):
        for d in range(1, NZ):
            a_copy(u, z, far(d)[1], me).wait_recv()
        send(y_copy(u, 1, j, near(1)[1], 0))
        send(y_copy(u, 2, j, near(2)[1], 1))

    gather(0)
    onward(0, 0, lambda: summed_dq(0))
    gather(1)
    onward(1, 0, lambda: summed_dq(1))
    gather(2)
    onward(2, 0)
    gather(3)
    weigh(z, 0, 1)
    for c in range(NC):
        kv_copy(c, me).wait_recv()
    onward(0, 1, lambda: shared_dq(0))
    onward(1, 1, lambda: shared_dq(1))
    onward(2, 1)
    weigh(z, 1, 2)
    finish(0)
    y_copy(0, 1, near(1)[0], me, 0).wait_recv()
    send(y_copy(0, 2, near(1)[0], near(2)[1], 2))
    y_copy(1, 2, near(2)[0], me, 1).wait_recv()
    send(y_copy(1, 1, near(2)[0], near(1)[1], 2))
    finish(1)

    outs = []

    def put(i):
        c = pltpu.make_async_copy(dqall.at[j ^ i], q_out.at[:, m128(j ^ i, JW)], loc.at[i])
        c.start()
        outs.append(c)

    put(0)
    y_copy(1, 1, near(1)[0], me, 0).wait_recv()
    put(1)
    y_copy(0, 2, near(2)[0], me, 1).wait_recv()
    put(2)
    y_copy(0, 2, near(3)[0], me, 2).wait_recv()
    y_copy(1, 1, near(3)[0], me, 2).wait_recv()
    put(3)
    for h in range(2):
        e_copy(h, me).wait_recv()
        at = m128(j ^ (2 + h), D)
        kw_out[:, at] = ybr[h, :, 0:D].astype(F32)
        vw_out[:, at] = ybr[h, :, D:2 * D].astype(F32)
    for c in outs:
        c.wait()
    for c in sends:
        c.wait_send()


def plane_shards(T, text_queries, text_grads, vision_keys, video_value_rows, vision, lengths, frame_range):
    R, QW = text_queries.shape
    rows, kv_width = vision_keys.shape
    G = kv_width // HEAD_WIDTH
    M = QW // kv_width
    NZ = T // G
    DW = vision.shape[1]
    FB = DW // T
    NK, RZ, JW = G * rows, G * R, M * HEAD_WIDTH
    NR = T * R * M
    cfg = dict(G=G, NZ=NZ, M=M, R=R, FR=rows // FRAME_DEV, NC=4, rows=rows, NK=NK, NR=NR, JW=JW, FB=FB, RZ=RZ,
               NS=lengths.shape[0])
    anyspec = pl.BlockSpec(memory_space=pl.ANY)
    vm = pl.BlockSpec(memory_space=pltpu.VMEM)
    sm = pl.BlockSpec(memory_space=pltpu.SMEM)
    V = pltpu.VMEM
    D = pltpu.SemaphoreType.DMA
    W2 = 2 * HEAD_WIDTH
    pairs = []
    for a, b in (((2, G),) * 2, ((2, NZ),) * 2, ((2, G),) * 2, ((3, NZ),) * 2, ((3, NZ),) * 2, ((NZ, NZ),) * 2, ((cfg["NC"],),) * 2,
                 ((2, NZ),) * 2, ((2, NZ),) * 2, ((3, 2),) * 2, ((NZ, 2), (2, NZ, 2)), ((2,),) * 2):
        pairs += [D(a), D(b)]
    return pl.pallas_call(
        functools.partial(plane_kernel, cfg),
        out_shape=(
            jax.ShapeDtypeStruct((T * R, QW), BF16),
            jax.ShapeDtypeStruct((FB, kv_width), F32),
            jax.ShapeDtypeStruct((FB, kv_width), F32),
        ),
        in_specs=[anyspec] * 5 + [sm] * 2,
        out_specs=(anyspec, vm, vm),
        scratch_shapes=[
            V((T * R, JW), BF16), V((T * R, JW), BF16),
            V((NR, HEAD_WIDTH), BF16), V((NR, HEAD_WIDTH), BF16),
            V((NK, HEAD_WIDTH), BF16), V((NK, HEAD_WIDTH), BF16),
            V((NZ, NK, 2 * FB), BF16),
            V((NK, NR), F32), V((NK, NR), F32),
            V((8, NR), F32), V((NZ, 8, NR), F32), V((8, NR), F32), V((8, NR), jnp.int32),
            V((2, NK, W2), BF16),
            V((HEAD_WIDTH, NR), F32), V((T * R, JW), BF16),
            V((NZ, RZ, JW), BF16), V((G, T * R, JW), BF16),
            V((G, 8, NR), F32),
            V((3, 2 * FB, W2), F32), V((2, NZ, 2 * FB, W2), BF16), V((2, NZ, 2, 2 * FB, W2), BF16),
            V((2, FB, W2), BF16), V((2, FB, W2), BF16),
            D((4,)), D((NZ, 2)),
        ] + pairs,
        compiler_params=pltpu.CompilerParams(
            collective_id=0, has_side_effects=True, vmem_limit_bytes=67043328
        ),
    )(text_queries, text_grads, vision_keys, video_value_rows, vision, lengths, frame_range.T)


def solution(mesh):
    return jax.shard_map(
        functools.partial(shards, mesh.shape["tok"], mesh.shape["head"]),
        mesh=mesh,
        in_specs=(
            P("tok", "head"),
            P("tok", "head"),
            P("tok", "head"),
            P("tok", "head"),
            P("tok", None),
            P(),
            P(),
        ),
        out_specs=(P(None, "head"), P("tok", "head"), P("tok", "head")),
        check_vma=False,
    )
```

```python
import functools

import jax
import jax.numpy as jnp
from jax import lax
from jax.experimental import pallas as pl
from jax.experimental.pallas import tpu as pltpu
from jax.sharding import PartitionSpec as P

HEAD_WIDTH = 128
FRAME_DEV = 4
NEG_FILL = -1e30
NT = (((1,), (1,)), ((), ()))
TN = (((0,), (0,)), ((), ()))
F32 = jnp.float32
BF16 = jnp.bfloat16


def dot(a, b, dims=(((1,), (0,)), ((), ()))):
    return lax.dot_general(a, b, dims, preferred_element_type=F32)


def kernel(cfg, q_in, g_in, k_in, v_in, x_in, bounds, q_out, kw_out, vw_out,
           qb, gb, kb, vb, vis, ebuf, dpb, stat, stin, coef, kv, dqt, dqs, dqin, dqall, part, rsb,
           loc, qs, qr, gs, gr, ks, kr, vs, vr, xs, xr, ss, sr, kvs, kvr, ds, dr, as_, ar, ys, yr, rs, rr, fs, fr):
    T, G, NZ = cfg["T"], cfg["G"], cfg["NZ"]
    blk, rows, NK, NR, FR = cfg["blk"], cfg["rows"], cfg["NK"], cfg["NR"], cfg["FR"]
    W, NV, FB = cfg["W"], cfg["NV"], cfg["FB"]
    H = cfg["H"]
    RB = cfg["RB"]
    scale = HEAD_WIDTH ** (-0.5)
    me = lax.axis_index("tok")
    z, j0 = me // G, me % G

    def remote(src, dst, s, r, peer):
        return pltpu.make_async_remote_copy(
            src_ref=src, dst_ref=dst, send_sem=s, recv_sem=r,
            device_id={"tok": peer}, device_id_type=pl.DeviceIdType.MESH)

    def m128(i, n):
        return pl.ds(pl.multiple_of(i * n, n), n)

    barrier = pltpu.get_barrier_semaphore()
    for d in range(1, T):
        pl.semaphore_signal(barrier, inc=1, device_id={"tok": lax.rem(me + d, T)}, device_id_type=pl.DeviceIdType.MESH)
    twin = lax.axis_index("head")
    if H > 1:
        twin = 1 - twin
        pl.semaphore_signal(barrier, inc=1, device_id={"head": twin}, device_id_type=pl.DeviceIdType.MESH)
    pl.semaphore_wait(barrier, T - 1 + (H > 1))

    def tpeer(d):
        return lax.rem(me + d, T), lax.rem(me + T - d, T)

    def gpeer(d):
        a, b = (j0 ^ d, j0 ^ d) if G & (G - 1) == 0 else (lax.rem(j0 + d, G), lax.rem(j0 + G - d, G))
        return a, b, z * G + a, z * G + b

    def zpeer(d):
        a, b = lax.rem(z + d, NZ), lax.rem(z + NZ - d, NZ)
        return a, b, a * G + j0, b * G + j0

    sends = []

    def send(c):
        c.start()
        sends.append(c)

    def q_copy(t_to, t_from):
        return (remote(q_in.at[lax.rem(t_to, G)], qb.at[m128(t_from, blk)], qs.at[t_to], qr.at[t_from], t_to),
                remote(g_in.at[lax.rem(t_to, G)], gb.at[m128(t_from, blk)], gs.at[t_to], gr.at[t_from], t_to))

    def k_copy(j_to, j_from, peer):
        return (remote(k_in.at[:, m128(j_to, 128)], kb.at[m128(j_from, rows)], ks.at[j_to], kr.at[j_from], peer),
                remote(v_in.at[:, m128(j_to, 128)], vb.at[m128(j_from, rows)], vs.at[j_to], vr.at[j_from], peer))

    WH = W // H
    half = lax.axis_index("head") * WH if H > 1 else 0

    def x_copy(b, j_to, j_from, peer):
        cols = pl.ds(pl.multiple_of((b * G + j_to) * W + half, WH), WH)
        dst = vis.at[b, m128(j_from, rows), pl.ds(pl.multiple_of(half, WH), WH)]
        return remote(x_in.at[:, cols], dst, xs.at[j_to, b], xr.at[j_from, b], peer)

    def f_copy(b, j_from, mine):
        at = half if mine else WH - half
        here = vis.at[b, m128(j_from, rows), pl.ds(pl.multiple_of(at, WH), WH)]
        return pltpu.make_async_remote_copy(
            src_ref=here, dst_ref=here, send_sem=fs.at[j_from, b], recv_sem=fr.at[j_from, b],
            device_id={"head": twin}, device_id_type=pl.DeviceIdType.MESH)

    local = [
        pltpu.make_async_copy(q_in.at[j0], qb.at[m128(me, blk)], loc.at[0]),
        pltpu.make_async_copy(g_in.at[j0], gb.at[m128(me, blk)], loc.at[1]),
        pltpu.make_async_copy(k_in.at[:, m128(j0, 128)], kb.at[m128(j0, rows)], loc.at[2]),
        pltpu.make_async_copy(v_in.at[:, m128(j0, 128)], vb.at[m128(j0, rows)], loc.at[3]),
    ]
    local_x = [pltpu.make_async_copy(x_in.at[:, m128(b * G + j0, W)], vis.at[b, m128(j0, rows)], loc.at[4 + b]) for b in range(NV)]
    for c in local:
        c.start()
    def q_sends(zd):
        a, _, _, _ = zpeer(zd)
        for i in range(G):
            to = a * G + (lax.rem(j0 + i, G) if zd else gpeer(i)[0])
            if zd or i:
                for c in q_copy(to, me):
                    send(c)

    q_sends(0)
    for d in range(1, G):
        a, _, peer, _ = gpeer(d)
        for c in k_copy(a, j0, peer):
            send(c)
    for d in range(1, NZ):
        q_sends(d)
    for c in local_x:
        c.start()
    for c in local:
        c.wait()
    for d in range(1, G):
        _, b, _, _ = gpeer(d)
        for c in k_copy(j0, b, me):
            c.wait_recv()

    def q_wait(zd):
        _, b, _, _ = zpeer(zd)
        for i in range(G):
            if zd or i:
                frm = b * G + (i if zd else gpeer(i)[1])
                for c in q_copy(me, frm):
                    c.wait_recv()

    n_frames = NK // FR
    frame0 = z * n_frames
    stat[0:1, :] = jnp.full((1, NR), NEG_FILL, F32)
    stat[1:8, :] = jnp.zeros((7, NR), F32)

    def totals(cols, width):
        first, end = bounds[0:1, cols], bounds[1:2, cols]
        UN = 2 if n_frames % 2 == 0 else 1

        def scored(i, top):
            for u in range(UN):
                f = i * UN + u
                ok = (first <= frame0 + f) & (frame0 + f < end)
                s = jnp.where(ok, dot(kb[m128(f, FR), :], qb[cols, :], NT) * scale, NEG_FILL)
                ebuf[m128(f, FR), cols] = s
                top = jnp.maximum(top, jnp.max(s, axis=0, keepdims=True))
            return top

        top = lax.fori_loop(0, n_frames // UN, scored, jnp.full((1, width), NEG_FILL, F32))

        def summed(i, carry):
            total, dotted = carry
            for u in range(UN):
                f = i * UN + u
                dp = dot(vb[m128(f, FR), :], gb[cols, :], NT)
                e = jnp.exp(ebuf[m128(f, FR), cols] - top)
                ebuf[m128(f, FR), cols] = e
                dpb[m128(f, FR), cols] = dp
                total += jnp.sum(e, axis=0, keepdims=True)
                dotted += jnp.sum(e * dp, axis=0, keepdims=True)
            return total, dotted

        zero = jnp.zeros((1, width), F32)
        total, dotted = lax.fori_loop(0, n_frames // UN, summed, (zero, zero))
        stat[0:1, cols] = top
        stat[1:2, cols] = total
        stat[2:3, cols] = dotted

    def x_sends():
        for d in range(1, G):
            a, _, peer, _ = gpeer(d)
            for b in range(NV):
                send(x_copy(b, a, j0, peer))

    by_z = (NR // NZ) % 128 == 0
    for d in range(NZ):
        q_wait(d)
        if d == NZ - 1:
            x_sends()
        if by_z:
            totals(m128(zpeer(d)[1], NR // NZ), NR // NZ)
    if not by_z:
        for r in range(0, NR, RB):
            totals(pl.ds(r, RB), RB)

    def s_copy(z_to, z_from, peer):
        return remote(stat, stin.at[z_from], ss.at[z_to], sr.at[z_from], peer)

    for d in range(1, NZ):
        a, _, peer, _ = zpeer(d)
        send(s_copy(a, z, peer))
    stin[z] = stat[...]
    for d in range(1, NZ):
        _, b, _, _ = zpeer(d)
        s_copy(z, b, me).wait_recv()
    top = stat[0:1, :]
    for i in range(NZ):
        top = jnp.maximum(top, stin[i, 0:1, :])
    total = jnp.zeros((1, NR), F32)
    dotted = jnp.zeros((1, NR), F32)
    for i in range(NZ):
        w = jnp.exp(stin[i, 0:1, :] - top)
        total += w * stin[i, 1:2, :]
        dotted += w * stin[i, 2:3, :]
    coef[0:1, :] = jnp.exp(stat[0:1, :] - top) / total
    coef[1:2, :] = dotted / total
    dqt[...] = jnp.zeros_like(dqt)

    NC = cfg["NC"]
    CH = NK // NC

    def kv_copy(c, j_to, j_from, peer):
        here = kv.at[j_from, pl.ds(c * CH, CH)]
        return remote(here, here, kvs.at[j_to, c], kvr.at[j_from, c], peer)

    for c in range(NC):
        @pl.loop(c * (CH // FR), (c + 1) * (CH // FR))
        def _(f):
            kt = kb[m128(f, FR), :].astype(F32).T.astype(BF16)
            dk = jnp.zeros((FR, HEAD_WIDTH), F32)
            dv = jnp.zeros((FR, HEAD_WIDTH), F32)
            for r in range(0, NR, RB):
                cols = pl.ds(r, RB)
                p = ebuf[m128(f, FR), cols] * coef[0:1, cols]
                t = (p * (dpb[m128(f, FR), cols] - coef[1:2, cols])).astype(BF16)
                dv += dot(p.astype(BF16), gb[cols, :])
                dk += dot(t, qb[cols, :])
                dqt[:, cols] += dot(kt, t)
            kv[j0, m128(f, FR), 0:HEAD_WIDTH] = (scale * dk).astype(BF16)
            kv[j0, m128(f, FR), HEAD_WIDTH:2 * HEAD_WIDTH] = dv.astype(BF16)

        for d in range(1, G - 1):
            a, _, peer, _ = gpeer(d)
            kv_copy(c, a, j0, peer).start()
        if H > 1 and c == NC // 2:
            for d in range(1, G):
                _, b, _, _ = gpeer(d)
                for i in range(NV):
                    x_copy(i, j0, b, me).wait_recv()
                    send(f_copy(i, b, True))

    for r in range(0, NR, 128):
        dqs[pl.ds(r, 128), :] = (scale * dqt[:, pl.ds(r, 128)].T).astype(BF16)
    QR = NR // NZ

    def d_copy(z_to, z_from, peer):
        return remote(dqs.at[m128(z_to, QR)], dqin.at[z_from], ds.at[z_to], dr.at[z_from], peer)

    def a_copy(z_to, z_from, peer):
        here = dqall.at[j0, m128(z_from, QR)]
        return remote(here, here, as_.at[z_to], ar.at[z_from], peer)

    def y_copy(j_to, j_from, peer):
        here = dqall.at[j_from]
        return remote(here, here, ys.at[j_to], yr.at[j_from], peer)

    def r_copy(j, z_to, z_from, peer):
        return remote(part.at[j, m128(z_to, FB)], rsb.at[z_from, j], rs.at[j, z_to], rr.at[j, z_from], peer)

    for d in range(1, NZ):
        a, _, peer, _ = zpeer(d)
        send(d_copy(a, z, peer))
    for c in local_x:
        c.wait()
    for d in range(1, G):
        _, b, _, _ = gpeer(d)
        for i in range(NV):
            (f_copy(i, b, False) if H > 1 else x_copy(i, j0, b, me)).wait_recv()

    def weigh(j):
        @pl.loop(0, NV)
        def _(b):
            part[j, m128(b, W), :] = dot(vis[b], kv[j], TN).astype(BF16)
        for d in range(1, NZ):
            a, _, peer, _ = zpeer(d)
            send(r_copy(j, a, z, peer))

    weigh(j0)
    mine = dqs[m128(z, QR), :].astype(F32)
    for d in range(1, NZ):
        _, b, _, _ = zpeer(d)
        d_copy(z, b, me).wait_recv()
        mine += dqin[b].astype(F32)
    dqall[j0, m128(z, QR), :] = mine.astype(BF16)
    for d in range(1, NZ):
        a, _, peer, _ = zpeer(d)
        send(a_copy(a, z, peer))

    def spread():
        for d in range(1, NZ):
            _, b, _, _ = zpeer(d)
            a_copy(z, b, me).wait_recv()
        for d in range(1, G):
            a, _, peer, _ = gpeer(d)
            send(y_copy(a, j0, peer))

    for d in range(1, G - 1):
        a, _, peer, _ = gpeer(d)
        for c in range(NC):
            kv_copy(c, a, j0, peer).wait_send()
    if G > 1:
        a, _, peer, _ = gpeer(G - 1)
        for c in range(NC):
            send(kv_copy(c, a, j0, peer))
    if G == 1:
        spread()
    for d in range(1, G):
        _, b, _, _ = gpeer(d)
        for c in range(NC):
            kv_copy(c, j0, b, me).wait_recv()
        weigh(b)
        if d == min(2, G - 1):
            spread()
    for d in range(1, G):
        _, b, _, _ = gpeer(d)
        y_copy(j0, b, me).wait_recv()
    out_copy = pltpu.make_async_copy(dqall, q_out, loc.at[0])
    out_copy.start()

    for d in range(1, NZ):
        _, b, _, _ = zpeer(d)
        for j in range(G):
            r_copy(j, z, b, me).wait_recv()
    for j in range(G):
        acc = part[j, m128(z, FB), :].astype(F32)
        for d in range(1, NZ):
            _, b, _, _ = zpeer(d)
            acc += rsb[b, j].astype(F32)
        kw_out[:, pl.ds(j * HEAD_WIDTH, HEAD_WIDTH)] = acc[:, 0:HEAD_WIDTH]
        vw_out[:, pl.ds(j * HEAD_WIDTH, HEAD_WIDTH)] = acc[:, HEAD_WIDTH:]
    out_copy.wait()
    for c in sends:
        c.wait_send()


def shards(T, cores, text_queries, text_grads, vision_keys, video_value_rows, vision, lengths, frame_range):
    R, QW = text_queries.shape
    rows, kv_width = vision_keys.shape
    G = kv_width // HEAD_WIDTH
    if cores == 2 and G == 4 and T == G * G and vision.shape[1] % (T * 128) == 0 and HEAD_WIDTH % (G * R) == 0 and 2 * vision.shape[1] == T * rows:
        return plane_shards(T, text_queries, text_grads, vision_keys, video_value_rows, vision, lengths, frame_range)
    M = QW // kv_width
    NZ = T // G
    DW = vision.shape[1]
    blk, NK, NR = M * R, G * rows, T * M * R
    FB = DW // T
    W = FB if FB % 128 == 0 else 256
    NV = DW // (G * W)
    FR = rows // FRAME_DEV
    NC = 4 if NK >= 16 * FR else 1
    cfg = dict(T=T, G=G, NZ=NZ, blk=blk, rows=rows, NK=NK, NR=NR, FR=FR, W=W, NV=NV, FB=FB, NC=NC, RB=min(NR, 512),
               H=2 if cores == 2 and G > 1 and W % 256 == 0 else 1)

    text_len = R * T
    row_ids = jnp.arange(text_len, dtype=jnp.int32)
    segment_ends = jnp.cumsum(lengths)
    segment = jnp.sum((row_ids[:, None] >= segment_ends[None, :]).astype(jnp.int32), axis=1)
    segment_pick = (
        segment[:, None] == jnp.arange(lengths.shape[0], dtype=jnp.int32)[None, :]
    ).astype(jnp.int32)
    bounds = jnp.sum(segment_pick[None] * frame_range.T[:, None, :], axis=2)
    bounds = jnp.broadcast_to(bounds.reshape(2, T, 1, R), (2, T, M, R)).reshape(2, NR)

    def split(a):
        return a.reshape(R, G, M, HEAD_WIDTH).transpose(1, 2, 0, 3).reshape(G, blk, HEAD_WIDTH)

    anyspec = pl.BlockSpec(memory_space=pl.ANY)
    vm = pl.BlockSpec(memory_space=pltpu.VMEM)
    V = pltpu.VMEM
    D = pltpu.SemaphoreType.DMA
    sem_pairs = []
    for shape in ((T,), (T,), (G,), (G,), (G, NV), (NZ,), (G, NC), (NZ,), (NZ,), (G,), (G, NZ), (G, NV)):
        sem_pairs += [D(shape), D(shape)]
    q_grad, kw, vw = pl.pallas_call(
        functools.partial(kernel, cfg),
        out_shape=(
            jax.ShapeDtypeStruct((G, NR, HEAD_WIDTH), BF16),
            jax.ShapeDtypeStruct((FB, kv_width), F32),
            jax.ShapeDtypeStruct((FB, kv_width), F32),
        ),
        in_specs=[anyspec] * 5 + [vm],
        out_specs=(anyspec, vm, vm),
        scratch_shapes=[
            V((NR, HEAD_WIDTH), BF16), V((NR, HEAD_WIDTH), BF16),
            V((NK, HEAD_WIDTH), BF16), V((NK, HEAD_WIDTH), BF16),
            V((NV, NK, W), BF16),
            V((NK, NR), F32), V((NK, NR), F32),
            V((8, NR), F32), V((NZ, 8, NR), F32), V((8, NR), F32),
            V((G, NK, 2 * HEAD_WIDTH), BF16),
            V((HEAD_WIDTH, NR), F32), V((NR, HEAD_WIDTH), BF16),
            V((NZ, NR // NZ, HEAD_WIDTH), BF16), V((G, NR, HEAD_WIDTH), BF16),
            V((G, DW // G, 2 * HEAD_WIDTH), BF16),
            V((NZ, G, FB, 2 * HEAD_WIDTH), BF16),
            D((4 + NV,)),
        ] + sem_pairs,
        compiler_params=pltpu.CompilerParams(
            collective_id=0, has_side_effects=True, vmem_limit_bytes=67043328
        ),
    )(split(text_queries), split(text_grads), vision_keys, video_value_rows, vision, bounds)
    q_grad = q_grad.reshape(G, T, M, R, HEAD_WIDTH).transpose(1, 3, 0, 2, 4).reshape(text_len, QW)
    return q_grad, kw, vw


def plane_kernel(cfg, q_in, g_in, k_in, v_in, x_in, lens, frames, q_out, kw_out, vw_out,
                 qraw, graw, qb, gb, kb, vb, vis, ebuf, dpb, stat, stin, coef, lim, kv, dqt, dqs, dqin, dqall,
                 gst, ktb, wres, ws, tmp, part, rin, ybs, ybr, loc, lx, qs, qr, zs, zr, ks, kr, xs, xr, fs, fr, ss, sr, kvs, kvr,
                 ds, dr, as_, ar, ys, yr, cs, cr, es, er):
    G, NZ, M, R, FR, NC = cfg["G"], cfg["NZ"], cfg["M"], cfg["R"], cfg["FR"], cfg["NC"]
    rows, NK, NR, JW, FB, RZ = cfg["rows"], cfg["NK"], cfg["NR"], cfg["JW"], cfg["FB"], cfg["RZ"]
    D = HEAD_WIDTH
    ZB = M * RZ
    scale = D ** (-0.5)
    me = lax.axis_index("tok")
    core = lax.axis_index("head")
    z, j = me // G, me % G
    y, x = j // 2, j % 2

    def m128(i, n):
        return pl.ds(pl.multiple_of(i * n, n), n)

    def remote(src, dst, s, r, peer):
        return pltpu.make_async_remote_copy(
            src_ref=src, dst_ref=dst, send_sem=s, recv_sem=r,
            device_id={"tok": peer}, device_id_type=pl.DeviceIdType.MESH)

    def near(d):
        return j ^ d, z * G + (j ^ d)

    def far(d):
        a, b = lax.rem(z + d, NZ), lax.rem(z + NZ - d, NZ)
        return a, b, a * G + j, b * G + j

    mirror = 2 * z > NZ - 1
    zz = jnp.where(mirror, NZ - 1 - z, z)

    def band(s):
        u = s - (NZ - 1 - 2 * zz)
        k, odd = u // 2, u % 2
        b = jnp.where(u < 0, NZ - 1 - s, k + odd * (2 * zz - 2 * k))
        return jnp.where(mirror, NZ - 1 - b, b)

    barrier = pltpu.get_barrier_semaphore()
    for d in range(1, G):
        pl.semaphore_signal(barrier, inc=1, device_id={"tok": near(d)[1]}, device_id_type=pl.DeviceIdType.MESH)
    for d in range(1, NZ):
        pl.semaphore_signal(barrier, inc=1, device_id={"tok": far(d)[2]}, device_id_type=pl.DeviceIdType.MESH)
    pl.semaphore_signal(barrier, inc=1, device_id={"head": 1 - core}, device_id_type=pl.DeviceIdType.MESH)
    pl.semaphore_wait(barrier, G + NZ - 1)

    sends = []

    def send(c):
        c.start()
        sends.append(c)

    def own_rows(t):
        return m128(t, R)

    def q_copy(d, t_from, peer, j_to):
        cols = m128(j_to, JW)
        return (remote(q_in.at[:, cols], qraw.at[own_rows(t_from)], qs.at[0, d], qr.at[0, d], peer),
                remote(g_in.at[:, cols], graw.at[own_rows(t_from)], qs.at[1, d], qr.at[1, d], peer))

    low, high = z > 0, z < NZ - 1
    inner = low & high

    def zq_copy(side, a, b):
        here = (qraw, graw)[a].at[m128(b, RZ)]
        return remote(here, here, zs.at[side, a, b], zr.at[a, b], (z + 1 - 2 * side) * G + j)

    def zq_each(act, b, into):
        for a in range(2):
            if into:
                zq_copy(0, a, b).wait_recv()

            @pl.when(high & (b <= z))
            def _():
                act(zq_copy(0, a, b))

            @pl.when(low & (b >= z))
            def _():
                act(zq_copy(1, a, b))

    def k_copy(d, j_to, j_from, peer):
        return (remote(k_in.at[:, m128(j_to, D)], kb.at[m128(j_from, rows)], ks.at[0, d], kr.at[0, d], peer),
                remote(v_in.at[:, m128(j_to, D)], vb.at[m128(j_from, rows)], ks.at[1, d], kr.at[1, d], peer))

    def lane_half(mine):
        return m128(core if mine else 1 - core, FB)

    def x_copy(kind, b, x_to, j_from, peer):
        cols = m128(b * G + core * 2 + x_to, FB)
        dst = vis.at[b, m128(j_from, rows), lane_half(True)]
        return remote(x_in.at[:, cols], dst, xs.at[kind, b], xr.at[kind, b], peer)

    def pass_copy(b, j_from, peer):
        here = vis.at[b, m128(j_from, rows), lane_half(True)]
        return remote(here, here, xs.at[2, b], xr.at[2, b], peer)

    def f_copy(kind, b, mine):
        here = vis.at[b, m128(j ^ (kind + 1), rows), lane_half(mine)]
        return pltpu.make_async_remote_copy(
            src_ref=here, dst_ref=here, send_sem=fs.at[kind, b], recv_sem=fr.at[kind, b],
            device_id={"head": 1 - core}, device_id_type=pl.DeviceIdType.MESH)

    local = [
        pltpu.make_async_copy(q_in.at[:, m128(j, JW)], qraw.at[own_rows(me)], loc.at[0]),
        pltpu.make_async_copy(g_in.at[:, m128(j, JW)], graw.at[own_rows(me)], loc.at[1]),
        pltpu.make_async_copy(k_in.at[:, m128(j, D)], kb.at[m128(j, rows)], loc.at[2]),
        pltpu.make_async_copy(v_in.at[:, m128(j, D)], vb.at[m128(j, rows)], loc.at[3]),
    ]
    for c in local:
        c.start()
    for d in range(G - 1, 0, -1):
        for c in q_copy(d, me, near(d)[1], near(d)[0]):
            send(c)
    for d in range(1, G):
        for c in k_copy(d, near(d)[0], j, near(d)[1]):
            send(c)
    local_x = []
    for b in range(NZ):
        for h in range(2):
            local_x.append(pltpu.make_async_copy(
                x_in.at[:, m128(b * G + 2 * h + x, FB)], vis.at[b, m128(j, rows), pl.ds(h * FB, FB)], lx.at[b, h]))

    col = lax.broadcasted_iota(jnp.int32, (1, NR), 1)
    text = (col // ZB) * RZ + col % RZ
    seg = jnp.zeros((1, NR), jnp.int32)
    end = jnp.int32(0)
    NS = cfg["NS"]
    for i in range(NS):
        end = end + lens[i]
        seg += (text >= end).astype(jnp.int32)
    first, last = jnp.zeros((1, NR), jnp.int32), jnp.zeros((1, NR), jnp.int32)
    for i in range(NS):
        first = jnp.where(seg == i, frames[0, i], first)
        last = jnp.where(seg == i, frames[1, i], last)
    lim[0:1, :] = first
    lim[1:2, :] = last
    stat[0:8, :] = jnp.zeros((8, NR), F32)

    for c in local[:2]:
        c.wait()
    for d in range(1, G):
        for c in q_copy(d, z * G + near(d)[0], me, j):
            c.wait_recv()
    zq_each(lambda c: c.start(), z, False)
    for s in range(NZ):
        send(x_copy(0, band(s), 1 - x, j, near(1)[1]))
        if s < NZ // 2:
            send(x_copy(1, band(s), x, j, near(2)[1]))
    for c in local_x:
        c.start()
    for c in local[2:]:
        c.wait()

    n_frames = rows // FR

    def totals(g, zb):
        cols = m128(zb, ZB)
        lo, hi = lim[0:1, cols], lim[1:2, cols]
        base = z * G * n_frames + g * n_frames

        def tokens(f):
            return m128(g * n_frames + f, FR)

        top = jnp.full((1, ZB), NEG_FILL, F32)
        for f in range(n_frames):
            ok = (lo <= base + f) & (base + f < hi)
            sc = jnp.where(ok, dot(kb[tokens(f), :], qb[cols, :], NT) * scale, NEG_FILL)
            ebuf[tokens(f), cols] = sc
            top = jnp.maximum(top, jnp.max(sc, axis=0, keepdims=True))
        total = jnp.zeros((1, ZB), F32)
        dotted = jnp.zeros((1, ZB), F32)
        for f in range(n_frames):
            dp = dot(vb[tokens(f), :], gb[cols, :], NT)
            e = jnp.exp(ebuf[tokens(f), cols] - top)
            ebuf[tokens(f), cols] = e
            dpb[tokens(f), cols] = dp
            total += jnp.sum(e, axis=0, keepdims=True)
            dotted += jnp.sum(e * dp, axis=0, keepdims=True)
        gst[g, 0:1, cols] = top
        gst[g, 1:2, cols] = total
        gst[g, 2:3, cols] = dotted

    def s_copy(zb, z_to, z_from, peer):
        cols = m128(zb, ZB)
        return remote(stat.at[:, cols], stin.at[z_from, :, cols], ss.at[zb, z_to], sr.at[zb, z_from], peer)

    def plane_totals(zb):
        cols = m128(zb, ZB)
        top = gst[0, 0:1, cols]
        for g in range(1, G):
            top = jnp.maximum(top, gst[g, 0:1, cols])
        total = jnp.zeros((1, ZB), F32)
        dotted = jnp.zeros((1, ZB), F32)
        for g in range(G):
            w = jnp.exp(gst[g, 0:1, cols] - top)
            total += w * gst[g, 1:2, cols]
            dotted += w * gst[g, 2:3, cols]
        stat[0:1, cols] = top
        stat[1:2, cols] = total
        stat[2:3, cols] = dotted
        for d in range(1, NZ):
            send(s_copy(zb, far(d)[0], z, far(d)[2]))

    def landed(s):
        b = band(s)
        x_copy(0, b, x, near(1)[0], me).wait_recv()
        send(pass_copy(b, near(1)[0], near(2)[1]))
        if s < NZ // 2:
            send(x_copy(1, band(s + NZ // 2), x, j, near(2)[1]))
        send(f_copy(0, b, True))

    have_g, have_z = {0}, set()

    def arrive(k):
        zq_each(lambda c: c.start(), band(NZ - 1 - k), True)

    def block(d, k):
        zb = band(NZ - 1 - k)
        if d not in have_g:
            have_g.add(d)
            for c in k_copy(d, j, near(d)[0], me):
                c.wait_recv()
        if k not in have_z:
            have_z.add(k)
            if k:
                pl.when(jnp.logical_not(inner))(lambda: arrive(k))
            for raw, buf in ((qraw, qb), (graw, gb)):
                for m in range(M):
                    buf[m128(zb * M + m, RZ), :] = raw[m128(zb, RZ), m * D:(m + 1) * D]
        totals(j ^ d, zb)

    block(0, 0)
    block(1, 0)

    @pl.when(inner)
    def _():
        arrive(1)
        arrive(2)
    for d, k in ((2, 0), (0, 1), (1, 1), (2, 1)):
        block(d, k)

    @pl.when(inner)
    def _():
        arrive(3)
    block(3, 0)
    plane_totals(band(NZ - 1))
    block(3, 1)
    plane_totals(band(NZ - 2))
    for k in range(2, NZ):
        for d in range(G):
            block(d, k)
        plane_totals(band(NZ - 1 - k))
        if k < NZ - 1:
            landed(k - 2)

    CH = NK // NC

    def kv_copy(c, peer):
        at = m128(c, CH)
        return remote(kv.at[0, at], kv.at[1, at], kvs.at[c], kvr.at[c], peer)

    def d_copy(z_to, z_from):
        return remote(dqs.at[m128(z_to, RZ)], dqin.at[z_from], ds.at[z_to], dr.at[z_from], z_to * G + j)

    def coefs(zb):
        cols = m128(zb, ZB)
        for d in range(1, NZ):
            s_copy(zb, z, far(d)[1], me).wait_recv()
        top = stat[0:1, cols]
        for d in range(1, NZ):
            top = jnp.maximum(top, stin[far(d)[1], 0:1, cols])
        w = jnp.exp(stat[0:1, cols] - top)
        total, dotted = w * stat[1:2, cols], w * stat[2:3, cols]
        for d in range(1, NZ):
            i = far(d)[1]
            w = jnp.exp(stin[i, 0:1, cols] - top)
            total += w * stin[i, 1:2, cols]
            dotted += w * stin[i, 2:3, cols]
        for g in range(G):
            coef[g:g + 1, cols] = jnp.exp(gst[g, 0:1, cols] - top) / total
        coef[G:G + 1, cols] = dotted / total

    brim = jnp.where(2 * z < NZ, 0, NZ - 1)
    core_z = jnp.where(2 * z < NZ, 1, NZ - 2)

    def grads(n, zb):
        cols = m128(zb, ZB)
        coefs(zb)
        dqt[...] = jnp.zeros_like(dqt)

        @pl.loop(0, NC)
        def _(c):
            w, off = coef[pl.ds(c, 1), cols], coef[G:G + 1, cols]
            part_q = None
            for i in range(CH // FR):
                at, tok = pl.ds(i * FR, FR), m128(c * (CH // FR) + i, FR)
                p = ebuf[tok, cols] * w
                t = (p * (dpb[tok, cols] - off)).astype(BF16)
                dv = dot(p.astype(BF16), gb[cols, :])
                dk = dot(t, qb[cols, :])
                dq = dot(ktb[:, tok], t)
                part_q = dq if part_q is None else part_q + dq
                if n:
                    dk += tmp[c, at, 0:D]
                    dv += tmp[c, at, D:2 * D]
                if n < NZ - 1:
                    tmp[c, at, 0:D] = dk
                    tmp[c, at, D:2 * D] = dv
                else:
                    kv[0, tok, 0:D] = (scale * dk).astype(BF16)
                    kv[0, tok, D:2 * D] = dv.astype(BF16)
            dqt[...] += part_q
            if n == NZ - 1:
                kv_copy(c, near(1)[1]).start()
        for i in range(ZB // D):
            t = (scale * dqt[:, pl.ds(i * D, D)].T).astype(BF16)
            for k in range(D // RZ):
                m = i * (D // RZ) + k
                dqs[m128(zb, RZ), pl.ds(m * D, D)] = t[k * RZ:(k + 1) * RZ, :]

        @pl.when(zb != z)
        def _():
            d_copy(zb, z).start()

    for f in range(NK // FR):
        ktb[:, pl.ds(f * FR, FR)] = kb[pl.ds(f * FR, FR), :].astype(F32).T.astype(BF16)
    grads(0, NZ - 1 - core_z)
    landed(NZ - 3)
    grads(1, core_z)
    grads(2, NZ - 1 - brim)
    landed(NZ - 2)
    grads(3, brim)
    HW = JW // 2

    def half(u):
        return pl.ds(u * HW, HW)

    def a_copy(kind, u, z_to, z_from):
        here = dqall.at[j, m128(z_from, RZ), half(u)]
        return remote(here, here, as_.at[kind, u, z_to], ar.at[u, z_from], z_to * G + j)

    def a_own(u, act):
        @pl.when(inner)
        def _():
            for d in range(1, NZ):
                act(a_copy(0, u, far(d)[0], z))

        @pl.when(jnp.logical_not(inner))
        def _():
            act(a_copy(0, u, jnp.where(low, NZ - 2, 1), z))

    def a_onward(u, act):
        act(a_copy(1, u, NZ - 1 - z, brim))
        act(a_copy(1, u, NZ - 1 - brim, brim))

    def y_copy(u, d, j_from, peer, kind):
        here = dqall.at[j_from, :, half(u)]
        return remote(here, here, ys.at[kind, u], yr.at[kind, u], peer)

    landed(NZ - 1)
    for c in local_x:
        c.wait()

    def c_copy(side, b, h, i, peer):
        at = m128(i, FB)
        return remote(part.at[h, b, at], rin.at[side, b, h, at], cs.at[b, h, i], cr.at[side, b, h, i], peer)

    def weigh(s, h):
        for i in range(2):
            tmp[h * NZ + s, pl.ds(i * FB, FB), :] = dot(vis[band(s), :, i * FB:(i + 1) * FB], kv[h], TN)

    def gather(s):
        b = band(s)
        x_copy(1, b, x, near(2)[0], me).wait_recv()
        send(f_copy(1, b, True))
        pass_copy(b, near(3)[0], me).wait_recv()
        send(f_copy(2, b, True))
        for kind in range(3):
            f_copy(kind, b, False).wait_recv()

    def hop(s):
        b = band(s)
        side = (b < z).astype(jnp.int32)
        return b, side, jnp.where(b > z, low, high), (z + 1 - 2 * side) * G + j

    def first(s, h):
        weigh(s, h)
        b, side, fed, peer = hop(s)

        @pl.when(jnp.logical_not(fed))
        def _():
            for i in (1 - y, y):
                at = m128(i, FB)
                part[h, b, at] = tmp[h * NZ + s, at].astype(BF16)
                c_copy(side, b, h, i, peer).start()

    def later(s, h):
        b, side, fed, peer = hop(s)

        @pl.when(fed)
        def _():
            for i in (1 - y, y):
                at = m128(i, FB)
                c_copy(side, b, h, i, me).wait_recv()
                part[h, b, at] = (tmp[h * NZ + s, at] + rin[side, b, h, at].astype(F32)).astype(BF16)
                c_copy(side, b, h, i, peer).start()

    def e_copy(h, peer):
        return remote(ybs.at[h], ybr.at[h], es.at[h], er.at[h], peer)

    outs = []

    def settle(head, slot, grad):
        cols = m128(head, D)
        for a, out in enumerate((kw_out, vw_out)):
            wres[a, :, cols] = grad[:, a * D:(a + 1) * D]
            c = pltpu.make_async_copy(wres.at[a, :, cols], out.at[:, cols], ws.at[a, slot])
            c.start()
            outs.append(c)

    def finish(h):
        own = h * NZ + NZ - 1
        for i in (1 - y, y):
            at = m128(i, FB)
            for side, there in ((0, low), (1, high)):
                @pl.when(there)
                def _():
                    c_copy(side, z, h, i, me).wait_recv()
                    tmp[own, at] += rin[side, z, h, at].astype(F32)
            if i is y:
                settle(j ^ h, h, tmp[own, at])
            else:
                ybs[h] = tmp[own, at].astype(BF16)
                send(e_copy(h, near(2)[1]))

    def summed_dq():
        mine = dqs[m128(z, RZ), :].astype(F32)
        for d in range(1, NZ):
            d_copy(z, far(d)[1]).wait_recv()
            mine += dqin[far(d)[1]].astype(F32)
        dqall[j, m128(z, RZ), :] = mine.astype(BF16)
        for u in range(2):
            a_own(u, lambda c: c.start())

    def relay_dq(u):
        @pl.when(inner)
        def _():
            a_copy(0, u, z, brim).wait_recv()
            a_onward(u, lambda c: c.start())

    def shared_dq(u):
        for d in range(1, NZ):
            b = far(d)[1]

            @pl.when(jnp.logical_not(inner) | (b != brim))
            def _():
                a_copy(0, u, z, b).wait_recv()
        send(y_copy(u, 1, j, near(1)[1], 0))
        send(y_copy(u, 2, j, near(2)[1], 1))

    gather(0)
    first(0, 0)
    summed_dq()
    gather(1)
    first(1, 0)
    later(0, 0)
    relay_dq(0)
    relay_dq(1)
    gather(2)
    first(2, 0)
    later(1, 0)
    gather(3)
    for c in range(NC):
        kv_copy(c, me).wait_recv()
    first(0, 1)
    shared_dq(0)
    shared_dq(1)
    for s in range(1, NZ - 1):
        first(s, 1)
    later(2, 0)
    weigh(3, 0)
    weigh(3, 1)
    y_copy(0, 1, near(1)[0], me, 0).wait_recv()
    send(y_copy(0, 2, near(1)[0], near(2)[1], 2))
    later(0, 1)
    y_copy(1, 2, near(2)[0], me, 1).wait_recv()
    send(y_copy(1, 1, near(2)[0], near(1)[1], 2))
    later(1, 1)
    later(2, 1)
    finish(0)

    def put(i):
        c = pltpu.make_async_copy(dqall.at[j ^ i], q_out.at[:, m128(j ^ i, JW)], loc.at[i])
        c.start()
        outs.append(c)

    put(0)
    y_copy(1, 1, near(1)[0], me, 0).wait_recv()
    put(1)
    y_copy(0, 2, near(2)[0], me, 1).wait_recv()
    put(2)
    y_copy(0, 2, near(3)[0], me, 2).wait_recv()
    y_copy(1, 1, near(3)[0], me, 2).wait_recv()
    put(3)
    finish(1)
    for h in range(2):
        e_copy(h, me).wait_recv()
        settle(j ^ (2 + h), 2 + h, ybr[h].astype(F32))
    for c in outs:
        c.wait()
    for c in sends:
        c.wait_send()
    for k in range(NZ):
        zq_each(lambda c: c.wait_send(), band(NZ - 1 - k), False)
    for u in range(2):
        a_own(u, lambda c: c.wait_send())
        pl.when(inner)(lambda: a_onward(u, lambda c: c.wait_send()))
    for s in range(NZ - 1):
        b, side, fed, peer = hop(s)
        for h in range(2):
            for i in range(2):
                c_copy(side, b, h, i, peer).wait_send()
    for d in range(1, NZ):
        d_copy(far(d)[0], z).wait_send()
    for c in range(NC):
        kv_copy(c, near(1)[1]).wait_send()


def deliver_kernel(parts, *refs):
    n = len(parts)
    srcs, dsts, bufs, ins, outs = refs[:n], refs[n:2 * n], refs[2 * n:3 * n], refs[3 * n], refs[3 * n + 1]
    moves, k = [], 0
    for src, dst, buf, p in zip(srcs, dsts, bufs, parts):
        step = src.shape[0] // p
        for i in range(p):
            at = pl.ds(i * step, step)
            moves.append((pltpu.make_async_copy(src.at[at], buf.at[at], ins.at[k]),
                          pltpu.make_async_copy(buf.at[at], dst.at[at], outs.at[k])))
            k += 1
    for a, _ in moves:
        a.start()
    for a, b in moves:
        a.wait()
        b.start()
    for _, b in moves:
        b.wait()


def deliver(*arrays):
    parts = [4, 1, 1]
    anyspec = pl.BlockSpec(memory_space=pl.ANY)
    return pl.pallas_call(
        functools.partial(deliver_kernel, parts),
        out_shape=[jax.ShapeDtypeStruct(a.shape, a.dtype) for a in arrays],
        in_specs=[anyspec] * len(arrays),
        out_specs=[anyspec] * len(arrays),
        scratch_shapes=[pltpu.VMEM(a.shape, a.dtype) for a in arrays]
        + [pltpu.SemaphoreType.DMA((sum(parts),)), pltpu.SemaphoreType.DMA((sum(parts),))],
        compiler_params=pltpu.CompilerParams(vmem_limit_bytes=67043328),
    )(*arrays)


def plane_shards(T, text_queries, text_grads, vision_keys, video_value_rows, vision, lengths, frame_range):
    R, QW = text_queries.shape
    rows, kv_width = vision_keys.shape
    G = kv_width // HEAD_WIDTH
    M = QW // kv_width
    NZ = T // G
    DW = vision.shape[1]
    FB = DW // T
    NK, RZ, JW = G * rows, G * R, M * HEAD_WIDTH
    NR = T * R * M
    cfg = dict(G=G, NZ=NZ, M=M, R=R, FR=rows // FRAME_DEV, NC=4, rows=rows, NK=NK, NR=NR, JW=JW, FB=FB, RZ=RZ,
               NS=lengths.shape[0])
    anyspec = pl.BlockSpec(memory_space=pl.ANY)
    vm = pl.BlockSpec(memory_space=pltpu.VMEM)
    sm = pl.BlockSpec(memory_space=pltpu.SMEM)
    V = pltpu.VMEM
    D = pltpu.SemaphoreType.DMA
    W2 = 2 * HEAD_WIDTH
    pairs = []
    for a, b in (((2, G),) * 2, ((2, 2, NZ), (2, NZ)), ((2, G),) * 2, ((3, NZ),) * 2, ((3, NZ),) * 2, ((NZ, NZ),) * 2, ((cfg["NC"],),) * 2,
                 ((NZ,),) * 2, ((2, 2, NZ), (2, NZ)), ((3, 2),) * 2, ((NZ, 2, 2), (2, NZ, 2, 2)), ((2,),) * 2):
        pairs += [D(a), D(b)]
    q_grad, kw, vw = pl.pallas_call(
        functools.partial(plane_kernel, cfg),
        out_shape=(
            jax.ShapeDtypeStruct((T * R, QW), BF16),
            jax.ShapeDtypeStruct((FB, kv_width), F32),
            jax.ShapeDtypeStruct((FB, kv_width), F32),
        ),
        in_specs=[anyspec] * 5 + [sm] * 2,
        out_specs=(anyspec,) * 3,
        scratch_shapes=[
            V((T * R, JW), BF16), V((T * R, JW), BF16),
            V((NR, HEAD_WIDTH), BF16), V((NR, HEAD_WIDTH), BF16),
            V((NK, HEAD_WIDTH), BF16), V((NK, HEAD_WIDTH), BF16),
            V((NZ, NK, 2 * FB), BF16),
            V((NK, NR), F32), V((NK, NR), F32),
            V((8, NR), F32), V((NZ, 8, NR), F32), V((8, NR), F32), V((8, NR), jnp.int32),
            V((2, NK, W2), BF16),
            V((HEAD_WIDTH, M * RZ), F32), V((T * R, JW), BF16),
            V((NZ, RZ, JW), BF16), V((G, T * R, JW), BF16),
            V((G, 8, NR), F32), V((HEAD_WIDTH, NK), BF16),
            V((2, FB, kv_width), F32), D((2, 4)),
            V((2 * NZ, 2 * FB, W2), F32), V((2, NZ, 2 * FB, W2), BF16), V((2, NZ, 2, 2 * FB, W2), BF16),
            V((2, FB, W2), BF16), V((2, FB, W2), BF16),
            D((4,)), D((NZ, 2)),
        ] + pairs,
        compiler_params=pltpu.CompilerParams(
            collective_id=0, has_side_effects=True, vmem_limit_bytes=67043328
        ),
    )(text_queries, text_grads, vision_keys, video_value_rows, vision, lengths, frame_range.T)
    return deliver(q_grad, kw, vw)


def solution(mesh):
    return jax.shard_map(
        functools.partial(shards, mesh.shape["tok"], mesh.shape["head"]),
        mesh=mesh,
        in_specs=(
            P("tok", "head"),
            P("tok", "head"),
            P("tok", "head"),
            P("tok", "head"),
            P("tok", None),
            P(),
            P(),
        ),
        out_specs=(P(None, "head"), P("tok", "head"), P("tok", "head")),
        check_vma=False,
    )
```

```python
import functools

import jax
import jax.numpy as jnp
from jax import lax
from jax.experimental import pallas as pl
from jax.experimental.pallas import tpu as pltpu
from jax.sharding import PartitionSpec as P

HEAD_WIDTH = 128
FRAME_DEV = 4
NEG_FILL = -1e30
NT = (((1,), (1,)), ((), ()))
TN = (((0,), (0,)), ((), ()))
F32 = jnp.float32
BF16 = jnp.bfloat16


def dot(a, b, dims=(((1,), (0,)), ((), ()))):
    return lax.dot_general(a, b, dims, preferred_element_type=F32)


def kernel(cfg, q_in, g_in, k_in, v_in, x_in, bounds, q_out, kw_out, vw_out,
           qb, gb, kb, vb, vis, ebuf, dpb, stat, stin, coef, kv, dqt, dqs, dqin, dqall, part, rsb,
           loc, qs, qr, gs, gr, ks, kr, vs, vr, xs, xr, ss, sr, kvs, kvr, ds, dr, as_, ar, ys, yr, rs, rr, fs, fr):
    T, G, NZ = cfg["T"], cfg["G"], cfg["NZ"]
    blk, rows, NK, NR, FR = cfg["blk"], cfg["rows"], cfg["NK"], cfg["NR"], cfg["FR"]
    W, NV, FB = cfg["W"], cfg["NV"], cfg["FB"]
    H = cfg["H"]
    RB = cfg["RB"]
    scale = HEAD_WIDTH ** (-0.5)
    me = lax.axis_index("tok")
    z, j0 = me // G, me % G

    def remote(src, dst, s, r, peer):
        return pltpu.make_async_remote_copy(
            src_ref=src, dst_ref=dst, send_sem=s, recv_sem=r,
            device_id={"tok": peer}, device_id_type=pl.DeviceIdType.MESH)

    def m128(i, n):
        return pl.ds(pl.multiple_of(i * n, n), n)

    barrier = pltpu.get_barrier_semaphore()
    for d in range(1, T):
        pl.semaphore_signal(barrier, inc=1, device_id={"tok": lax.rem(me + d, T)}, device_id_type=pl.DeviceIdType.MESH)
    twin = lax.axis_index("head")
    if H > 1:
        twin = 1 - twin
        pl.semaphore_signal(barrier, inc=1, device_id={"head": twin}, device_id_type=pl.DeviceIdType.MESH)
    pl.semaphore_wait(barrier, T - 1 + (H > 1))

    def tpeer(d):
        return lax.rem(me + d, T), lax.rem(me + T - d, T)

    def gpeer(d):
        a, b = (j0 ^ d, j0 ^ d) if G & (G - 1) == 0 else (lax.rem(j0 + d, G), lax.rem(j0 + G - d, G))
        return a, b, z * G + a, z * G + b

    def zpeer(d):
        a, b = lax.rem(z + d, NZ), lax.rem(z + NZ - d, NZ)
        return a, b, a * G + j0, b * G + j0

    sends = []

    def send(c):
        c.start()
        sends.append(c)

    def q_copy(t_to, t_from):
        return (remote(q_in.at[lax.rem(t_to, G)], qb.at[m128(t_from, blk)], qs.at[t_to], qr.at[t_from], t_to),
                remote(g_in.at[lax.rem(t_to, G)], gb.at[m128(t_from, blk)], gs.at[t_to], gr.at[t_from], t_to))

    def k_copy(j_to, j_from, peer):
        return (remote(k_in.at[:, m128(j_to, 128)], kb.at[m128(j_from, rows)], ks.at[j_to], kr.at[j_from], peer),
                remote(v_in.at[:, m128(j_to, 128)], vb.at[m128(j_from, rows)], vs.at[j_to], vr.at[j_from], peer))

    WH = W // H
    half = lax.axis_index("head") * WH if H > 1 else 0

    def x_copy(b, j_to, j_from, peer):
        cols = pl.ds(pl.multiple_of((b * G + j_to) * W + half, WH), WH)
        dst = vis.at[b, m128(j_from, rows), pl.ds(pl.multiple_of(half, WH), WH)]
        return remote(x_in.at[:, cols], dst, xs.at[j_to, b], xr.at[j_from, b], peer)

    def f_copy(b, j_from, mine):
        at = half if mine else WH - half
        here = vis.at[b, m128(j_from, rows), pl.ds(pl.multiple_of(at, WH), WH)]
        return pltpu.make_async_remote_copy(
            src_ref=here, dst_ref=here, send_sem=fs.at[j_from, b], recv_sem=fr.at[j_from, b],
            device_id={"head": twin}, device_id_type=pl.DeviceIdType.MESH)

    local = [
        pltpu.make_async_copy(q_in.at[j0], qb.at[m128(me, blk)], loc.at[0]),
        pltpu.make_async_copy(g_in.at[j0], gb.at[m128(me, blk)], loc.at[1]),
        pltpu.make_async_copy(k_in.at[:, m128(j0, 128)], kb.at[m128(j0, rows)], loc.at[2]),
        pltpu.make_async_copy(v_in.at[:, m128(j0, 128)], vb.at[m128(j0, rows)], loc.at[3]),
    ]
    local_x = [pltpu.make_async_copy(x_in.at[:, m128(b * G + j0, W)], vis.at[b, m128(j0, rows)], loc.at[4 + b]) for b in range(NV)]
    for c in local:
        c.start()
    def q_sends(zd):
        a, _, _, _ = zpeer(zd)
        for i in range(G):
            to = a * G + (lax.rem(j0 + i, G) if zd else gpeer(i)[0])
            if zd or i:
                for c in q_copy(to, me):
                    send(c)

    q_sends(0)
    for d in range(1, G):
        a, _, peer, _ = gpeer(d)
        for c in k_copy(a, j0, peer):
            send(c)
    for d in range(1, NZ):
        q_sends(d)
    for c in local_x:
        c.start()
    for c in local:
        c.wait()
    for d in range(1, G):
        _, b, _, _ = gpeer(d)
        for c in k_copy(j0, b, me):
            c.wait_recv()

    def q_wait(zd):
        _, b, _, _ = zpeer(zd)
        for i in range(G):
            if zd or i:
                frm = b * G + (i if zd else gpeer(i)[1])
                for c in q_copy(me, frm):
                    c.wait_recv()

    n_frames = NK // FR
    frame0 = z * n_frames
    stat[0:1, :] = jnp.full((1, NR), NEG_FILL, F32)
    stat[1:8, :] = jnp.zeros((7, NR), F32)

    def totals(cols, width):
        first, end = bounds[0:1, cols], bounds[1:2, cols]
        UN = 2 if n_frames % 2 == 0 else 1

        def scored(i, top):
            for u in range(UN):
                f = i * UN + u
                ok = (first <= frame0 + f) & (frame0 + f < end)
                s = jnp.where(ok, dot(kb[m128(f, FR), :], qb[cols, :], NT) * scale, NEG_FILL)
                ebuf[m128(f, FR), cols] = s
                top = jnp.maximum(top, jnp.max(s, axis=0, keepdims=True))
            return top

        top = lax.fori_loop(0, n_frames // UN, scored, jnp.full((1, width), NEG_FILL, F32))

        def summed(i, carry):
            total, dotted = carry
            for u in range(UN):
                f = i * UN + u
                dp = dot(vb[m128(f, FR), :], gb[cols, :], NT)
                e = jnp.exp(ebuf[m128(f, FR), cols] - top)
                ebuf[m128(f, FR), cols] = e
                dpb[m128(f, FR), cols] = dp
                total += jnp.sum(e, axis=0, keepdims=True)
                dotted += jnp.sum(e * dp, axis=0, keepdims=True)
            return total, dotted

        zero = jnp.zeros((1, width), F32)
        total, dotted = lax.fori_loop(0, n_frames // UN, summed, (zero, zero))
        stat[0:1, cols] = top
        stat[1:2, cols] = total
        stat[2:3, cols] = dotted

    def x_sends():
        for d in range(1, G):
            a, _, peer, _ = gpeer(d)
            for b in range(NV):
                send(x_copy(b, a, j0, peer))

    by_z = (NR // NZ) % 128 == 0
    for d in range(NZ):
        q_wait(d)
        if d == NZ - 1:
            x_sends()
        if by_z:
            totals(m128(zpeer(d)[1], NR // NZ), NR // NZ)
    if not by_z:
        for r in range(0, NR, RB):
            totals(pl.ds(r, RB), RB)

    def s_copy(z_to, z_from, peer):
        return remote(stat, stin.at[z_from], ss.at[z_to], sr.at[z_from], peer)

    for d in range(1, NZ):
        a, _, peer, _ = zpeer(d)
        send(s_copy(a, z, peer))
    stin[z] = stat[...]
    for d in range(1, NZ):
        _, b, _, _ = zpeer(d)
        s_copy(z, b, me).wait_recv()
    top = stat[0:1, :]
    for i in range(NZ):
        top = jnp.maximum(top, stin[i, 0:1, :])
    total = jnp.zeros((1, NR), F32)
    dotted = jnp.zeros((1, NR), F32)
    for i in range(NZ):
        w = jnp.exp(stin[i, 0:1, :] - top)
        total += w * stin[i, 1:2, :]
        dotted += w * stin[i, 2:3, :]
    coef[0:1, :] = jnp.exp(stat[0:1, :] - top) / total
    coef[1:2, :] = dotted / total
    dqt[...] = jnp.zeros_like(dqt)

    NC = cfg["NC"]
    CH = NK // NC

    def kv_copy(c, j_to, j_from, peer):
        here = kv.at[j_from, pl.ds(c * CH, CH)]
        return remote(here, here, kvs.at[j_to, c], kvr.at[j_from, c], peer)

    for c in range(NC):
        @pl.loop(c * (CH // FR), (c + 1) * (CH // FR))
        def _(f):
            kt = kb[m128(f, FR), :].astype(F32).T.astype(BF16)
            dk = jnp.zeros((FR, HEAD_WIDTH), F32)
            dv = jnp.zeros((FR, HEAD_WIDTH), F32)
            for r in range(0, NR, RB):
                cols = pl.ds(r, RB)
                p = ebuf[m128(f, FR), cols] * coef[0:1, cols]
                t = (p * (dpb[m128(f, FR), cols] - coef[1:2, cols])).astype(BF16)
                dv += dot(p.astype(BF16), gb[cols, :])
                dk += dot(t, qb[cols, :])
                dqt[:, cols] += dot(kt, t)
            kv[j0, m128(f, FR), 0:HEAD_WIDTH] = (scale * dk).astype(BF16)
            kv[j0, m128(f, FR), HEAD_WIDTH:2 * HEAD_WIDTH] = dv.astype(BF16)

        for d in range(1, G - 1):
            a, _, peer, _ = gpeer(d)
            kv_copy(c, a, j0, peer).start()
        if H > 1 and c == NC // 2:
            for d in range(1, G):
                _, b, _, _ = gpeer(d)
                for i in range(NV):
                    x_copy(i, j0, b, me).wait_recv()
                    send(f_copy(i, b, True))

    for r in range(0, NR, 128):
        dqs[pl.ds(r, 128), :] = (scale * dqt[:, pl.ds(r, 128)].T).astype(BF16)
    QR = NR // NZ

    def d_copy(z_to, z_from, peer):
        return remote(dqs.at[m128(z_to, QR)], dqin.at[z_from], ds.at[z_to], dr.at[z_from], peer)

    def a_copy(z_to, z_from, peer):
        here = dqall.at[j0, m128(z_from, QR)]
        return remote(here, here, as_.at[z_to], ar.at[z_from], peer)

    def y_copy(j_to, j_from, peer):
        here = dqall.at[j_from]
        return remote(here, here, ys.at[j_to], yr.at[j_from], peer)

    def r_copy(j, z_to, z_from, peer):
        return remote(part.at[j, m128(z_to, FB)], rsb.at[z_from, j], rs.at[j, z_to], rr.at[j, z_from], peer)

    for d in range(1, NZ):
        a, _, peer, _ = zpeer(d)
        send(d_copy(a, z, peer))
    for c in local_x:
        c.wait()
    for d in range(1, G):
        _, b, _, _ = gpeer(d)
        for i in range(NV):
            (f_copy(i, b, False) if H > 1 else x_copy(i, j0, b, me)).wait_recv()

    def weigh(j):
        @pl.loop(0, NV)
        def _(b):
            part[j, m128(b, W), :] = dot(vis[b], kv[j], TN).astype(BF16)
        for d in range(1, NZ):
            a, _, peer, _ = zpeer(d)
            send(r_copy(j, a, z, peer))

    weigh(j0)
    mine = dqs[m128(z, QR), :].astype(F32)
    for d in range(1, NZ):
        _, b, _, _ = zpeer(d)
        d_copy(z, b, me).wait_recv()
        mine += dqin[b].astype(F32)
    dqall[j0, m128(z, QR), :] = mine.astype(BF16)
    for d in range(1, NZ):
        a, _, peer, _ = zpeer(d)
        send(a_copy(a, z, peer))

    def spread():
        for d in range(1, NZ):
            _, b, _, _ = zpeer(d)
            a_copy(z, b, me).wait_recv()
        for d in range(1, G):
            a, _, peer, _ = gpeer(d)
            send(y_copy(a, j0, peer))

    for d in range(1, G - 1):
        a, _, peer, _ = gpeer(d)
        for c in range(NC):
            kv_copy(c, a, j0, peer).wait_send()
    if G > 1:
        a, _, peer, _ = gpeer(G - 1)
        for c in range(NC):
            send(kv_copy(c, a, j0, peer))
    if G == 1:
        spread()
    for d in range(1, G):
        _, b, _, _ = gpeer(d)
        for c in range(NC):
            kv_copy(c, j0, b, me).wait_recv()
        weigh(b)
        if d == min(2, G - 1):
            spread()
    for d in range(1, G):
        _, b, _, _ = gpeer(d)
        y_copy(j0, b, me).wait_recv()
    out_copy = pltpu.make_async_copy(dqall, q_out, loc.at[0])
    out_copy.start()

    for d in range(1, NZ):
        _, b, _, _ = zpeer(d)
        for j in range(G):
            r_copy(j, z, b, me).wait_recv()
    for j in range(G):
        acc = part[j, m128(z, FB), :].astype(F32)
        for d in range(1, NZ):
            _, b, _, _ = zpeer(d)
            acc += rsb[b, j].astype(F32)
        kw_out[:, pl.ds(j * HEAD_WIDTH, HEAD_WIDTH)] = acc[:, 0:HEAD_WIDTH]
        vw_out[:, pl.ds(j * HEAD_WIDTH, HEAD_WIDTH)] = acc[:, HEAD_WIDTH:]
    out_copy.wait()
    for c in sends:
        c.wait_send()


def shards(T, cores, text_queries, text_grads, vision_keys, video_value_rows, vision, lengths, frame_range):
    R, QW = text_queries.shape
    rows, kv_width = vision_keys.shape
    G = kv_width // HEAD_WIDTH
    if cores == 2 and G == 4 and T == G * G and vision.shape[1] % (T * 128) == 0 and HEAD_WIDTH % (G * R) == 0 and 2 * vision.shape[1] == T * rows:
        return plane_shards(T, text_queries, text_grads, vision_keys, video_value_rows, vision, lengths, frame_range)
    M = QW // kv_width
    NZ = T // G
    DW = vision.shape[1]
    blk, NK, NR = M * R, G * rows, T * M * R
    FB = DW // T
    W = FB if FB % 128 == 0 else 256
    NV = DW // (G * W)
    FR = rows // FRAME_DEV
    NC = 4 if NK >= 16 * FR else 1
    cfg = dict(T=T, G=G, NZ=NZ, blk=blk, rows=rows, NK=NK, NR=NR, FR=FR, W=W, NV=NV, FB=FB, NC=NC, RB=min(NR, 512),
               H=2 if cores == 2 and G > 1 and W % 256 == 0 else 1)

    text_len = R * T
    row_ids = jnp.arange(text_len, dtype=jnp.int32)
    segment_ends = jnp.cumsum(lengths)
    segment = jnp.sum((row_ids[:, None] >= segment_ends[None, :]).astype(jnp.int32), axis=1)
    segment_pick = (
        segment[:, None] == jnp.arange(lengths.shape[0], dtype=jnp.int32)[None, :]
    ).astype(jnp.int32)
    bounds = jnp.sum(segment_pick[None] * frame_range.T[:, None, :], axis=2)
    bounds = jnp.broadcast_to(bounds.reshape(2, T, 1, R), (2, T, M, R)).reshape(2, NR)

    def split(a):
        return a.reshape(R, G, M, HEAD_WIDTH).transpose(1, 2, 0, 3).reshape(G, blk, HEAD_WIDTH)

    anyspec = pl.BlockSpec(memory_space=pl.ANY)
    vm = pl.BlockSpec(memory_space=pltpu.VMEM)
    V = pltpu.VMEM
    D = pltpu.SemaphoreType.DMA
    sem_pairs = []
    for shape in ((T,), (T,), (G,), (G,), (G, NV), (NZ,), (G, NC), (NZ,), (NZ,), (G,), (G, NZ), (G, NV)):
        sem_pairs += [D(shape), D(shape)]
    q_grad, kw, vw = pl.pallas_call(
        functools.partial(kernel, cfg),
        out_shape=(
            jax.ShapeDtypeStruct((G, NR, HEAD_WIDTH), BF16),
            jax.ShapeDtypeStruct((FB, kv_width), F32),
            jax.ShapeDtypeStruct((FB, kv_width), F32),
        ),
        in_specs=[anyspec] * 5 + [vm],
        out_specs=(anyspec, vm, vm),
        scratch_shapes=[
            V((NR, HEAD_WIDTH), BF16), V((NR, HEAD_WIDTH), BF16),
            V((NK, HEAD_WIDTH), BF16), V((NK, HEAD_WIDTH), BF16),
            V((NV, NK, W), BF16),
            V((NK, NR), F32), V((NK, NR), F32),
            V((8, NR), F32), V((NZ, 8, NR), F32), V((8, NR), F32),
            V((G, NK, 2 * HEAD_WIDTH), BF16),
            V((HEAD_WIDTH, NR), F32), V((NR, HEAD_WIDTH), BF16),
            V((NZ, NR // NZ, HEAD_WIDTH), BF16), V((G, NR, HEAD_WIDTH), BF16),
            V((G, DW // G, 2 * HEAD_WIDTH), BF16),
            V((NZ, G, FB, 2 * HEAD_WIDTH), BF16),
            D((4 + NV,)),
        ] + sem_pairs,
        compiler_params=pltpu.CompilerParams(
            collective_id=0, has_side_effects=True, vmem_limit_bytes=67043328
        ),
    )(split(text_queries), split(text_grads), vision_keys, video_value_rows, vision, bounds)
    q_grad = q_grad.reshape(G, T, M, R, HEAD_WIDTH).transpose(1, 3, 0, 2, 4).reshape(text_len, QW)
    return q_grad, kw, vw


def plane_kernel(cfg, q_in, g_in, k_in, v_in, x_in, lens_in, frames_in, q_out, kw_out, vw_out,
                 qraw, graw, qb, gb, kb, vb, vis, ebuf, dpb, stat, stin, coef, lim, kv, dqt, dqs, dqin, dqall,
                 gst, ktb, wres, ws, lens, frames, tmp, part, rin, ybs, ybr, loc, lx, qs, qr, zs, zr, ks, kr, xs, xr, fs, fr, ss, sr, kvs, kvr,
                 ds, dr, as_, ar, ys, yr, cs, cr, es, er):
    G, NZ, M, R, FR, NC = cfg["G"], cfg["NZ"], cfg["M"], cfg["R"], cfg["FR"], cfg["NC"]
    rows, NK, NR, JW, FB, RZ = cfg["rows"], cfg["NK"], cfg["NR"], cfg["JW"], cfg["FB"], cfg["RZ"]
    D = HEAD_WIDTH
    ZB = M * RZ
    scale = D ** (-0.5)
    me = lax.axis_index("tok")
    core = lax.axis_index("head")
    z, j = me // G, me % G
    y, x = j // 2, j % 2

    def m128(i, n):
        return pl.ds(pl.multiple_of(i * n, n), n)

    def remote(src, dst, s, r, peer):
        return pltpu.make_async_remote_copy(
            src_ref=src, dst_ref=dst, send_sem=s, recv_sem=r,
            device_id={"tok": peer}, device_id_type=pl.DeviceIdType.MESH)

    def near(d):
        return j ^ d, z * G + (j ^ d)

    def far(d):
        a, b = lax.rem(z + d, NZ), lax.rem(z + NZ - d, NZ)
        return a, b, a * G + j, b * G + j

    mirror = 2 * z > NZ - 1
    zz = jnp.where(mirror, NZ - 1 - z, z)

    def band(s):
        u = s - (NZ - 1 - 2 * zz)
        k, odd = u // 2, u % 2
        b = jnp.where(u < 0, NZ - 1 - s, k + odd * (2 * zz - 2 * k))
        return jnp.where(mirror, NZ - 1 - b, b)

    barrier = pltpu.get_barrier_semaphore()
    for d in range(1, G):
        pl.semaphore_signal(barrier, inc=1, device_id={"tok": near(d)[1]}, device_id_type=pl.DeviceIdType.MESH)
    for d in range(1, NZ):
        pl.semaphore_signal(barrier, inc=1, device_id={"tok": far(d)[2]}, device_id_type=pl.DeviceIdType.MESH)
    pl.semaphore_signal(barrier, inc=1, device_id={"head": 1 - core}, device_id_type=pl.DeviceIdType.MESH)
    pl.semaphore_wait(barrier, G + NZ - 1)

    sends = []

    def send(c):
        c.start()
        sends.append(c)

    def own_rows(t):
        return m128(t, R)

    def q_copy(d, t_from, peer, j_to):
        cols = m128(j_to, JW)
        return (remote(q_in.at[:, cols], qraw.at[own_rows(t_from)], qs.at[0, d], qr.at[0, d], peer),
                remote(g_in.at[:, cols], graw.at[own_rows(t_from)], qs.at[1, d], qr.at[1, d], peer))

    low, high = z > 0, z < NZ - 1
    inner = low & high

    def zq_copy(side, a, b):
        here = (qraw, graw)[a].at[m128(b, RZ)]
        return remote(here, here, zs.at[side, a, b], zr.at[a, b], (z + 1 - 2 * side) * G + j)

    def zq_each(act, b, into, which=(0, 1)):
        for a in which:
            if into:
                zq_copy(0, a, b).wait_recv()

            @pl.when(high & (b <= z))
            def _():
                act(zq_copy(0, a, b))

            @pl.when(low & (b >= z))
            def _():
                act(zq_copy(1, a, b))

    def k_copy(d, j_to, j_from, peer):
        return (remote(k_in.at[:, m128(j_to, D)], kb.at[m128(j_from, rows)], ks.at[0, d], kr.at[0, d], peer),
                remote(v_in.at[:, m128(j_to, D)], vb.at[m128(j_from, rows)], ks.at[1, d], kr.at[1, d], peer))

    def lane_half(mine):
        return m128(core if mine else 1 - core, FB)

    def x_copy(kind, b, x_to, j_from, peer):
        cols = m128(b * G + core * 2 + x_to, FB)
        dst = vis.at[b, m128(j_from, rows), lane_half(True)]
        return remote(x_in.at[:, cols], dst, xs.at[kind, b], xr.at[kind, b], peer)

    def pass_copy(b, j_from, peer):
        here = vis.at[b, m128(j_from, rows), lane_half(True)]
        return remote(here, here, xs.at[2, b], xr.at[2, b], peer)

    def f_copy(kind, b, mine):
        here = vis.at[b, m128(j ^ (kind + 1), rows), lane_half(mine)]
        return pltpu.make_async_remote_copy(
            src_ref=here, dst_ref=here, send_sem=fs.at[kind, b], recv_sem=fr.at[kind, b],
            device_id={"head": 1 - core}, device_id_type=pl.DeviceIdType.MESH)

    local = [
        pltpu.make_async_copy(q_in.at[:, m128(j, JW)], qraw.at[own_rows(me)], loc.at[0]),
        pltpu.make_async_copy(g_in.at[:, m128(j, JW)], graw.at[own_rows(me)], loc.at[1]),
        pltpu.make_async_copy(k_in.at[:, m128(j, D)], kb.at[m128(j, rows)], loc.at[2]),
        pltpu.make_async_copy(v_in.at[:, m128(j, D)], vb.at[m128(j, rows)], loc.at[3]),
        pltpu.make_async_copy(lens_in, lens, loc.at[4]),
        pltpu.make_async_copy(frames_in, frames, loc.at[5]),
    ]
    for c in local:
        c.start()
    for d in range(G - 1, 0, -1):
        for c in q_copy(d, me, near(d)[1], near(d)[0]):
            send(c)
    for d in range(1, G):
        for c in k_copy(d, near(d)[0], j, near(d)[1]):
            send(c)
    local_x = []
    for b in range(NZ):
        for h in range(2):
            local_x.append(pltpu.make_async_copy(
                x_in.at[:, m128(b * G + 2 * h + x, FB)], vis.at[b, m128(j, rows), pl.ds(h * FB, FB)], lx.at[b, h]))

    for c in local[4:]:
        c.wait()
    col = lax.broadcasted_iota(jnp.int32, (1, NR), 1)
    text = (col // ZB) * RZ + col % RZ
    seg = jnp.zeros((1, NR), jnp.int32)
    end = jnp.int32(0)
    NS = cfg["NS"]
    for i in range(NS):
        end = end + lens[i]
        seg += (text >= end).astype(jnp.int32)
    first, last = jnp.zeros((1, NR), jnp.int32), jnp.zeros((1, NR), jnp.int32)
    for i in range(NS):
        first = jnp.where(seg == i, frames[0, i], first)
        last = jnp.where(seg == i, frames[1, i], last)
    lim[0:1, :] = first
    lim[1:2, :] = last
    stat[0:8, :] = jnp.zeros((8, NR), F32)

    for c in local[:2]:
        c.wait()
    for d in range(1, G):
        for c in q_copy(d, z * G + near(d)[0], me, j):
            c.wait_recv()
    zq_each(lambda c: c.start(), z, False)
    for s in range(NZ):
        send(x_copy(0, band(s), 1 - x, j, near(1)[1]))
        if s < NZ // 2:
            send(x_copy(1, band(s), x, j, near(2)[1]))
    for c in local_x:
        c.start()
    for c in local[2:4]:
        c.wait()

    n_frames = rows // FR

    def tokens(g, f):
        return m128(g * n_frames + f, FR)

    def scored(g, zb):
        cols = m128(zb, ZB)
        lo, hi = lim[0:1, cols], lim[1:2, cols]
        base = z * G * n_frames + g * n_frames
        top = jnp.full((1, ZB), NEG_FILL, F32)
        for f in range(n_frames):
            ok = (lo <= base + f) & (base + f < hi)
            sc = jnp.where(ok, dot(kb[tokens(g, f), :], qb[cols, :], NT) * scale, NEG_FILL)
            ebuf[tokens(g, f), cols] = sc
            top = jnp.maximum(top, jnp.max(sc, axis=0, keepdims=True))
        gst[g, 0:1, cols] = top

    def summed(g, zb):
        cols = m128(zb, ZB)
        top = gst[g, 0:1, cols]
        total = jnp.zeros((1, ZB), F32)
        dotted = jnp.zeros((1, ZB), F32)
        for f in range(n_frames):
            dp = dot(vb[tokens(g, f), :], gb[cols, :], NT)
            e = jnp.exp(ebuf[tokens(g, f), cols] - top)
            ebuf[tokens(g, f), cols] = e
            dpb[tokens(g, f), cols] = dp
            total += jnp.sum(e, axis=0, keepdims=True)
            dotted += jnp.sum(e * dp, axis=0, keepdims=True)
        gst[g, 1:2, cols] = total
        gst[g, 2:3, cols] = dotted

    def s_copy(zb, z_to, z_from, peer):
        cols = m128(zb, ZB)
        return remote(stat.at[:, cols], stin.at[z_from, :, cols], ss.at[zb, z_to], sr.at[zb, z_from], peer)

    def plane_totals(zb):
        cols = m128(zb, ZB)
        top = gst[0, 0:1, cols]
        for g in range(1, G):
            top = jnp.maximum(top, gst[g, 0:1, cols])
        total = jnp.zeros((1, ZB), F32)
        dotted = jnp.zeros((1, ZB), F32)
        for g in range(G):
            w = jnp.exp(gst[g, 0:1, cols] - top)
            total += w * gst[g, 1:2, cols]
            dotted += w * gst[g, 2:3, cols]
        stat[0:1, cols] = top
        stat[1:2, cols] = total
        stat[2:3, cols] = dotted
        for d in range(1, NZ):
            s_copy(zb, far(d)[0], z, far(d)[2]).start()

    def landed(s):
        b = band(s)
        x_copy(0, b, x, near(1)[0], me).wait_recv()
        send(pass_copy(b, near(1)[0], near(2)[1]))
        if s < NZ // 2:
            send(x_copy(1, band(s + NZ // 2), x, j, near(2)[1]))
        send(f_copy(0, b, True))

    have_g, have_z = {0}, set()

    def arrive(k, which=(0, 1)):
        zq_each(lambda c: c.start(), band(NZ - 1 - k), True, which)

    def head_rows(zb, which=(0, 1)):
        for a in which:
            raw, buf = (qraw, graw)[a], (qb, gb)[a]
            for m in range(M):
                buf[m128(zb * M + m, RZ), :] = raw[m128(zb, RZ), m * D:(m + 1) * D]

    def block(d, k):
        zb = band(NZ - 1 - k)
        if d not in have_g:
            have_g.add(d)
            for c in k_copy(d, j, near(d)[0], me):
                c.wait_recv()
        if k not in have_z:
            have_z.add(k)
            if k:
                pl.when(jnp.logical_not(inner))(lambda: arrive(k))
            head_rows(zb)
        scored(j ^ d, zb)
        summed(j ^ d, zb)

    def last_block(k, waits):
        zb = band(NZ - 1 - k)
        for a, work in ((0, scored), (1, summed)):
            if waits:
                arrive(k, (a,))
            head_rows(zb, (a,))
            for d in range(G):
                work(j ^ d, zb)
        plane_totals(zb)

    block(0, 0)
    block(1, 0)

    @pl.when(inner)
    def _():
        arrive(1)
        arrive(2)
    for d, k in ((2, 0), (0, 1), (1, 1), (2, 1)):
        block(d, k)

    @pl.when(inner)
    def _():
        arrive(3)
    block(3, 0)
    plane_totals(band(NZ - 1))
    block(3, 1)
    plane_totals(band(NZ - 2))
    for d in range(G):
        block(d, 2)
    plane_totals(band(NZ - 3))
    landed(0)
    pl.when(inner)(lambda: last_block(3, False))
    pl.when(jnp.logical_not(inner))(lambda: last_block(3, True))

    CH = NK // NC

    def kv_copy(c, peer):
        at = m128(c, CH)
        return remote(kv.at[0, at], kv.at[1, at], kvs.at[c], kvr.at[c], peer)

    def d_copy(z_to, z_from):
        return remote(dqs.at[m128(z_to, RZ)], dqin.at[z_from], ds.at[z_to], dr.at[z_from], z_to * G + j)

    def coefs(zb):
        cols = m128(zb, ZB)
        for d in range(1, NZ):
            s_copy(zb, z, far(d)[1], me).wait_recv()
        top = stat[0:1, cols]
        for d in range(1, NZ):
            top = jnp.maximum(top, stin[far(d)[1], 0:1, cols])
        w = jnp.exp(stat[0:1, cols] - top)
        total, dotted = w * stat[1:2, cols], w * stat[2:3, cols]
        for d in range(1, NZ):
            i = far(d)[1]
            w = jnp.exp(stin[i, 0:1, cols] - top)
            total += w * stin[i, 1:2, cols]
            dotted += w * stin[i, 2:3, cols]
        for g in range(G):
            coef[g:g + 1, cols] = jnp.exp(gst[g, 0:1, cols] - top) / total
        coef[G:G + 1, cols] = dotted / total

    brim = jnp.where(2 * z < NZ, 0, NZ - 1)
    core_z = jnp.where(2 * z < NZ, 1, NZ - 2)

    def grads(n, zb):
        cols = m128(zb, ZB)
        coefs(zb)
        dqt[...] = jnp.zeros_like(dqt)

        @pl.loop(0, NC)
        def _(c):
            w, off = coef[pl.ds(c, 1), cols], coef[G:G + 1, cols]
            part_q = None
            for i in range(CH // FR):
                at, tok = pl.ds(i * FR, FR), m128(c * (CH // FR) + i, FR)
                p = ebuf[tok, cols] * w
                t = (p * (dpb[tok, cols] - off)).astype(BF16)
                dv = dot(p.astype(BF16), gb[cols, :])
                dk = dot(t, qb[cols, :])
                dq = dot(ktb[:, tok], t)
                part_q = dq if part_q is None else part_q + dq
                if n:
                    dk += tmp[c, at, 0:D]
                    dv += tmp[c, at, D:2 * D]
                if n < NZ - 1:
                    tmp[c, at, 0:D] = dk
                    tmp[c, at, D:2 * D] = dv
                else:
                    kv[0, tok, 0:D] = (scale * dk).astype(BF16)
                    kv[0, tok, D:2 * D] = dv.astype(BF16)
            dqt[...] += part_q
            if n == NZ - 1:
                kv_copy(c, near(1)[1]).start()
        for i in range(ZB // D):
            t = (scale * dqt[:, pl.ds(i * D, D)].T).astype(BF16)
            for k in range(D // RZ):
                m = i * (D // RZ) + k
                dqs[m128(zb, RZ), pl.ds(m * D, D)] = t[k * RZ:(k + 1) * RZ, :]

        @pl.when(zb != z)
        def _():
            d_copy(zb, z).start()

    for f in range(NK // FR):
        ktb[:, pl.ds(f * FR, FR)] = kb[pl.ds(f * FR, FR), :].astype(F32).T.astype(BF16)
    grads(0, NZ - 1 - core_z)
    landed(NZ - 3)
    grads(1, core_z)
    grads(2, NZ - 1 - brim)
    landed(NZ - 2)
    grads(3, brim)
    HW = JW // 2

    def half(u):
        return pl.ds(u * HW, HW)

    def a_copy(kind, u, z_to, z_from):
        here = dqall.at[j, m128(z_from, RZ), half(u)]
        return remote(here, here, as_.at[kind, u, z_to], ar.at[u, z_from], z_to * G + j)

    def a_own(u, act):
        @pl.when(inner)
        def _():
            for d in range(1, NZ):
                act(a_copy(0, u, far(d)[0], z))

        @pl.when(jnp.logical_not(inner))
        def _():
            act(a_copy(0, u, jnp.where(low, NZ - 2, 1), z))

    def a_onward(u, act):
        act(a_copy(1, u, NZ - 1 - z, brim))
        act(a_copy(1, u, NZ - 1 - brim, brim))

    QW = JW // 4

    def y_copy(u, j_from, peer, kind):
        here = dqall.at[j_from, :, pl.ds(u * QW, QW)]
        return remote(here, here, ys.at[kind, u], yr.at[kind, u], peer)

    def y_pass(u, frm, to):
        y_copy(u, near(frm)[0], me, frm - 1).wait_recv()
        send(y_copy(u, near(frm)[0], near(to)[1], 2))

    for c in local_x:
        c.wait()

    def c_copy(side, b, h, i, peer):
        at = m128(i, FB)
        return remote(part.at[h, b, at], rin.at[side, b, h, at], cs.at[b, h, i], cr.at[side, b, h, i], peer)

    def weigh(s, h):
        for i in range(2):
            tmp[h * NZ + s, pl.ds(i * FB, FB), :] = dot(vis[band(s), :, i * FB:(i + 1) * FB], kv[h], TN)

    def gather(s):
        b = band(s)
        x_copy(1, b, x, near(2)[0], me).wait_recv()
        send(f_copy(1, b, True))
        pass_copy(b, near(3)[0], me).wait_recv()
        send(f_copy(2, b, True))
        for kind in range(3):
            f_copy(kind, b, False).wait_recv()

    def hop(s):
        b = band(s)
        side = (b < z).astype(jnp.int32)
        return b, side, jnp.where(b > z, low, high), (z + 1 - 2 * side) * G + j

    def first(s, h):
        weigh(s, h)
        b, side, fed, peer = hop(s)

        @pl.when(jnp.logical_not(fed))
        def _():
            for i in (1 - y, y):
                at = m128(i, FB)
                part[h, b, at] = tmp[h * NZ + s, at].astype(BF16)
                c_copy(side, b, h, i, peer).start()

    def later(s, h):
        b, side, fed, peer = hop(s)

        @pl.when(fed)
        def _():
            for i in (1 - y, y):
                at = m128(i, FB)
                c_copy(side, b, h, i, me).wait_recv()
                part[h, b, at] = (tmp[h * NZ + s, at] + rin[side, b, h, at].astype(F32)).astype(BF16)
                c_copy(side, b, h, i, peer).start()

    def e_copy(h, peer):
        return remote(ybs.at[h], ybr.at[h], es.at[h], er.at[h], peer)

    outs = []

    def settle(head, slot, grad):
        cols = m128(head, D)
        for a, out in enumerate((kw_out, vw_out)):
            wres[a, :, cols] = grad[:, a * D:(a + 1) * D]
            c = pltpu.make_async_copy(wres.at[a, :, cols], out.at[:, cols], ws.at[a, slot])
            c.start()
            outs.append(c)

    def finish(h):
        own = h * NZ + NZ - 1
        for i in (1 - y, y):
            at = m128(i, FB)
            for side, there in ((0, low), (1, high)):
                @pl.when(there)
                def _():
                    c_copy(side, z, h, i, me).wait_recv()
                    tmp[own, at] += rin[side, z, h, at].astype(F32)
            if i is y:
                settle(j ^ h, h, tmp[own, at])
            else:
                ybs[h] = tmp[own, at].astype(BF16)
                send(e_copy(h, near(2)[1]))

    def summed_dq():
        mine = dqs[m128(z, RZ), :].astype(F32)
        for d in range(1, NZ):
            d_copy(z, far(d)[1]).wait_recv()
            mine += dqin[far(d)[1]].astype(F32)
        dqall[j, m128(z, RZ), :] = mine.astype(BF16)
        for u in range(2):
            a_own(u, lambda c: c.start())

    def relay_dq(u):
        @pl.when(inner)
        def _():
            a_copy(0, u, z, brim).wait_recv()
            a_onward(u, lambda c: c.start())

    def shared_dq():
        for u in range(2):
            for d in range(1, NZ):
                b = far(d)[1]

                @pl.when(jnp.logical_not(inner) | (b != brim))
                def _():
                    a_copy(0, u, z, b).wait_recv()
        for u in range(4):
            send(y_copy(u, j, near(1)[1], 0))
            send(y_copy((u + 1) % 4, j, near(2)[1], 1))

    gather(0)
    first(0, 0)
    landed(NZ - 1)
    summed_dq()
    gather(1)
    first(1, 0)
    later(0, 0)
    relay_dq(0)
    relay_dq(1)
    gather(2)
    first(2, 0)
    shared_dq()
    later(1, 0)
    gather(3)
    for c in range(NC):
        kv_copy(c, me).wait_recv()
    first(0, 1)
    for s in range(1, NZ - 1):
        first(s, 1)
    later(2, 0)
    weigh(3, 0)
    weigh(3, 1)
    def put(i):
        c = pltpu.make_async_copy(dqall.at[j ^ i], q_out.at[:, m128(j ^ i, JW)], loc.at[i])
        c.start()
        outs.append(c)

    put(0)
    y_pass(0, 1, 2)
    y_pass(1, 2, 1)
    later(0, 1)
    y_pass(2, 2, 1)
    finish(0)
    y_pass(3, 2, 1)
    later(1, 1)
    later(2, 1)
    for u in range(1, 4):
        y_copy(u, near(1)[0], me, 0).wait_recv()
    put(1)
    y_copy(0, near(2)[0], me, 1).wait_recv()
    put(2)
    finish(1)
    for u in range(4):
        y_copy(u, near(3)[0], me, 2).wait_recv()
    put(3)
    for h in range(2):
        e_copy(h, me).wait_recv()
        settle(j ^ (2 + h), 2 + h, ybr[h].astype(F32))
    for c in outs:
        c.wait()
    for c in sends:
        c.wait_send()
    for k in range(NZ):
        zq_each(lambda c: c.wait_send(), band(NZ - 1 - k), False)
    for u in range(2):
        a_own(u, lambda c: c.wait_send())
        pl.when(inner)(lambda: a_onward(u, lambda c: c.wait_send()))
    for s in range(NZ - 1):
        b, side, fed, peer = hop(s)
        for h in range(2):
            for i in range(2):
                c_copy(side, b, h, i, peer).wait_send()
    for d in range(1, NZ):
        d_copy(far(d)[0], z).wait_send()
    for c in range(NC):
        kv_copy(c, near(1)[1]).wait_send()
    for zb in range(NZ):
        for d in range(1, NZ):
            s_copy(zb, far(d)[0], z, far(d)[2]).wait_send()


def deliver_kernel(parts, *refs):
    n = len(parts)
    srcs, dsts, bufs, ins, outs = refs[:n], refs[n:2 * n], refs[2 * n:3 * n], refs[3 * n], refs[3 * n + 1]
    moves, k = [], 0
    for src, dst, buf, p in zip(srcs, dsts, bufs, parts):
        step = src.shape[0] // p
        for i in range(p):
            at = pl.ds(i * step, step)
            moves.append((pltpu.make_async_copy(src.at[at], buf.at[at], ins.at[k]),
                          pltpu.make_async_copy(buf.at[at], dst.at[at], outs.at[k])))
            k += 1
    for a, _ in moves:
        a.start()
    for a, b in moves:
        a.wait()
        b.start()
    for _, b in moves:
        b.wait()


def deliver(*arrays):
    parts = [8, 2, 2]
    anyspec = pl.BlockSpec(memory_space=pl.ANY)
    return pl.pallas_call(
        functools.partial(deliver_kernel, parts),
        out_shape=[jax.ShapeDtypeStruct(a.shape, a.dtype) for a in arrays],
        in_specs=[anyspec] * len(arrays),
        out_specs=[anyspec] * len(arrays),
        scratch_shapes=[pltpu.VMEM(a.shape, a.dtype) for a in arrays]
        + [pltpu.SemaphoreType.DMA((sum(parts),)), pltpu.SemaphoreType.DMA((sum(parts),))],
        compiler_params=pltpu.CompilerParams(vmem_limit_bytes=67043328),
    )(*arrays)


def plane_shards(T, text_queries, text_grads, vision_keys, video_value_rows, vision, lengths, frame_range):
    R, QW = text_queries.shape
    rows, kv_width = vision_keys.shape
    G = kv_width // HEAD_WIDTH
    M = QW // kv_width
    NZ = T // G
    DW = vision.shape[1]
    FB = DW // T
    NK, RZ, JW = G * rows, G * R, M * HEAD_WIDTH
    NR = T * R * M
    cfg = dict(G=G, NZ=NZ, M=M, R=R, FR=rows // FRAME_DEV, NC=4, rows=rows, NK=NK, NR=NR, JW=JW, FB=FB, RZ=RZ,
               NS=lengths.shape[0])
    anyspec = pl.BlockSpec(memory_space=pl.ANY)
    vm = pl.BlockSpec(memory_space=pltpu.VMEM)
    V = pltpu.VMEM
    D = pltpu.SemaphoreType.DMA
    W2 = 2 * HEAD_WIDTH
    pairs = []
    for a, b in (((2, G),) * 2, ((2, 2, NZ), (2, NZ)), ((2, G),) * 2, ((3, NZ),) * 2, ((3, NZ),) * 2, ((NZ, NZ),) * 2, ((cfg["NC"],),) * 2,
                 ((NZ,),) * 2, ((2, 2, NZ), (2, NZ)), ((3, 4),) * 2, ((NZ, 2, 2), (2, NZ, 2, 2)), ((2,),) * 2):
        pairs += [D(a), D(b)]
    q_grad, kw, vw = pl.pallas_call(
        functools.partial(plane_kernel, cfg),
        out_shape=(
            jax.ShapeDtypeStruct((T * R, QW), BF16),
            jax.ShapeDtypeStruct((FB, kv_width), F32),
            jax.ShapeDtypeStruct((FB, kv_width), F32),
        ),
        in_specs=[anyspec] * 7,
        out_specs=(anyspec,) * 3,
        scratch_shapes=[
            V((T * R, JW), BF16), V((T * R, JW), BF16),
            V((NR, HEAD_WIDTH), BF16), V((NR, HEAD_WIDTH), BF16),
            V((NK, HEAD_WIDTH), BF16), V((NK, HEAD_WIDTH), BF16),
            V((NZ, NK, 2 * FB), BF16),
            V((NK, NR), F32), V((NK, NR), F32),
            V((8, NR), F32), V((NZ, 8, NR), F32), V((8, NR), F32), V((8, NR), jnp.int32),
            V((2, NK, W2), BF16),
            V((HEAD_WIDTH, M * RZ), F32), V((T * R, JW), BF16),
            V((NZ, RZ, JW), BF16), V((G, T * R, JW), BF16),
            V((G, 8, NR), F32), V((HEAD_WIDTH, NK), BF16),
            V((2, FB, kv_width), F32), D((2, 4)),
            pltpu.SMEM(lengths.shape, jnp.int32), pltpu.SMEM(frame_range.shape[::-1], jnp.int32),
            V((2 * NZ, 2 * FB, W2), F32), V((2, NZ, 2 * FB, W2), BF16), V((2, NZ, 2, 2 * FB, W2), BF16),
            V((2, FB, W2), BF16), V((2, FB, W2), BF16),
            D((6,)), D((NZ, 2)),
        ] + pairs,
        compiler_params=pltpu.CompilerParams(
            collective_id=0, has_side_effects=True, vmem_limit_bytes=67043328
        ),
    )(text_queries, text_grads, vision_keys, video_value_rows, vision, lengths, frame_range.T)
    return deliver(q_grad, kw, vw)


def solution(mesh):
    return jax.shard_map(
        functools.partial(shards, mesh.shape["tok"], mesh.shape["head"]),
        mesh=mesh,
        in_specs=(
            P("tok", "head"),
            P("tok", "head"),
            P("tok", "head"),
            P("tok", "head"),
            P("tok", None),
            P(),
            P(),
        ),
        out_specs=(P(None, "head"), P("tok", "head"), P("tok", "head")),
        check_vma=False,
    )
```

```python
import functools

import jax
import jax.numpy as jnp
from jax import lax
from jax.experimental import pallas as pl
from jax.experimental.pallas import tpu as pltpu
from jax.sharding import PartitionSpec as P

HEAD_WIDTH = 128
FRAME_DEV = 4
NEG_FILL = -1e30
NT = (((1,), (1,)), ((), ()))
TN = (((0,), (0,)), ((), ()))
F32 = jnp.float32
BF16 = jnp.bfloat16


def dot(a, b, dims=(((1,), (0,)), ((), ()))):
    return lax.dot_general(a, b, dims, preferred_element_type=F32)


def kernel(cfg, q_in, g_in, k_in, v_in, x_in, bounds, q_out, kw_out, vw_out,
           qb, gb, kb, vb, vis, ebuf, dpb, stat, stin, coef, kv, dqt, dqs, dqin, dqall, part, rsb,
           loc, qs, qr, gs, gr, ks, kr, vs, vr, xs, xr, ss, sr, kvs, kvr, ds, dr, as_, ar, ys, yr, rs, rr, fs, fr):
    T, G, NZ = cfg["T"], cfg["G"], cfg["NZ"]
    blk, rows, NK, NR, FR = cfg["blk"], cfg["rows"], cfg["NK"], cfg["NR"], cfg["FR"]
    W, NV, FB = cfg["W"], cfg["NV"], cfg["FB"]
    H = cfg["H"]
    RB = cfg["RB"]
    scale = HEAD_WIDTH ** (-0.5)
    me = lax.axis_index("tok")
    z, j0 = me // G, me % G

    def remote(src, dst, s, r, peer):
        return pltpu.make_async_remote_copy(
            src_ref=src, dst_ref=dst, send_sem=s, recv_sem=r,
            device_id={"tok": peer}, device_id_type=pl.DeviceIdType.MESH)

    def m128(i, n):
        return pl.ds(pl.multiple_of(i * n, n), n)

    barrier = pltpu.get_barrier_semaphore()
    for d in range(1, T):
        pl.semaphore_signal(barrier, inc=1, device_id={"tok": lax.rem(me + d, T)}, device_id_type=pl.DeviceIdType.MESH)
    twin = lax.axis_index("head")
    if H > 1:
        twin = 1 - twin
        pl.semaphore_signal(barrier, inc=1, device_id={"head": twin}, device_id_type=pl.DeviceIdType.MESH)
    pl.semaphore_wait(barrier, T - 1 + (H > 1))

    def tpeer(d):
        return lax.rem(me + d, T), lax.rem(me + T - d, T)

    def gpeer(d):
        a, b = (j0 ^ d, j0 ^ d) if G & (G - 1) == 0 else (lax.rem(j0 + d, G), lax.rem(j0 + G - d, G))
        return a, b, z * G + a, z * G + b

    def zpeer(d):
        a, b = lax.rem(z + d, NZ), lax.rem(z + NZ - d, NZ)
        return a, b, a * G + j0, b * G + j0

    sends = []

    def send(c):
        c.start()
        sends.append(c)

    def q_copy(t_to, t_from):
        return (remote(q_in.at[lax.rem(t_to, G)], qb.at[m128(t_from, blk)], qs.at[t_to], qr.at[t_from], t_to),
                remote(g_in.at[lax.rem(t_to, G)], gb.at[m128(t_from, blk)], gs.at[t_to], gr.at[t_from], t_to))

    def k_copy(j_to, j_from, peer):
        return (remote(k_in.at[:, m128(j_to, 128)], kb.at[m128(j_from, rows)], ks.at[j_to], kr.at[j_from], peer),
                remote(v_in.at[:, m128(j_to, 128)], vb.at[m128(j_from, rows)], vs.at[j_to], vr.at[j_from], peer))

    WH = W // H
    half = lax.axis_index("head") * WH if H > 1 else 0

    def x_copy(b, j_to, j_from, peer):
        cols = pl.ds(pl.multiple_of((b * G + j_to) * W + half, WH), WH)
        dst = vis.at[b, m128(j_from, rows), pl.ds(pl.multiple_of(half, WH), WH)]
        return remote(x_in.at[:, cols], dst, xs.at[j_to, b], xr.at[j_from, b], peer)

    def f_copy(b, j_from, mine):
        at = half if mine else WH - half
        here = vis.at[b, m128(j_from, rows), pl.ds(pl.multiple_of(at, WH), WH)]
        return pltpu.make_async_remote_copy(
            src_ref=here, dst_ref=here, send_sem=fs.at[j_from, b], recv_sem=fr.at[j_from, b],
            device_id={"head": twin}, device_id_type=pl.DeviceIdType.MESH)

    local = [
        pltpu.make_async_copy(q_in.at[j0], qb.at[m128(me, blk)], loc.at[0]),
        pltpu.make_async_copy(g_in.at[j0], gb.at[m128(me, blk)], loc.at[1]),
        pltpu.make_async_copy(k_in.at[:, m128(j0, 128)], kb.at[m128(j0, rows)], loc.at[2]),
        pltpu.make_async_copy(v_in.at[:, m128(j0, 128)], vb.at[m128(j0, rows)], loc.at[3]),
    ]
    local_x = [pltpu.make_async_copy(x_in.at[:, m128(b * G + j0, W)], vis.at[b, m128(j0, rows)], loc.at[4 + b]) for b in range(NV)]
    for c in local:
        c.start()
    def q_sends(zd):
        a, _, _, _ = zpeer(zd)
        for i in range(G):
            to = a * G + (lax.rem(j0 + i, G) if zd else gpeer(i)[0])
            if zd or i:
                for c in q_copy(to, me):
                    send(c)

    q_sends(0)
    for d in range(1, G):
        a, _, peer, _ = gpeer(d)
        for c in k_copy(a, j0, peer):
            send(c)
    for d in range(1, NZ):
        q_sends(d)
    for c in local_x:
        c.start()
    for c in local:
        c.wait()
    for d in range(1, G):
        _, b, _, _ = gpeer(d)
        for c in k_copy(j0, b, me):
            c.wait_recv()

    def q_wait(zd):
        _, b, _, _ = zpeer(zd)
        for i in range(G):
            if zd or i:
                frm = b * G + (i if zd else gpeer(i)[1])
                for c in q_copy(me, frm):
                    c.wait_recv()

    n_frames = NK // FR
    frame0 = z * n_frames
    stat[0:1, :] = jnp.full((1, NR), NEG_FILL, F32)
    stat[1:8, :] = jnp.zeros((7, NR), F32)

    def totals(cols, width):
        first, end = bounds[0:1, cols], bounds[1:2, cols]
        UN = 2 if n_frames % 2 == 0 else 1

        def scored(i, top):
            for u in range(UN):
                f = i * UN + u
                ok = (first <= frame0 + f) & (frame0 + f < end)
                s = jnp.where(ok, dot(kb[m128(f, FR), :], qb[cols, :], NT) * scale, NEG_FILL)
                ebuf[m128(f, FR), cols] = s
                top = jnp.maximum(top, jnp.max(s, axis=0, keepdims=True))
            return top

        top = lax.fori_loop(0, n_frames // UN, scored, jnp.full((1, width), NEG_FILL, F32))

        def summed(i, carry):
            total, dotted = carry
            for u in range(UN):
                f = i * UN + u
                dp = dot(vb[m128(f, FR), :], gb[cols, :], NT)
                e = jnp.exp(ebuf[m128(f, FR), cols] - top)
                ebuf[m128(f, FR), cols] = e
                dpb[m128(f, FR), cols] = dp
                total += jnp.sum(e, axis=0, keepdims=True)
                dotted += jnp.sum(e * dp, axis=0, keepdims=True)
            return total, dotted

        zero = jnp.zeros((1, width), F32)
        total, dotted = lax.fori_loop(0, n_frames // UN, summed, (zero, zero))
        stat[0:1, cols] = top
        stat[1:2, cols] = total
        stat[2:3, cols] = dotted

    def x_sends():
        for d in range(1, G):
            a, _, peer, _ = gpeer(d)
            for b in range(NV):
                send(x_copy(b, a, j0, peer))

    by_z = (NR // NZ) % 128 == 0
    for d in range(NZ):
        q_wait(d)
        if d == NZ - 1:
            x_sends()
        if by_z:
            totals(m128(zpeer(d)[1], NR // NZ), NR // NZ)
    if not by_z:
        for r in range(0, NR, RB):
            totals(pl.ds(r, RB), RB)

    def s_copy(z_to, z_from, peer):
        return remote(stat, stin.at[z_from], ss.at[z_to], sr.at[z_from], peer)

    for d in range(1, NZ):
        a, _, peer, _ = zpeer(d)
        send(s_copy(a, z, peer))
    stin[z] = stat[...]
    for d in range(1, NZ):
        _, b, _, _ = zpeer(d)
        s_copy(z, b, me).wait_recv()
    top = stat[0:1, :]
    for i in range(NZ):
        top = jnp.maximum(top, stin[i, 0:1, :])
    total = jnp.zeros((1, NR), F32)
    dotted = jnp.zeros((1, NR), F32)
    for i in range(NZ):
        w = jnp.exp(stin[i, 0:1, :] - top)
        total += w * stin[i, 1:2, :]
        dotted += w * stin[i, 2:3, :]
    coef[0:1, :] = jnp.exp(stat[0:1, :] - top) / total
    coef[1:2, :] = dotted / total
    dqt[...] = jnp.zeros_like(dqt)

    NC = cfg["NC"]
    CH = NK // NC

    def kv_copy(c, j_to, j_from, peer):
        here = kv.at[j_from, pl.ds(c * CH, CH)]
        return remote(here, here, kvs.at[j_to, c], kvr.at[j_from, c], peer)

    for c in range(NC):
        @pl.loop(c * (CH // FR), (c + 1) * (CH // FR))
        def _(f):
            kt = kb[m128(f, FR), :].astype(F32).T.astype(BF16)
            dk = jnp.zeros((FR, HEAD_WIDTH), F32)
            dv = jnp.zeros((FR, HEAD_WIDTH), F32)
            for r in range(0, NR, RB):
                cols = pl.ds(r, RB)
                p = ebuf[m128(f, FR), cols] * coef[0:1, cols]
                t = (p * (dpb[m128(f, FR), cols] - coef[1:2, cols])).astype(BF16)
                dv += dot(p.astype(BF16), gb[cols, :])
                dk += dot(t, qb[cols, :])
                dqt[:, cols] += dot(kt, t)
            kv[j0, m128(f, FR), 0:HEAD_WIDTH] = (scale * dk).astype(BF16)
            kv[j0, m128(f, FR), HEAD_WIDTH:2 * HEAD_WIDTH] = dv.astype(BF16)

        for d in range(1, G - 1):
            a, _, peer, _ = gpeer(d)
            kv_copy(c, a, j0, peer).start()
        if H > 1 and c == NC // 2:
            for d in range(1, G):
                _, b, _, _ = gpeer(d)
                for i in range(NV):
                    x_copy(i, j0, b, me).wait_recv()
                    send(f_copy(i, b, True))

    for r in range(0, NR, 128):
        dqs[pl.ds(r, 128), :] = (scale * dqt[:, pl.ds(r, 128)].T).astype(BF16)
    QR = NR // NZ

    def d_copy(z_to, z_from, peer):
        return remote(dqs.at[m128(z_to, QR)], dqin.at[z_from], ds.at[z_to], dr.at[z_from], peer)

    def a_copy(z_to, z_from, peer):
        here = dqall.at[j0, m128(z_from, QR)]
        return remote(here, here, as_.at[z_to], ar.at[z_from], peer)

    def y_copy(j_to, j_from, peer):
        here = dqall.at[j_from]
        return remote(here, here, ys.at[j_to], yr.at[j_from], peer)

    def r_copy(j, z_to, z_from, peer):
        return remote(part.at[j, m128(z_to, FB)], rsb.at[z_from, j], rs.at[j, z_to], rr.at[j, z_from], peer)

    for d in range(1, NZ):
        a, _, peer, _ = zpeer(d)
        send(d_copy(a, z, peer))
    for c in local_x:
        c.wait()
    for d in range(1, G):
        _, b, _, _ = gpeer(d)
        for i in range(NV):
            (f_copy(i, b, False) if H > 1 else x_copy(i, j0, b, me)).wait_recv()

    def weigh(j):
        @pl.loop(0, NV)
        def _(b):
            part[j, m128(b, W), :] = dot(vis[b], kv[j], TN).astype(BF16)
        for d in range(1, NZ):
            a, _, peer, _ = zpeer(d)
            send(r_copy(j, a, z, peer))

    weigh(j0)
    mine = dqs[m128(z, QR), :].astype(F32)
    for d in range(1, NZ):
        _, b, _, _ = zpeer(d)
        d_copy(z, b, me).wait_recv()
        mine += dqin[b].astype(F32)
    dqall[j0, m128(z, QR), :] = mine.astype(BF16)
    for d in range(1, NZ):
        a, _, peer, _ = zpeer(d)
        send(a_copy(a, z, peer))

    def spread():
        for d in range(1, NZ):
            _, b, _, _ = zpeer(d)
            a_copy(z, b, me).wait_recv()
        for d in range(1, G):
            a, _, peer, _ = gpeer(d)
            send(y_copy(a, j0, peer))

    for d in range(1, G - 1):
        a, _, peer, _ = gpeer(d)
        for c in range(NC):
            kv_copy(c, a, j0, peer).wait_send()
    if G > 1:
        a, _, peer, _ = gpeer(G - 1)
        for c in range(NC):
            send(kv_copy(c, a, j0, peer))
    if G == 1:
        spread()
    for d in range(1, G):
        _, b, _, _ = gpeer(d)
        for c in range(NC):
            kv_copy(c, j0, b, me).wait_recv()
        weigh(b)
        if d == min(2, G - 1):
            spread()
    for d in range(1, G):
        _, b, _, _ = gpeer(d)
        y_copy(j0, b, me).wait_recv()
    out_copy = pltpu.make_async_copy(dqall, q_out, loc.at[0])
    out_copy.start()

    for d in range(1, NZ):
        _, b, _, _ = zpeer(d)
        for j in range(G):
            r_copy(j, z, b, me).wait_recv()
    for j in range(G):
        acc = part[j, m128(z, FB), :].astype(F32)
        for d in range(1, NZ):
            _, b, _, _ = zpeer(d)
            acc += rsb[b, j].astype(F32)
        kw_out[:, pl.ds(j * HEAD_WIDTH, HEAD_WIDTH)] = acc[:, 0:HEAD_WIDTH]
        vw_out[:, pl.ds(j * HEAD_WIDTH, HEAD_WIDTH)] = acc[:, HEAD_WIDTH:]
    out_copy.wait()
    for c in sends:
        c.wait_send()


def shards(T, cores, text_queries, text_grads, vision_keys, video_value_rows, vision, lengths, frame_range):
    R, QW = text_queries.shape
    rows, kv_width = vision_keys.shape
    G = kv_width // HEAD_WIDTH
    if cores == 2 and G == 4 and T == G * G and vision.shape[1] % (T * 128) == 0 and HEAD_WIDTH % (G * R) == 0 and 2 * vision.shape[1] == T * rows:
        return plane_shards(T, text_queries, text_grads, vision_keys, video_value_rows, vision, lengths, frame_range)
    M = QW // kv_width
    NZ = T // G
    DW = vision.shape[1]
    blk, NK, NR = M * R, G * rows, T * M * R
    FB = DW // T
    W = FB if FB % 128 == 0 else 256
    NV = DW // (G * W)
    FR = rows // FRAME_DEV
    NC = 4 if NK >= 16 * FR else 1
    cfg = dict(T=T, G=G, NZ=NZ, blk=blk, rows=rows, NK=NK, NR=NR, FR=FR, W=W, NV=NV, FB=FB, NC=NC, RB=min(NR, 512),
               H=2 if cores == 2 and G > 1 and W % 256 == 0 else 1)

    text_len = R * T
    row_ids = jnp.arange(text_len, dtype=jnp.int32)
    segment_ends = jnp.cumsum(lengths)
    segment = jnp.sum((row_ids[:, None] >= segment_ends[None, :]).astype(jnp.int32), axis=1)
    segment_pick = (
        segment[:, None] == jnp.arange(lengths.shape[0], dtype=jnp.int32)[None, :]
    ).astype(jnp.int32)
    bounds = jnp.sum(segment_pick[None] * frame_range.T[:, None, :], axis=2)
    bounds = jnp.broadcast_to(bounds.reshape(2, T, 1, R), (2, T, M, R)).reshape(2, NR)

    def split(a):
        return a.reshape(R, G, M, HEAD_WIDTH).transpose(1, 2, 0, 3).reshape(G, blk, HEAD_WIDTH)

    anyspec = pl.BlockSpec(memory_space=pl.ANY)
    vm = pl.BlockSpec(memory_space=pltpu.VMEM)
    V = pltpu.VMEM
    D = pltpu.SemaphoreType.DMA
    sem_pairs = []
    for shape in ((T,), (T,), (G,), (G,), (G, NV), (NZ,), (G, NC), (NZ,), (NZ,), (G,), (G, NZ), (G, NV)):
        sem_pairs += [D(shape), D(shape)]
    q_grad, kw, vw = pl.pallas_call(
        functools.partial(kernel, cfg),
        out_shape=(
            jax.ShapeDtypeStruct((G, NR, HEAD_WIDTH), BF16),
            jax.ShapeDtypeStruct((FB, kv_width), F32),
            jax.ShapeDtypeStruct((FB, kv_width), F32),
        ),
        in_specs=[anyspec] * 5 + [vm],
        out_specs=(anyspec, vm, vm),
        scratch_shapes=[
            V((NR, HEAD_WIDTH), BF16), V((NR, HEAD_WIDTH), BF16),
            V((NK, HEAD_WIDTH), BF16), V((NK, HEAD_WIDTH), BF16),
            V((NV, NK, W), BF16),
            V((NK, NR), F32), V((NK, NR), F32),
            V((8, NR), F32), V((NZ, 8, NR), F32), V((8, NR), F32),
            V((G, NK, 2 * HEAD_WIDTH), BF16),
            V((HEAD_WIDTH, NR), F32), V((NR, HEAD_WIDTH), BF16),
            V((NZ, NR // NZ, HEAD_WIDTH), BF16), V((G, NR, HEAD_WIDTH), BF16),
            V((G, DW // G, 2 * HEAD_WIDTH), BF16),
            V((NZ, G, FB, 2 * HEAD_WIDTH), BF16),
            D((4 + NV,)),
        ] + sem_pairs,
        compiler_params=pltpu.CompilerParams(
            collective_id=0, has_side_effects=True, vmem_limit_bytes=67043328
        ),
    )(split(text_queries), split(text_grads), vision_keys, video_value_rows, vision, bounds)
    q_grad = q_grad.reshape(G, T, M, R, HEAD_WIDTH).transpose(1, 3, 0, 2, 4).reshape(text_len, QW)
    return q_grad, kw, vw


def plane_kernel(cfg, q_in, g_in, k_in, v_in, x_in, lens_in, frames_in, q_out, kw_out, vw_out,
                 qraw, graw, qb, gb, kb, vb, vis, ebuf, dpb, stat, stin, coef, lim, kv, kvn, dqt, dqs, dqin, dqall,
                 gst, ktb, wres, ws, lens, frames, tmp, part, rin, ybs, ybr, loc, lx, qs, qr, zs, zr, ks, kr, xs, xr, fs, fr, ss, sr, kvs, kvr,
                 ds, dr, as_, ar, ys, yr, cs, cr, es, er):
    G, NZ, M, R, FR, NC = cfg["G"], cfg["NZ"], cfg["M"], cfg["R"], cfg["FR"], cfg["NC"]
    rows, NK, NR, JW, FB, RZ = cfg["rows"], cfg["NK"], cfg["NR"], cfg["JW"], cfg["FB"], cfg["RZ"]
    D = HEAD_WIDTH
    ZB = M * RZ
    scale = D ** (-0.5)
    me = lax.axis_index("tok")
    core = lax.axis_index("head")
    z, j = me // G, me % G
    y, x = j // 2, j % 2

    def m128(i, n):
        return pl.ds(pl.multiple_of(i * n, n), n)

    def remote(src, dst, s, r, peer):
        return pltpu.make_async_remote_copy(
            src_ref=src, dst_ref=dst, send_sem=s, recv_sem=r,
            device_id={"tok": peer}, device_id_type=pl.DeviceIdType.MESH)

    def near(d):
        return j ^ d, z * G + (j ^ d)

    def far(d):
        a, b = lax.rem(z + d, NZ), lax.rem(z + NZ - d, NZ)
        return a, b, a * G + j, b * G + j

    mirror = 2 * z > NZ - 1
    zz = jnp.where(mirror, NZ - 1 - z, z)

    def band(s):
        u = s - (NZ - 1 - 2 * zz)
        k, odd = u // 2, u % 2
        b = jnp.where(u < 0, NZ - 1 - s, k + odd * (2 * zz - 2 * k))
        return jnp.where(mirror, NZ - 1 - b, b)

    barrier = pltpu.get_barrier_semaphore()
    for d in range(1, G):
        pl.semaphore_signal(barrier, inc=1, device_id={"tok": near(d)[1]}, device_id_type=pl.DeviceIdType.MESH)
    for d in range(1, NZ):
        pl.semaphore_signal(barrier, inc=1, device_id={"tok": far(d)[2]}, device_id_type=pl.DeviceIdType.MESH)
    pl.semaphore_signal(barrier, inc=1, device_id={"head": 1 - core}, device_id_type=pl.DeviceIdType.MESH)
    pl.semaphore_wait(barrier, G + NZ - 1)

    sends = []

    def send(c):
        c.start()
        sends.append(c)

    def own_rows(t):
        return m128(t, R)

    def q_copy(d, t_from, peer, j_to):
        cols = m128(j_to, JW)
        return (remote(q_in.at[:, cols], qraw.at[own_rows(t_from)], qs.at[0, d], qr.at[0, d], peer),
                remote(g_in.at[:, cols], graw.at[own_rows(t_from)], qs.at[1, d], qr.at[1, d], peer))

    low, high = z > 0, z < NZ - 1
    inner = low & high

    def zq_copy(side, a, b):
        here = (qraw, graw)[a].at[m128(b, RZ)]
        return remote(here, here, zs.at[side, a, b], zr.at[a, b], (z + 1 - 2 * side) * G + j)

    def zq_each(act, b, into, which=(0, 1)):
        for a in which:
            if into:
                zq_copy(0, a, b).wait_recv()

            @pl.when(high & (b <= z))
            def _():
                act(zq_copy(0, a, b))

            @pl.when(low & (b >= z))
            def _():
                act(zq_copy(1, a, b))

    def k_copy(d, j_to, j_from, peer):
        return (remote(k_in.at[:, m128(j_to, D)], kb.at[m128(j_from, rows)], ks.at[0, d], kr.at[0, d], peer),
                remote(v_in.at[:, m128(j_to, D)], vb.at[m128(j_from, rows)], ks.at[1, d], kr.at[1, d], peer))

    def lane_half(mine):
        return m128(core if mine else 1 - core, FB)

    def x_copy(kind, b, x_to, j_from, peer):
        cols = m128(b * G + core * 2 + x_to, FB)
        dst = vis.at[b, m128(j_from, rows), lane_half(True)]
        return remote(x_in.at[:, cols], dst, xs.at[kind, b], xr.at[kind, b], peer)

    def pass_copy(b, j_from, peer):
        here = vis.at[b, m128(j_from, rows), lane_half(True)]
        return remote(here, here, xs.at[2, b], xr.at[2, b], peer)

    def f_copy(kind, b, mine):
        here = vis.at[b, m128(j ^ (kind + 1), rows), lane_half(mine)]
        return pltpu.make_async_remote_copy(
            src_ref=here, dst_ref=here, send_sem=fs.at[kind, b], recv_sem=fr.at[kind, b],
            device_id={"head": 1 - core}, device_id_type=pl.DeviceIdType.MESH)

    local = [
        pltpu.make_async_copy(q_in.at[:, m128(j, JW)], qraw.at[own_rows(me)], loc.at[0]),
        pltpu.make_async_copy(g_in.at[:, m128(j, JW)], graw.at[own_rows(me)], loc.at[1]),
        pltpu.make_async_copy(k_in.at[:, m128(j, D)], kb.at[m128(j, rows)], loc.at[2]),
        pltpu.make_async_copy(v_in.at[:, m128(j, D)], vb.at[m128(j, rows)], loc.at[3]),
        pltpu.make_async_copy(lens_in, lens, loc.at[4]),
        pltpu.make_async_copy(frames_in, frames, loc.at[5]),
    ]
    for c in local:
        c.start()
    for d in range(G - 1, 0, -1):
        for c in q_copy(d, me, near(d)[1], near(d)[0]):
            send(c)
    for d in range(1, G):
        for c in k_copy(d, near(d)[0], j, near(d)[1]):
            send(c)
    local_x = []
    for b in range(NZ):
        for h in range(2):
            local_x.append(pltpu.make_async_copy(
                x_in.at[:, m128(b * G + 2 * h + x, FB)], vis.at[b, m128(j, rows), pl.ds(h * FB, FB)], lx.at[b, h]))

    for c in local[4:]:
        c.wait()
    col = lax.broadcasted_iota(jnp.int32, (1, NR), 1)
    text = (col // ZB) * RZ + col % RZ
    seg = jnp.zeros((1, NR), jnp.int32)
    end = jnp.int32(0)
    NS = cfg["NS"]
    for i in range(NS):
        end = end + lens[i]
        seg += (text >= end).astype(jnp.int32)
    first, last = jnp.zeros((1, NR), jnp.int32), jnp.zeros((1, NR), jnp.int32)
    for i in range(NS):
        first = jnp.where(seg == i, frames[0, i], first)
        last = jnp.where(seg == i, frames[1, i], last)
    lim[0:1, :] = first
    lim[1:2, :] = last
    stat[0:8, :] = jnp.zeros((8, NR), F32)

    for c in local[:2]:
        c.wait()
    for d in range(1, G):
        for c in q_copy(d, z * G + near(d)[0], me, j):
            c.wait_recv()
    zq_each(lambda c: c.start(), z, False)
    for s in range(NZ):
        send(x_copy(0, band(s), 1 - x, j, near(1)[1]))
        if s < NZ // 2:
            send(x_copy(1, band(s), x, j, near(2)[1]))
    for c in local_x:
        c.start()
    for c in local[2:4]:
        c.wait()

    n_frames = rows // FR

    def tokens(g, f):
        return m128(g * n_frames + f, FR)

    def scored(g, zb):
        cols = m128(zb, ZB)
        lo, hi = lim[0:1, cols], lim[1:2, cols]
        base = z * G * n_frames + g * n_frames
        top = jnp.full((1, ZB), NEG_FILL, F32)
        for f in range(n_frames):
            ok = (lo <= base + f) & (base + f < hi)
            sc = jnp.where(ok, dot(kb[tokens(g, f), :], qb[cols, :], NT) * scale, NEG_FILL)
            ebuf[tokens(g, f), cols] = sc
            top = jnp.maximum(top, jnp.max(sc, axis=0, keepdims=True))
        gst[g, 0:1, cols] = top

    def summed(g, zb):
        cols = m128(zb, ZB)
        top = gst[g, 0:1, cols]
        total = jnp.zeros((1, ZB), F32)
        dotted = jnp.zeros((1, ZB), F32)
        for f in range(n_frames):
            dp = dot(vb[tokens(g, f), :], gb[cols, :], NT)
            e = jnp.exp(ebuf[tokens(g, f), cols] - top)
            ebuf[tokens(g, f), cols] = e
            dpb[tokens(g, f), cols] = dp
            total += jnp.sum(e, axis=0, keepdims=True)
            dotted += jnp.sum(e * dp, axis=0, keepdims=True)
        gst[g, 1:2, cols] = total
        gst[g, 2:3, cols] = dotted

    def s_copy(zb, z_to, z_from, peer):
        cols = m128(zb, ZB)
        return remote(stat.at[:, cols], stin.at[z_from, :, cols], ss.at[zb, z_to], sr.at[zb, z_from], peer)

    def plane_totals(zb):
        cols = m128(zb, ZB)
        top = gst[0, 0:1, cols]
        for g in range(1, G):
            top = jnp.maximum(top, gst[g, 0:1, cols])
        total = jnp.zeros((1, ZB), F32)
        dotted = jnp.zeros((1, ZB), F32)
        for g in range(G):
            w = jnp.exp(gst[g, 0:1, cols] - top)
            total += w * gst[g, 1:2, cols]
            dotted += w * gst[g, 2:3, cols]
        stat[0:1, cols] = top
        stat[1:2, cols] = total
        stat[2:3, cols] = dotted
        for d in range(1, NZ):
            s_copy(zb, far(d)[0], z, far(d)[2]).start()

    def landed(s):
        b = band(s)
        x_copy(0, b, x, near(1)[0], me).wait_recv()
        send(pass_copy(b, near(1)[0], near(2)[1]))
        if s < NZ // 2:
            send(x_copy(1, band(s + NZ // 2), x, j, near(2)[1]))
        send(f_copy(0, b, True))

    have_g, have_z = {0}, set()

    def arrive(k, which=(0, 1)):
        zq_each(lambda c: c.start(), band(NZ - 1 - k), True, which)

    def head_rows(zb, which=(0, 1)):
        for a in which:
            raw, buf = (qraw, graw)[a], (qb, gb)[a]
            for m in range(M):
                buf[m128(zb * M + m, RZ), :] = raw[m128(zb, RZ), m * D:(m + 1) * D]

    def block(d, k):
        zb = band(NZ - 1 - k)
        if d not in have_g:
            have_g.add(d)
            for c in k_copy(d, j, near(d)[0], me):
                c.wait_recv()
        if k not in have_z:
            have_z.add(k)
            if k:
                pl.when(jnp.logical_not(inner))(lambda: arrive(k))
            head_rows(zb)
        scored(j ^ d, zb)
        summed(j ^ d, zb)

    def last_block(k, waits):
        zb = band(NZ - 1 - k)
        for a, work in ((0, scored), (1, summed)):
            if waits:
                arrive(k, (a,))
            head_rows(zb, (a,))
            for d in range(G):
                work(j ^ d, zb)
        plane_totals(zb)

    block(0, 0)
    block(1, 0)

    @pl.when(inner)
    def _():
        arrive(1)
        arrive(2)
    for d, k in ((2, 0), (0, 1), (1, 1), (2, 1)):
        block(d, k)

    @pl.when(inner)
    def _():
        arrive(3)
    block(3, 0)
    plane_totals(band(NZ - 1))
    block(3, 1)
    plane_totals(band(NZ - 2))
    for d in range(G):
        block(d, 2)
    plane_totals(band(NZ - 3))
    landed(0)
    pl.when(inner)(lambda: last_block(3, False))
    pl.when(jnp.logical_not(inner))(lambda: last_block(3, True))

    CH = NK // NC

    def kv_copy(p, peer):
        return remote(kv.at[:, pl.ds(p * D, D)], kvn.at[p], kvs.at[p], kvr.at[p], peer)

    def d_copy(z_to, z_from):
        return remote(dqs.at[m128(z_to, RZ)], dqin.at[z_from], ds.at[z_to], dr.at[z_from], z_to * G + j)

    def coefs(zb):
        cols = m128(zb, ZB)
        for d in range(1, NZ):
            s_copy(zb, z, far(d)[1], me).wait_recv()
        top = stat[0:1, cols]
        for d in range(1, NZ):
            top = jnp.maximum(top, stin[far(d)[1], 0:1, cols])
        w = jnp.exp(stat[0:1, cols] - top)
        total, dotted = w * stat[1:2, cols], w * stat[2:3, cols]
        for d in range(1, NZ):
            i = far(d)[1]
            w = jnp.exp(stin[i, 0:1, cols] - top)
            total += w * stin[i, 1:2, cols]
            dotted += w * stin[i, 2:3, cols]
        for g in range(G):
            coef[g:g + 1, cols] = jnp.exp(gst[g, 0:1, cols] - top) / total
        coef[G:G + 1, cols] = dotted / total

    brim = jnp.where(2 * z < NZ, 0, NZ - 1)
    core_z = jnp.where(2 * z < NZ, 1, NZ - 2)

    def grads(n, zb):
        cols = m128(zb, ZB)
        coefs(zb)
        dqt[...] = jnp.zeros_like(dqt)

        @pl.loop(0, NC)
        def _(c):
            w, off = coef[pl.ds(c, 1), cols], coef[G:G + 1, cols]
            part_q = None
            for i in range(CH // FR):
                at, tok = pl.ds(i * FR, FR), m128(c * (CH // FR) + i, FR)
                p = ebuf[tok, cols] * w
                t = (p * (dpb[tok, cols] - off)).astype(BF16)
                dv = dot(p.astype(BF16), gb[cols, :])
                dk = dot(t, qb[cols, :])
                dq = dot(ktb[:, tok], t)
                part_q = dq if part_q is None else part_q + dq
                if n:
                    dk += tmp[c, at, 0:D]
                    dv += tmp[c, at, D:2 * D]
                if n < NZ - 1:
                    tmp[c, at, 0:D] = dk
                    tmp[c, at, D:2 * D] = dv
                else:
                    kv[tok, 0:D] = (scale * dk).astype(BF16)
                    kv[tok, D:2 * D] = dv.astype(BF16)
            dqt[...] += part_q

        if n == NZ - 1:
            for p in (1, 0):
                send(kv_copy(p, near(1)[1]))
        for i in range(ZB // D):
            t = (scale * dqt[:, pl.ds(i * D, D)].T).astype(BF16)
            for k in range(D // RZ):
                m = i * (D // RZ) + k
                dqs[m128(zb, RZ), pl.ds(m * D, D)] = t[k * RZ:(k + 1) * RZ, :]

        @pl.when(zb != z)
        def _():
            d_copy(zb, z).start()

    for f in range(NK // FR):
        ktb[:, pl.ds(f * FR, FR)] = kb[pl.ds(f * FR, FR), :].astype(F32).T.astype(BF16)
    grads(0, NZ - 1 - core_z)
    landed(NZ - 3)
    grads(1, core_z)
    grads(2, NZ - 1 - brim)
    landed(NZ - 2)
    grads(3, brim)
    HW = JW // 2

    def half(u):
        return pl.ds(u * HW, HW)

    def a_copy(kind, u, z_to, z_from):
        here = dqall.at[j, m128(z_from, RZ), half(u)]
        return remote(here, here, as_.at[kind, u, z_to], ar.at[u, z_from], z_to * G + j)

    def a_own(u, act):
        @pl.when(inner)
        def _():
            for d in range(1, NZ):
                act(a_copy(0, u, far(d)[0], z))

        @pl.when(jnp.logical_not(inner))
        def _():
            act(a_copy(0, u, jnp.where(low, NZ - 2, 1), z))

    def a_onward(u, act):
        act(a_copy(1, u, NZ - 1 - z, brim))
        act(a_copy(1, u, NZ - 1 - brim, brim))

    QW = JW // 4

    def y_copy(u, j_from, peer, kind):
        here = dqall.at[j_from, :, pl.ds(u * QW, QW)]
        return remote(here, here, ys.at[kind, u], yr.at[kind, u], peer)

    def y_pass(u, frm, to):
        y_copy(u, near(frm)[0], me, frm - 1).wait_recv()
        send(y_copy(u, near(frm)[0], near(to)[1], 2))

    for c in local_x:
        c.wait()

    def piece(h, p, i):
        cols = pl.ds(p * D, D) if h else pl.ds(0, 2 * D)
        return m128(i, FB), cols, (2 + 2 * p + i if h else i)

    def c_copy(side, b, h, p, i, peer):
        at, cols, n = piece(h, p, i)
        return remote(part.at[h, b, at, cols], rin.at[side, b, h, at, cols], cs.at[b, n], cr.at[side, b, n], peer)

    def weigh(s, h, p):
        for i in range(2):
            at, cols, _ = piece(h, p, i)
            tmp[h * NZ + s, at, cols] = dot(vis[band(s), :, i * FB:(i + 1) * FB], kvn[p] if h else kv[...], TN)

    def gather(s):
        b = band(s)
        x_copy(1, b, x, near(2)[0], me).wait_recv()
        send(f_copy(1, b, True))
        pass_copy(b, near(3)[0], me).wait_recv()
        send(f_copy(2, b, True))
        for kind in range(3):
            f_copy(kind, b, False).wait_recv()

    def hop(s):
        b = band(s)
        side = (b < z).astype(jnp.int32)
        return b, side, jnp.where(b > z, low, high), (z + 1 - 2 * side) * G + j

    def first(s, h, p=0):
        weigh(s, h, p)
        b, side, fed, peer = hop(s)

        @pl.when(jnp.logical_not(fed))
        def _():
            for i in (1 - y, y):
                at, cols, _ = piece(h, p, i)
                part[h, b, at, cols] = tmp[h * NZ + s, at, cols].astype(BF16)
                c_copy(side, b, h, p, i, peer).start()

    def later(s, h, p=0):
        b, side, fed, peer = hop(s)

        @pl.when(fed)
        def _():
            for i in (1 - y, y):
                at, cols, _ = piece(h, p, i)
                c_copy(side, b, h, p, i, me).wait_recv()
                part[h, b, at, cols] = (tmp[h * NZ + s, at, cols] + rin[side, b, h, at, cols].astype(F32)).astype(BF16)
                c_copy(side, b, h, p, i, peer).start()

    def e_copy(h, p, peer):
        cols = piece(h, p, 0)[1]
        return remote(ybs.at[h, :, cols], ybr.at[h, :, cols], es.at[h + h * p], er.at[h + h * p], peer)

    outs = []

    def settle(head, slot, grads_of, grad):
        cols = m128(head, D)
        for n, a in enumerate(grads_of):
            wres[a, :, cols] = grad[:, n * D:(n + 1) * D]
            c = pltpu.make_async_copy(wres.at[a, :, cols], (kw_out, vw_out)[a].at[:, cols], ws.at[a, slot])
            c.start()
            outs.append(c)

    def finish(h, p=0):
        own = h * NZ + NZ - 1
        for i in (1 - y, y):
            at, cols, _ = piece(h, p, i)
            for side, there in ((0, low), (1, high)):
                @pl.when(there)
                def _():
                    c_copy(side, z, h, p, i, me).wait_recv()
                    tmp[own, at, cols] += rin[side, z, h, at, cols].astype(F32)
            if i is y:
                settle(j ^ h, h, (p,) if h else (0, 1), tmp[own, at, cols])
            else:
                ybs[h, :, cols] = tmp[own, at, cols].astype(BF16)
                send(e_copy(h, p, near(2)[1]))

    def summed_dq():
        mine = dqs[m128(z, RZ), :].astype(F32)
        for d in range(1, NZ):
            d_copy(z, far(d)[1]).wait_recv()
            mine += dqin[far(d)[1]].astype(F32)
        dqall[j, m128(z, RZ), :] = mine.astype(BF16)
        for u in range(2):
            a_own(u, lambda c: c.start())

    def relay_dq(u):
        @pl.when(inner)
        def _():
            a_copy(0, u, z, brim).wait_recv()
            a_onward(u, lambda c: c.start())

    def shared_dq():
        for u in range(2):
            for d in range(1, NZ):
                b = far(d)[1]

                @pl.when(jnp.logical_not(inner) | (b != brim))
                def _():
                    a_copy(0, u, z, b).wait_recv()
        for u in range(4):
            send(y_copy(u, j, near(1)[1], 0))
            send(y_copy((u + 1) % 4, j, near(2)[1], 1))

    gather(0)
    first(0, 0)
    landed(NZ - 1)
    summed_dq()
    gather(1)
    first(1, 0)
    later(0, 0)
    relay_dq(0)
    relay_dq(1)
    kv_copy(1, me).wait_recv()
    first(0, 1, 1)
    first(1, 1, 1)
    later(1, 0)
    gather(2)
    first(2, 0)
    shared_dq()
    first(2, 1, 1)
    later(0, 1, 1)
    gather(3)
    kv_copy(0, me).wait_recv()
    for s in range(NZ - 1):
        first(s, 1, 0)
    later(1, 1, 1)
    later(2, 0)
    weigh(3, 0, 0)
    weigh(3, 1, 1)
    weigh(3, 1, 0)

    def put(i):
        c = pltpu.make_async_copy(dqall.at[j ^ i], q_out.at[:, m128(j ^ i, JW)], loc.at[i])
        c.start()
        outs.append(c)

    put(0)
    y_pass(0, 1, 2)
    y_pass(1, 2, 1)
    later(2, 1, 1)
    finish(0)
    later(0, 1, 0)
    y_pass(2, 2, 1)
    y_pass(3, 2, 1)
    later(1, 1, 0)
    later(2, 1, 0)
    for u in range(1, 4):
        y_copy(u, near(1)[0], me, 0).wait_recv()
    put(1)
    y_copy(0, near(2)[0], me, 1).wait_recv()
    put(2)
    finish(1, 1)
    finish(1, 0)
    for u in range(4):
        y_copy(u, near(3)[0], me, 2).wait_recv()
    put(3)
    for h, p, grads_of in ((0, 0, (0, 1)), (1, 1, (1,)), (1, 0, (0,))):
        e_copy(h, p, me).wait_recv()
        settle(j ^ (2 + h), 2 + h, grads_of, ybr[h, :, piece(h, p, 0)[1]].astype(F32))
    for c in outs:
        c.wait()
    for c in sends:
        c.wait_send()
    for k in range(NZ):
        zq_each(lambda c: c.wait_send(), band(NZ - 1 - k), False)
    for u in range(2):
        a_own(u, lambda c: c.wait_send())
        pl.when(inner)(lambda: a_onward(u, lambda c: c.wait_send()))
    for s in range(NZ - 1):
        b, side, fed, peer = hop(s)
        for h, p in ((0, 0), (1, 0), (1, 1)):
            for i in range(2):
                c_copy(side, b, h, p, i, peer).wait_send()
    for d in range(1, NZ):
        d_copy(far(d)[0], z).wait_send()
    for zb in range(NZ):
        for d in range(1, NZ):
            s_copy(zb, far(d)[0], z, far(d)[2]).wait_send()


def deliver_kernel(parts, *refs):
    n = len(parts)
    srcs, dsts, bufs, ins, outs = refs[:n], refs[n:2 * n], refs[2 * n:3 * n], refs[3 * n], refs[3 * n + 1]
    moves, k = [], 0
    for src, dst, buf, p in zip(srcs, dsts, bufs, parts):
        step = src.shape[0] // p
        for i in range(p):
            at = pl.ds(i * step, step)
            moves.append((pltpu.make_async_copy(src.at[at], buf.at[at], ins.at[k]),
                          pltpu.make_async_copy(buf.at[at], dst.at[at], outs.at[k])))
            k += 1
    for a, _ in moves:
        a.start()
    for a, b in moves:
        a.wait()
        b.start()
    for _, b in moves:
        b.wait()


def deliver(*arrays):
    parts = [8, 2, 2]
    anyspec = pl.BlockSpec(memory_space=pl.ANY)
    return pl.pallas_call(
        functools.partial(deliver_kernel, parts),
        out_shape=[jax.ShapeDtypeStruct(a.shape, a.dtype) for a in arrays],
        in_specs=[anyspec] * len(arrays),
        out_specs=[anyspec] * len(arrays),
        scratch_shapes=[pltpu.VMEM(a.shape, a.dtype) for a in arrays]
        + [pltpu.SemaphoreType.DMA((sum(parts),)), pltpu.SemaphoreType.DMA((sum(parts),))],
        compiler_params=pltpu.CompilerParams(vmem_limit_bytes=67043328),
    )(*arrays)


def plane_shards(T, text_queries, text_grads, vision_keys, video_value_rows, vision, lengths, frame_range):
    R, QW = text_queries.shape
    rows, kv_width = vision_keys.shape
    G = kv_width // HEAD_WIDTH
    M = QW // kv_width
    NZ = T // G
    DW = vision.shape[1]
    FB = DW // T
    NK, RZ, JW = G * rows, G * R, M * HEAD_WIDTH
    NR = T * R * M
    cfg = dict(G=G, NZ=NZ, M=M, R=R, FR=rows // FRAME_DEV, NC=4, rows=rows, NK=NK, NR=NR, JW=JW, FB=FB, RZ=RZ,
               NS=lengths.shape[0])
    anyspec = pl.BlockSpec(memory_space=pl.ANY)
    vm = pl.BlockSpec(memory_space=pltpu.VMEM)
    V = pltpu.VMEM
    D = pltpu.SemaphoreType.DMA
    W2 = 2 * HEAD_WIDTH
    pairs = []
    for a, b in (((2, G),) * 2, ((2, 2, NZ), (2, NZ)), ((2, G),) * 2, ((3, NZ),) * 2, ((3, NZ),) * 2, ((NZ, NZ),) * 2, ((2,),) * 2,
                 ((NZ,),) * 2, ((2, 2, NZ), (2, NZ)), ((3, 4),) * 2, ((NZ, 6), (2, NZ, 6)), ((3,),) * 2):
        pairs += [D(a), D(b)]
    q_grad, kw, vw = pl.pallas_call(
        functools.partial(plane_kernel, cfg),
        out_shape=(
            jax.ShapeDtypeStruct((T * R, QW), BF16),
            jax.ShapeDtypeStruct((FB, kv_width), F32),
            jax.ShapeDtypeStruct((FB, kv_width), F32),
        ),
        in_specs=[anyspec] * 7,
        out_specs=(anyspec,) * 3,
        scratch_shapes=[
            V((T * R, JW), BF16), V((T * R, JW), BF16),
            V((NR, HEAD_WIDTH), BF16), V((NR, HEAD_WIDTH), BF16),
            V((NK, HEAD_WIDTH), BF16), V((NK, HEAD_WIDTH), BF16),
            V((NZ, NK, 2 * FB), BF16),
            V((NK, NR), F32), V((NK, NR), F32),
            V((8, NR), F32), V((NZ, 8, NR), F32), V((8, NR), F32), V((8, NR), jnp.int32),
            V((NK, W2), BF16), V((2, NK, HEAD_WIDTH), BF16),
            V((HEAD_WIDTH, M * RZ), F32), V((T * R, JW), BF16),
            V((NZ, RZ, JW), BF16), V((G, T * R, JW), BF16),
            V((G, 8, NR), F32), V((HEAD_WIDTH, NK), BF16),
            V((2, FB, kv_width), F32), D((2, 4)),
            pltpu.SMEM(lengths.shape, jnp.int32), pltpu.SMEM(frame_range.shape[::-1], jnp.int32),
            V((2 * NZ, 2 * FB, W2), F32), V((2, NZ, 2 * FB, W2), BF16), V((2, NZ, 2, 2 * FB, W2), BF16),
            V((2, FB, W2), BF16), V((2, FB, W2), BF16),
            D((6,)), D((NZ, 2)),
        ] + pairs,
        compiler_params=pltpu.CompilerParams(
            collective_id=0, has_side_effects=True, vmem_limit_bytes=67043328
        ),
    )(text_queries, text_grads, vision_keys, video_value_rows, vision, lengths, frame_range.T)
    return deliver(q_grad, kw, vw)


def solution(mesh):
    return jax.shard_map(
        functools.partial(shards, mesh.shape["tok"], mesh.shape["head"]),
        mesh=mesh,
        in_specs=(
            P("tok", "head"),
            P("tok", "head"),
            P("tok", "head"),
            P("tok", "head"),
            P("tok", None),
            P(),
            P(),
        ),
        out_specs=(P(None, "head"), P("tok", "head"), P("tok", "head")),
        check_vma=False,
    )
```

```python
import functools

import jax
import jax.numpy as jnp
from jax import lax
from jax.experimental import pallas as pl
from jax.experimental.pallas import tpu as pltpu
from jax.sharding import PartitionSpec as P

HEAD_WIDTH = 128
FRAME_DEV = 4
NEG_FILL = -1e30
NT = (((1,), (1,)), ((), ()))
TN = (((0,), (0,)), ((), ()))
F32 = jnp.float32
BF16 = jnp.bfloat16


def dot(a, b, dims=(((1,), (0,)), ((), ()))):
    return lax.dot_general(a, b, dims, preferred_element_type=F32)


def kernel(cfg, q_in, g_in, k_in, v_in, x_in, bounds, q_out, kw_out, vw_out,
           qb, gb, kb, vb, vis, ebuf, dpb, stat, stin, coef, kv, dqt, dqs, dqin, dqall, part, rsb,
           loc, qs, qr, gs, gr, ks, kr, vs, vr, xs, xr, ss, sr, kvs, kvr, ds, dr, as_, ar, ys, yr, rs, rr, fs, fr):
    T, G, NZ = cfg["T"], cfg["G"], cfg["NZ"]
    blk, rows, NK, NR, FR = cfg["blk"], cfg["rows"], cfg["NK"], cfg["NR"], cfg["FR"]
    W, NV, FB = cfg["W"], cfg["NV"], cfg["FB"]
    H = cfg["H"]
    RB = cfg["RB"]
    scale = HEAD_WIDTH ** (-0.5)
    me = lax.axis_index("tok")
    z, j0 = me // G, me % G

    def remote(src, dst, s, r, peer):
        return pltpu.make_async_remote_copy(
            src_ref=src, dst_ref=dst, send_sem=s, recv_sem=r,
            device_id={"tok": peer}, device_id_type=pl.DeviceIdType.MESH)

    def m128(i, n):
        return pl.ds(pl.multiple_of(i * n, n), n)

    barrier = pltpu.get_barrier_semaphore()
    for d in range(1, T):
        pl.semaphore_signal(barrier, inc=1, device_id={"tok": lax.rem(me + d, T)}, device_id_type=pl.DeviceIdType.MESH)
    twin = lax.axis_index("head")
    if H > 1:
        twin = 1 - twin
        pl.semaphore_signal(barrier, inc=1, device_id={"head": twin}, device_id_type=pl.DeviceIdType.MESH)
    pl.semaphore_wait(barrier, T - 1 + (H > 1))

    def tpeer(d):
        return lax.rem(me + d, T), lax.rem(me + T - d, T)

    def gpeer(d):
        a, b = (j0 ^ d, j0 ^ d) if G & (G - 1) == 0 else (lax.rem(j0 + d, G), lax.rem(j0 + G - d, G))
        return a, b, z * G + a, z * G + b

    def zpeer(d):
        a, b = lax.rem(z + d, NZ), lax.rem(z + NZ - d, NZ)
        return a, b, a * G + j0, b * G + j0

    sends = []

    def send(c):
        c.start()
        sends.append(c)

    def q_copy(t_to, t_from):
        return (remote(q_in.at[lax.rem(t_to, G)], qb.at[m128(t_from, blk)], qs.at[t_to], qr.at[t_from], t_to),
                remote(g_in.at[lax.rem(t_to, G)], gb.at[m128(t_from, blk)], gs.at[t_to], gr.at[t_from], t_to))

    def k_copy(j_to, j_from, peer):
        return (remote(k_in.at[:, m128(j_to, 128)], kb.at[m128(j_from, rows)], ks.at[j_to], kr.at[j_from], peer),
                remote(v_in.at[:, m128(j_to, 128)], vb.at[m128(j_from, rows)], vs.at[j_to], vr.at[j_from], peer))

    WH = W // H
    half = lax.axis_index("head") * WH if H > 1 else 0

    def x_copy(b, j_to, j_from, peer):
        cols = pl.ds(pl.multiple_of((b * G + j_to) * W + half, WH), WH)
        dst = vis.at[b, m128(j_from, rows), pl.ds(pl.multiple_of(half, WH), WH)]
        return remote(x_in.at[:, cols], dst, xs.at[j_to, b], xr.at[j_from, b], peer)

    def f_copy(b, j_from, mine):
        at = half if mine else WH - half
        here = vis.at[b, m128(j_from, rows), pl.ds(pl.multiple_of(at, WH), WH)]
        return pltpu.make_async_remote_copy(
            src_ref=here, dst_ref=here, send_sem=fs.at[j_from, b], recv_sem=fr.at[j_from, b],
            device_id={"head": twin}, device_id_type=pl.DeviceIdType.MESH)

    local = [
        pltpu.make_async_copy(q_in.at[j0], qb.at[m128(me, blk)], loc.at[0]),
        pltpu.make_async_copy(g_in.at[j0], gb.at[m128(me, blk)], loc.at[1]),
        pltpu.make_async_copy(k_in.at[:, m128(j0, 128)], kb.at[m128(j0, rows)], loc.at[2]),
        pltpu.make_async_copy(v_in.at[:, m128(j0, 128)], vb.at[m128(j0, rows)], loc.at[3]),
    ]
    local_x = [pltpu.make_async_copy(x_in.at[:, m128(b * G + j0, W)], vis.at[b, m128(j0, rows)], loc.at[4 + b]) for b in range(NV)]
    for c in local:
        c.start()
    def q_sends(zd):
        a, _, _, _ = zpeer(zd)
        for i in range(G):
            to = a * G + (lax.rem(j0 + i, G) if zd else gpeer(i)[0])
            if zd or i:
                for c in q_copy(to, me):
                    send(c)

    q_sends(0)
    for d in range(1, G):
        a, _, peer, _ = gpeer(d)
        for c in k_copy(a, j0, peer):
            send(c)
    for d in range(1, NZ):
        q_sends(d)
    for c in local_x:
        c.start()
    for c in local:
        c.wait()
    for d in range(1, G):
        _, b, _, _ = gpeer(d)
        for c in k_copy(j0, b, me):
            c.wait_recv()

    def q_wait(zd):
        _, b, _, _ = zpeer(zd)
        for i in range(G):
            if zd or i:
                frm = b * G + (i if zd else gpeer(i)[1])
                for c in q_copy(me, frm):
                    c.wait_recv()

    n_frames = NK // FR
    frame0 = z * n_frames
    stat[0:1, :] = jnp.full((1, NR), NEG_FILL, F32)
    stat[1:8, :] = jnp.zeros((7, NR), F32)

    def totals(cols, width):
        first, end = bounds[0:1, cols], bounds[1:2, cols]
        UN = 2 if n_frames % 2 == 0 else 1

        def scored(i, top):
            for u in range(UN):
                f = i * UN + u
                ok = (first <= frame0 + f) & (frame0 + f < end)
                s = jnp.where(ok, dot(kb[m128(f, FR), :], qb[cols, :], NT) * scale, NEG_FILL)
                ebuf[m128(f, FR), cols] = s
                top = jnp.maximum(top, jnp.max(s, axis=0, keepdims=True))
            return top

        top = lax.fori_loop(0, n_frames // UN, scored, jnp.full((1, width), NEG_FILL, F32))

        def summed(i, carry):
            total, dotted = carry
            for u in range(UN):
                f = i * UN + u
                dp = dot(vb[m128(f, FR), :], gb[cols, :], NT)
                e = jnp.exp(ebuf[m128(f, FR), cols] - top)
                ebuf[m128(f, FR), cols] = e
                dpb[m128(f, FR), cols] = dp
                total += jnp.sum(e, axis=0, keepdims=True)
                dotted += jnp.sum(e * dp, axis=0, keepdims=True)
            return total, dotted

        zero = jnp.zeros((1, width), F32)
        total, dotted = lax.fori_loop(0, n_frames // UN, summed, (zero, zero))
        stat[0:1, cols] = top
        stat[1:2, cols] = total
        stat[2:3, cols] = dotted

    def x_sends():
        for d in range(1, G):
            a, _, peer, _ = gpeer(d)
            for b in range(NV):
                send(x_copy(b, a, j0, peer))

    by_z = (NR // NZ) % 128 == 0
    for d in range(NZ):
        q_wait(d)
        if d == NZ - 1:
            x_sends()
        if by_z:
            totals(m128(zpeer(d)[1], NR // NZ), NR // NZ)
    if not by_z:
        for r in range(0, NR, RB):
            totals(pl.ds(r, RB), RB)

    def s_copy(z_to, z_from, peer):
        return remote(stat, stin.at[z_from], ss.at[z_to], sr.at[z_from], peer)

    for d in range(1, NZ):
        a, _, peer, _ = zpeer(d)
        send(s_copy(a, z, peer))
    stin[z] = stat[...]
    for d in range(1, NZ):
        _, b, _, _ = zpeer(d)
        s_copy(z, b, me).wait_recv()
    top = stat[0:1, :]
    for i in range(NZ):
        top = jnp.maximum(top, stin[i, 0:1, :])
    total = jnp.zeros((1, NR), F32)
    dotted = jnp.zeros((1, NR), F32)
    for i in range(NZ):
        w = jnp.exp(stin[i, 0:1, :] - top)
        total += w * stin[i, 1:2, :]
        dotted += w * stin[i, 2:3, :]
    coef[0:1, :] = jnp.exp(stat[0:1, :] - top) / total
    coef[1:2, :] = dotted / total
    dqt[...] = jnp.zeros_like(dqt)

    NC = cfg["NC"]
    CH = NK // NC

    def kv_copy(c, j_to, j_from, peer):
        here = kv.at[j_from, pl.ds(c * CH, CH)]
        return remote(here, here, kvs.at[j_to, c], kvr.at[j_from, c], peer)

    for c in range(NC):
        @pl.loop(c * (CH // FR), (c + 1) * (CH // FR))
        def _(f):
            kt = kb[m128(f, FR), :].astype(F32).T.astype(BF16)
            dk = jnp.zeros((FR, HEAD_WIDTH), F32)
            dv = jnp.zeros((FR, HEAD_WIDTH), F32)
            for r in range(0, NR, RB):
                cols = pl.ds(r, RB)
                p = ebuf[m128(f, FR), cols] * coef[0:1, cols]
                t = (p * (dpb[m128(f, FR), cols] - coef[1:2, cols])).astype(BF16)
                dv += dot(p.astype(BF16), gb[cols, :])
                dk += dot(t, qb[cols, :])
                dqt[:, cols] += dot(kt, t)
            kv[j0, m128(f, FR), 0:HEAD_WIDTH] = (scale * dk).astype(BF16)
            kv[j0, m128(f, FR), HEAD_WIDTH:2 * HEAD_WIDTH] = dv.astype(BF16)

        for d in range(1, G - 1):
            a, _, peer, _ = gpeer(d)
            kv_copy(c, a, j0, peer).start()
        if H > 1 and c == NC // 2:
            for d in range(1, G):
                _, b, _, _ = gpeer(d)
                for i in range(NV):
                    x_copy(i, j0, b, me).wait_recv()
                    send(f_copy(i, b, True))

    for r in range(0, NR, 128):
        dqs[pl.ds(r, 128), :] = (scale * dqt[:, pl.ds(r, 128)].T).astype(BF16)
    QR = NR // NZ

    def d_copy(z_to, z_from, peer):
        return remote(dqs.at[m128(z_to, QR)], dqin.at[z_from], ds.at[z_to], dr.at[z_from], peer)

    def a_copy(z_to, z_from, peer):
        here = dqall.at[j0, m128(z_from, QR)]
        return remote(here, here, as_.at[z_to], ar.at[z_from], peer)

    def y_copy(j_to, j_from, peer):
        here = dqall.at[j_from]
        return remote(here, here, ys.at[j_to], yr.at[j_from], peer)

    def r_copy(j, z_to, z_from, peer):
        return remote(part.at[j, m128(z_to, FB)], rsb.at[z_from, j], rs.at[j, z_to], rr.at[j, z_from], peer)

    for d in range(1, NZ):
        a, _, peer, _ = zpeer(d)
        send(d_copy(a, z, peer))
    for c in local_x:
        c.wait()
    for d in range(1, G):
        _, b, _, _ = gpeer(d)
        for i in range(NV):
            (f_copy(i, b, False) if H > 1 else x_copy(i, j0, b, me)).wait_recv()

    def weigh(j):
        @pl.loop(0, NV)
        def _(b):
            part[j, m128(b, W), :] = dot(vis[b], kv[j], TN).astype(BF16)
        for d in range(1, NZ):
            a, _, peer, _ = zpeer(d)
            send(r_copy(j, a, z, peer))

    weigh(j0)
    mine = dqs[m128(z, QR), :].astype(F32)
    for d in range(1, NZ):
        _, b, _, _ = zpeer(d)
        d_copy(z, b, me).wait_recv()
        mine += dqin[b].astype(F32)
    dqall[j0, m128(z, QR), :] = mine.astype(BF16)
    for d in range(1, NZ):
        a, _, peer, _ = zpeer(d)
        send(a_copy(a, z, peer))

    def spread():
        for d in range(1, NZ):
            _, b, _, _ = zpeer(d)
            a_copy(z, b, me).wait_recv()
        for d in range(1, G):
            a, _, peer, _ = gpeer(d)
            send(y_copy(a, j0, peer))

    for d in range(1, G - 1):
        a, _, peer, _ = gpeer(d)
        for c in range(NC):
            kv_copy(c, a, j0, peer).wait_send()
    if G > 1:
        a, _, peer, _ = gpeer(G - 1)
        for c in range(NC):
            send(kv_copy(c, a, j0, peer))
    if G == 1:
        spread()
    for d in range(1, G):
        _, b, _, _ = gpeer(d)
        for c in range(NC):
            kv_copy(c, j0, b, me).wait_recv()
        weigh(b)
        if d == min(2, G - 1):
            spread()
    for d in range(1, G):
        _, b, _, _ = gpeer(d)
        y_copy(j0, b, me).wait_recv()
    out_copy = pltpu.make_async_copy(dqall, q_out, loc.at[0])
    out_copy.start()

    for d in range(1, NZ):
        _, b, _, _ = zpeer(d)
        for j in range(G):
            r_copy(j, z, b, me).wait_recv()
    for j in range(G):
        acc = part[j, m128(z, FB), :].astype(F32)
        for d in range(1, NZ):
            _, b, _, _ = zpeer(d)
            acc += rsb[b, j].astype(F32)
        kw_out[:, pl.ds(j * HEAD_WIDTH, HEAD_WIDTH)] = acc[:, 0:HEAD_WIDTH]
        vw_out[:, pl.ds(j * HEAD_WIDTH, HEAD_WIDTH)] = acc[:, HEAD_WIDTH:]
    out_copy.wait()
    for c in sends:
        c.wait_send()


def shards(T, cores, text_queries, text_grads, vision_keys, video_value_rows, vision, lengths, frame_range):
    R, QW = text_queries.shape
    rows, kv_width = vision_keys.shape
    G = kv_width // HEAD_WIDTH
    if cores == 2 and G == 4 and T == G * G and vision.shape[1] % (T * 128) == 0 and HEAD_WIDTH % (G * R) == 0 and 2 * vision.shape[1] == T * rows:
        return plane_shards(T, text_queries, text_grads, vision_keys, video_value_rows, vision, lengths, frame_range)
    M = QW // kv_width
    NZ = T // G
    DW = vision.shape[1]
    blk, NK, NR = M * R, G * rows, T * M * R
    FB = DW // T
    W = FB if FB % 128 == 0 else 256
    NV = DW // (G * W)
    FR = rows // FRAME_DEV
    NC = 4 if NK >= 16 * FR else 1
    cfg = dict(T=T, G=G, NZ=NZ, blk=blk, rows=rows, NK=NK, NR=NR, FR=FR, W=W, NV=NV, FB=FB, NC=NC, RB=min(NR, 512),
               H=2 if cores == 2 and G > 1 and W % 256 == 0 else 1)

    text_len = R * T
    row_ids = jnp.arange(text_len, dtype=jnp.int32)
    segment_ends = jnp.cumsum(lengths)
    segment = jnp.sum((row_ids[:, None] >= segment_ends[None, :]).astype(jnp.int32), axis=1)
    segment_pick = (
        segment[:, None] == jnp.arange(lengths.shape[0], dtype=jnp.int32)[None, :]
    ).astype(jnp.int32)
    bounds = jnp.sum(segment_pick[None] * frame_range.T[:, None, :], axis=2)
    bounds = jnp.broadcast_to(bounds.reshape(2, T, 1, R), (2, T, M, R)).reshape(2, NR)

    def split(a):
        return a.reshape(R, G, M, HEAD_WIDTH).transpose(1, 2, 0, 3).reshape(G, blk, HEAD_WIDTH)

    anyspec = pl.BlockSpec(memory_space=pl.ANY)
    vm = pl.BlockSpec(memory_space=pltpu.VMEM)
    V = pltpu.VMEM
    D = pltpu.SemaphoreType.DMA
    sem_pairs = []
    for shape in ((T,), (T,), (G,), (G,), (G, NV), (NZ,), (G, NC), (NZ,), (NZ,), (G,), (G, NZ), (G, NV)):
        sem_pairs += [D(shape), D(shape)]
    q_grad, kw, vw = pl.pallas_call(
        functools.partial(kernel, cfg),
        out_shape=(
            jax.ShapeDtypeStruct((G, NR, HEAD_WIDTH), BF16),
            jax.ShapeDtypeStruct((FB, kv_width), F32),
            jax.ShapeDtypeStruct((FB, kv_width), F32),
        ),
        in_specs=[anyspec] * 5 + [vm],
        out_specs=(anyspec, vm, vm),
        scratch_shapes=[
            V((NR, HEAD_WIDTH), BF16), V((NR, HEAD_WIDTH), BF16),
            V((NK, HEAD_WIDTH), BF16), V((NK, HEAD_WIDTH), BF16),
            V((NV, NK, W), BF16),
            V((NK, NR), F32), V((NK, NR), F32),
            V((8, NR), F32), V((NZ, 8, NR), F32), V((8, NR), F32),
            V((G, NK, 2 * HEAD_WIDTH), BF16),
            V((HEAD_WIDTH, NR), F32), V((NR, HEAD_WIDTH), BF16),
            V((NZ, NR // NZ, HEAD_WIDTH), BF16), V((G, NR, HEAD_WIDTH), BF16),
            V((G, DW // G, 2 * HEAD_WIDTH), BF16),
            V((NZ, G, FB, 2 * HEAD_WIDTH), BF16),
            D((4 + NV,)),
        ] + sem_pairs,
        compiler_params=pltpu.CompilerParams(
            collective_id=0, has_side_effects=True, vmem_limit_bytes=67043328
        ),
    )(split(text_queries), split(text_grads), vision_keys, video_value_rows, vision, bounds)
    q_grad = q_grad.reshape(G, T, M, R, HEAD_WIDTH).transpose(1, 3, 0, 2, 4).reshape(text_len, QW)
    return q_grad, kw, vw


def plane_kernel(cfg, q_in, g_in, k_in, v_in, x_in, lens_in, frames_in, q_out, kw_out, vw_out,
                 qraw, graw, qb, gb, kb, vb, vis, ebuf, dpb, stat, stin, coef, lim, kv, kvn, dqt, dqs, dqin,
                 gst, ktb, lens, frames, tmp, part, rin, ybs, ybr, loc, lx, qs, qr, zs, zr, ks, kr, xs, xr, fs, fr, ss, sr, kvs, kvr,
                 ds, dr, as_, ar, ys, yr, cs, cr, es, er):
    G, NZ, M, R, FR, NC = cfg["G"], cfg["NZ"], cfg["M"], cfg["R"], cfg["FR"], cfg["NC"]
    rows, NK, NR, JW, FB, RZ = cfg["rows"], cfg["NK"], cfg["NR"], cfg["JW"], cfg["FB"], cfg["RZ"]
    D = HEAD_WIDTH
    ZB = M * RZ
    scale = D ** (-0.5)
    me = lax.axis_index("tok")
    core = lax.axis_index("head")
    z, j = me // G, me % G
    y, x = j // 2, j % 2

    def m128(i, n):
        return pl.ds(pl.multiple_of(i * n, n), n)

    def remote(src, dst, s, r, peer):
        return pltpu.make_async_remote_copy(
            src_ref=src, dst_ref=dst, send_sem=s, recv_sem=r,
            device_id={"tok": peer}, device_id_type=pl.DeviceIdType.MESH)

    def near(d):
        return j ^ d, z * G + (j ^ d)

    def far(d):
        a, b = lax.rem(z + d, NZ), lax.rem(z + NZ - d, NZ)
        return a, b, a * G + j, b * G + j

    mirror = 2 * z > NZ - 1
    zz = jnp.where(mirror, NZ - 1 - z, z)

    def band(s):
        u = s - (NZ - 1 - 2 * zz)
        k, odd = u // 2, u % 2
        b = jnp.where(u < 0, NZ - 1 - s, k + odd * (2 * zz - 2 * k))
        return jnp.where(mirror, NZ - 1 - b, b)

    barrier = pltpu.get_barrier_semaphore()
    for d in range(1, G):
        pl.semaphore_signal(barrier, inc=1, device_id={"tok": near(d)[1]}, device_id_type=pl.DeviceIdType.MESH)
    for d in range(1, NZ):
        pl.semaphore_signal(barrier, inc=1, device_id={"tok": far(d)[2]}, device_id_type=pl.DeviceIdType.MESH)
    pl.semaphore_signal(barrier, inc=1, device_id={"head": 1 - core}, device_id_type=pl.DeviceIdType.MESH)
    pl.semaphore_wait(barrier, G + NZ - 1)

    sends = []

    def send(c):
        c.start()
        sends.append(c)

    def own_rows(t):
        return m128(t, R)

    def q_copy(d, t_from, peer, j_to):
        cols = m128(j_to, JW)
        return (remote(q_in.at[:, cols], qraw.at[own_rows(t_from)], qs.at[0, d], qr.at[0, d], peer),
                remote(g_in.at[:, cols], graw.at[own_rows(t_from)], qs.at[1, d], qr.at[1, d], peer))

    low, high = z > 0, z < NZ - 1
    inner = low & high

    def zq_copy(side, a, b):
        here = (qraw, graw)[a].at[m128(b, RZ)]
        return remote(here, here, zs.at[side, a, b], zr.at[a, b], (z + 1 - 2 * side) * G + j)

    def zq_each(act, b, into, which=(0, 1)):
        for a in which:
            if into:
                zq_copy(0, a, b).wait_recv()

            @pl.when(high & (b <= z))
            def _():
                act(zq_copy(0, a, b))

            @pl.when(low & (b >= z))
            def _():
                act(zq_copy(1, a, b))

    def k_copy(d, j_to, j_from, peer):
        return (remote(k_in.at[:, m128(j_to, D)], kb.at[m128(j_from, rows)], ks.at[0, d], kr.at[0, d], peer),
                remote(v_in.at[:, m128(j_to, D)], vb.at[m128(j_from, rows)], ks.at[1, d], kr.at[1, d], peer))

    def lane_half(mine):
        return m128(core if mine else 1 - core, FB)

    def x_copy(kind, b, x_to, j_from, peer):
        cols = m128(b * G + core * 2 + x_to, FB)
        dst = vis.at[b, m128(j_from, rows), lane_half(True)]
        return remote(x_in.at[:, cols], dst, xs.at[kind, b], xr.at[kind, b], peer)

    def pass_copy(b, j_from, peer):
        here = vis.at[b, m128(j_from, rows), lane_half(True)]
        return remote(here, here, xs.at[2, b], xr.at[2, b], peer)

    def f_copy(kind, b, mine):
        here = vis.at[b, m128(j ^ (kind + 1), rows), lane_half(mine)]
        return pltpu.make_async_remote_copy(
            src_ref=here, dst_ref=here, send_sem=fs.at[kind, b], recv_sem=fr.at[kind, b],
            device_id={"head": 1 - core}, device_id_type=pl.DeviceIdType.MESH)

    local = [
        pltpu.make_async_copy(q_in.at[:, m128(j, JW)], qraw.at[own_rows(me)], loc.at[0]),
        pltpu.make_async_copy(g_in.at[:, m128(j, JW)], graw.at[own_rows(me)], loc.at[1]),
        pltpu.make_async_copy(k_in.at[:, m128(j, D)], kb.at[m128(j, rows)], loc.at[2]),
        pltpu.make_async_copy(v_in.at[:, m128(j, D)], vb.at[m128(j, rows)], loc.at[3]),
        pltpu.make_async_copy(lens_in, lens, loc.at[4]),
        pltpu.make_async_copy(frames_in, frames, loc.at[5]),
    ]
    for c in local:
        c.start()
    for d in range(G - 1, 0, -1):
        for c in q_copy(d, me, near(d)[1], near(d)[0]):
            send(c)
    for d in range(1, G):
        for c in k_copy(d, near(d)[0], j, near(d)[1]):
            send(c)
    local_x = []
    for b in range(NZ):
        for h in range(2):
            local_x.append(pltpu.make_async_copy(
                x_in.at[:, m128(b * G + 2 * h + x, FB)], vis.at[b, m128(j, rows), pl.ds(h * FB, FB)], lx.at[b, h]))

    for c in local[4:]:
        c.wait()
    col = lax.broadcasted_iota(jnp.int32, (1, NR), 1)
    text = (col // ZB) * RZ + col % RZ
    seg = jnp.zeros((1, NR), jnp.int32)
    end = jnp.int32(0)
    NS = cfg["NS"]
    for i in range(NS):
        end = end + lens[i]
        seg += (text >= end).astype(jnp.int32)
    first, last = jnp.zeros((1, NR), jnp.int32), jnp.zeros((1, NR), jnp.int32)
    for i in range(NS):
        first = jnp.where(seg == i, frames[0, i], first)
        last = jnp.where(seg == i, frames[1, i], last)
    lim[0:1, :] = first
    lim[1:2, :] = last
    stat[0:8, :] = jnp.zeros((8, NR), F32)

    for c in local[:2]:
        c.wait()
    for d in range(1, G):
        for c in q_copy(d, z * G + near(d)[0], me, j):
            c.wait_recv()
    zq_each(lambda c: c.start(), z, False)
    for s in range(NZ):
        send(x_copy(0, band(s), 1 - x, j, near(1)[1]))
        if s < NZ // 2:
            send(x_copy(1, band(s), x, j, near(2)[1]))
    for c in local_x:
        c.start()
    for c in local[2:4]:
        c.wait()

    n_frames = rows // FR

    def tokens(g, f):
        return m128(g * n_frames + f, FR)

    def scored(g, zb):
        cols = m128(zb, ZB)
        lo, hi = lim[0:1, cols], lim[1:2, cols]
        base = z * G * n_frames + g * n_frames
        top = jnp.full((1, ZB), NEG_FILL, F32)
        for f in range(n_frames):
            ok = (lo <= base + f) & (base + f < hi)
            sc = jnp.where(ok, dot(kb[tokens(g, f), :], qb[cols, :], NT) * scale, NEG_FILL)
            ebuf[tokens(g, f), cols] = sc
            top = jnp.maximum(top, jnp.max(sc, axis=0, keepdims=True))
        gst[g, 0:1, cols] = top

    def summed(g, zb):
        cols = m128(zb, ZB)
        top = gst[g, 0:1, cols]
        total = jnp.zeros((1, ZB), F32)
        dotted = jnp.zeros((1, ZB), F32)
        for f in range(n_frames):
            dp = dot(vb[tokens(g, f), :], gb[cols, :], NT)
            e = jnp.exp(ebuf[tokens(g, f), cols] - top)
            ebuf[tokens(g, f), cols] = e
            dpb[tokens(g, f), cols] = dp
            total += jnp.sum(e, axis=0, keepdims=True)
            dotted += jnp.sum(e * dp, axis=0, keepdims=True)
        gst[g, 1:2, cols] = total
        gst[g, 2:3, cols] = dotted

    def s_copy(zb, z_to, z_from, peer):
        cols = m128(zb, ZB)
        return remote(stat.at[:, cols], stin.at[z_from, :, cols], ss.at[zb, z_to], sr.at[zb, z_from], peer)

    def plane_totals(zb):
        cols = m128(zb, ZB)
        top = gst[0, 0:1, cols]
        for g in range(1, G):
            top = jnp.maximum(top, gst[g, 0:1, cols])
        total = jnp.zeros((1, ZB), F32)
        dotted = jnp.zeros((1, ZB), F32)
        for g in range(G):
            w = jnp.exp(gst[g, 0:1, cols] - top)
            total += w * gst[g, 1:2, cols]
            dotted += w * gst[g, 2:3, cols]
        stat[0:1, cols] = top
        stat[1:2, cols] = total
        stat[2:3, cols] = dotted
        for d in range(1, NZ):
            s_copy(zb, far(d)[0], z, far(d)[2]).start()

    def landed(s):
        b = band(s)
        x_copy(0, b, x, near(1)[0], me).wait_recv()
        send(pass_copy(b, near(1)[0], near(2)[1]))
        if s < NZ // 2:
            send(x_copy(1, band(s + NZ // 2), x, j, near(2)[1]))
        send(f_copy(0, b, True))

    have_g, have_z = {0}, set()

    def arrive(k, which=(0, 1)):
        zq_each(lambda c: c.start(), band(NZ - 1 - k), True, which)

    def head_rows(zb, which=(0, 1)):
        for a in which:
            raw, buf = (qraw, graw)[a], (qb, gb)[a]
            for m in range(M):
                buf[m128(zb * M + m, RZ), :] = raw[m128(zb, RZ), m * D:(m + 1) * D]

    def block(d, k):
        zb = band(NZ - 1 - k)
        if d not in have_g:
            have_g.add(d)
            for c in k_copy(d, j, near(d)[0], me):
                c.wait_recv()
        if k not in have_z:
            have_z.add(k)
            if k:
                pl.when(jnp.logical_not(inner))(lambda: arrive(k))
            head_rows(zb)
        scored(j ^ d, zb)
        summed(j ^ d, zb)

    def last_block(k, waits):
        zb = band(NZ - 1 - k)
        for a, work in ((0, scored), (1, summed)):
            if waits:
                arrive(k, (a,))
            head_rows(zb, (a,))
            for d in range(G):
                work(j ^ d, zb)
        plane_totals(zb)

    block(0, 0)
    block(1, 0)

    @pl.when(inner)
    def _():
        arrive(1)
        arrive(2)
    for d, k in ((2, 0), (0, 1), (1, 1), (2, 1)):
        block(d, k)

    @pl.when(inner)
    def _():
        arrive(3)
    block(3, 0)
    plane_totals(band(NZ - 1))
    block(3, 1)
    plane_totals(band(NZ - 2))
    for d in range(G):
        block(d, 2)
    plane_totals(band(NZ - 3))
    landed(0)
    pl.when(inner)(lambda: last_block(3, False))
    pl.when(jnp.logical_not(inner))(lambda: last_block(3, True))

    CH = NK // NC

    def kv_copy(p, peer):
        return remote(kv.at[:, pl.ds(p * D, D)], kvn.at[p], kvs.at[p], kvr.at[p], peer)

    def d_copy(z_to, z_from):
        return remote(dqs.at[m128(z_to, RZ)], dqin.at[z_from], ds.at[z_to], dr.at[z_from], z_to * G + j)

    def coefs(zb):
        cols = m128(zb, ZB)
        for d in range(1, NZ):
            s_copy(zb, z, far(d)[1], me).wait_recv()
        top = stat[0:1, cols]
        for d in range(1, NZ):
            top = jnp.maximum(top, stin[far(d)[1], 0:1, cols])
        w = jnp.exp(stat[0:1, cols] - top)
        total, dotted = w * stat[1:2, cols], w * stat[2:3, cols]
        for d in range(1, NZ):
            i = far(d)[1]
            w = jnp.exp(stin[i, 0:1, cols] - top)
            total += w * stin[i, 1:2, cols]
            dotted += w * stin[i, 2:3, cols]
        for g in range(G):
            coef[g:g + 1, cols] = jnp.exp(gst[g, 0:1, cols] - top) / total
        coef[G:G + 1, cols] = dotted / total

    brim = jnp.where(2 * z < NZ, 0, NZ - 1)
    core_z = jnp.where(2 * z < NZ, 1, NZ - 2)

    def grads(n, zb):
        cols = m128(zb, ZB)
        coefs(zb)
        dqt[...] = jnp.zeros_like(dqt)

        @pl.loop(0, NC)
        def _(c):
            w, off = coef[pl.ds(c, 1), cols], coef[G:G + 1, cols]
            part_q = None
            for i in range(CH // FR):
                at, tok = pl.ds(i * FR, FR), m128(c * (CH // FR) + i, FR)
                p = ebuf[tok, cols] * w
                t = (p * (dpb[tok, cols] - off)).astype(BF16)
                dv = dot(p.astype(BF16), gb[cols, :])
                dk = dot(t, qb[cols, :])
                dq = dot(ktb[:, tok], t)
                part_q = dq if part_q is None else part_q + dq
                if n:
                    dk += tmp[c, at, 0:D]
                    dv += tmp[c, at, D:2 * D]
                if n < NZ - 1:
                    tmp[c, at, 0:D] = dk
                    tmp[c, at, D:2 * D] = dv
                else:
                    kv[tok, 0:D] = (scale * dk).astype(BF16)
                    kv[tok, D:2 * D] = dv.astype(BF16)
            dqt[...] += part_q

        if n == NZ - 1:
            for p in (1, 0):
                send(kv_copy(p, near(1)[1]))
        for i in range(ZB // D):
            t = (scale * dqt[:, pl.ds(i * D, D)].T).astype(BF16)
            for k in range(D // RZ):
                m = i * (D // RZ) + k
                dqs[m128(zb, RZ), pl.ds(m * D, D)] = t[k * RZ:(k + 1) * RZ, :]

        @pl.when(zb != z)
        def _():
            d_copy(zb, z).start()

    for f in range(NK // FR):
        ktb[:, pl.ds(f * FR, FR)] = kb[pl.ds(f * FR, FR), :].astype(F32).T.astype(BF16)
    grads(0, NZ - 1 - core_z)
    landed(NZ - 3)
    grads(1, core_z)
    grads(2, NZ - 1 - brim)
    landed(NZ - 2)
    grads(3, brim)
    HW = JW // 2

    def jcols(head, off, n):
        return pl.ds(pl.multiple_of(head * JW + off, n), n)

    def half(u):
        return pl.ds(u * HW, HW)

    def a_copy(kind, u, z_to, z_from):
        here = q_out.at[m128(z_from, RZ), jcols(j, u * HW, HW)]
        return remote(here, here, as_.at[kind, u, z_to], ar.at[u, z_from], z_to * G + j)

    def a_own(u, act):
        @pl.when(inner)
        def _():
            for d in range(1, NZ):
                act(a_copy(0, u, far(d)[0], z))

        @pl.when(jnp.logical_not(inner))
        def _():
            act(a_copy(0, u, jnp.where(low, NZ - 2, 1), z))

    def a_onward(u, act):
        act(a_copy(1, u, NZ - 1 - z, brim))
        act(a_copy(1, u, NZ - 1 - brim, brim))

    QW = JW // 4

    def y_copy(u, j_from, peer, kind):
        here = q_out.at[:, jcols(j_from, u * QW, QW)]
        return remote(here, here, ys.at[kind, u], yr.at[kind, u], peer)

    def y_pass(u, frm, to):
        y_copy(u, near(frm)[0], me, frm - 1).wait_recv()
        send(y_copy(u, near(frm)[0], near(to)[1], 2))

    for c in local_x:
        c.wait()

    def piece(h, p, i):
        cols = pl.ds(p * D, D) if h else pl.ds(0, 2 * D)
        return m128(i, FB), cols, (2 + 2 * p + i if h else i)

    def c_copy(side, b, h, p, i, peer):
        at, cols, n = piece(h, p, i)
        return remote(part.at[h, b, at, cols], rin.at[side, b, h, at, cols], cs.at[b, n], cr.at[side, b, n], peer)

    def weigh(s, h, p):
        for i in range(2):
            at, cols, _ = piece(h, p, i)
            tmp[h * NZ + s, at, cols] = dot(vis[band(s), :, i * FB:(i + 1) * FB], kvn[p] if h else kv[...], TN)

    def gather(s):
        b = band(s)
        x_copy(1, b, x, near(2)[0], me).wait_recv()
        send(f_copy(1, b, True))
        pass_copy(b, near(3)[0], me).wait_recv()
        send(f_copy(2, b, True))
        for kind in range(3):
            f_copy(kind, b, False).wait_recv()

    def hop(s):
        b = band(s)
        side = (b < z).astype(jnp.int32)
        return b, side, jnp.where(b > z, low, high), (z + 1 - 2 * side) * G + j

    def first(s, h, p=0):
        weigh(s, h, p)
        b, side, fed, peer = hop(s)

        @pl.when(jnp.logical_not(fed))
        def _():
            for i in (1 - y, y):
                at, cols, _ = piece(h, p, i)
                part[h, b, at, cols] = tmp[h * NZ + s, at, cols].astype(BF16)
                c_copy(side, b, h, p, i, peer).start()

    def later(s, h, p=0):
        b, side, fed, peer = hop(s)

        @pl.when(fed)
        def _():
            for i in (1 - y, y):
                at, cols, _ = piece(h, p, i)
                c_copy(side, b, h, p, i, me).wait_recv()
                part[h, b, at, cols] = (tmp[h * NZ + s, at, cols] + rin[side, b, h, at, cols].astype(F32)).astype(BF16)
                c_copy(side, b, h, p, i, peer).start()

    def e_copy(h, p, peer):
        cols = piece(h, p, 0)[1]
        return remote(ybs.at[h, :, cols], ybr.at[h, :, cols], es.at[h + h * p], er.at[h + h * p], peer)

    def settle(head, grads_of, grad):
        cols = m128(head, D)
        for n, a in enumerate(grads_of):
            (kw_out, vw_out)[a][:, cols] = grad[:, n * D:(n + 1) * D]

    def finish(h, p=0):
        own = h * NZ + NZ - 1
        for i in (1 - y, y):
            at, cols, _ = piece(h, p, i)
            for side, there in ((0, low), (1, high)):
                @pl.when(there)
                def _():
                    c_copy(side, z, h, p, i, me).wait_recv()
                    tmp[own, at, cols] += rin[side, z, h, at, cols].astype(F32)
            if i is y:
                settle(j ^ h, (p,) if h else (0, 1), tmp[own, at, cols])
            else:
                ybs[h, :, cols] = tmp[own, at, cols].astype(BF16)
                send(e_copy(h, p, near(2)[1]))

    def summed_dq():
        mine = dqs[m128(z, RZ), :].astype(F32)
        for d in range(1, NZ):
            d_copy(z, far(d)[1]).wait_recv()
            mine += dqin[far(d)[1]].astype(F32)
        q_out[m128(z, RZ), m128(j, JW)] = mine.astype(BF16)
        for u in range(2):
            a_own(u, lambda c: c.start())

    def relay_dq(u):
        @pl.when(inner)
        def _():
            a_copy(0, u, z, brim).wait_recv()
            a_onward(u, lambda c: c.start())

    def shared_dq():
        for u in range(2):
            for d in range(1, NZ):
                b = far(d)[1]

                @pl.when(jnp.logical_not(inner) | (b != brim))
                def _():
                    a_copy(0, u, z, b).wait_recv()
        for u in range(4):
            send(y_copy(u, j, near(1)[1], 0))
            send(y_copy((u + 1) % 4, j, near(2)[1], 1))

    gather(0)
    first(0, 0)
    landed(NZ - 1)
    summed_dq()
    gather(1)
    first(1, 0)
    later(0, 0)
    relay_dq(0)
    relay_dq(1)
    kv_copy(1, me).wait_recv()
    first(0, 1, 1)
    first(1, 1, 1)
    later(1, 0)
    gather(2)
    first(2, 0)
    shared_dq()
    first(2, 1, 1)
    later(0, 1, 1)
    gather(3)
    kv_copy(0, me).wait_recv()
    for s in range(NZ - 1):
        first(s, 1, 0)
    later(1, 1, 1)
    later(2, 0)
    weigh(3, 0, 0)
    weigh(3, 1, 1)
    weigh(3, 1, 0)

    y_pass(0, 1, 2)
    y_pass(1, 2, 1)
    later(2, 1, 1)
    finish(0)
    later(0, 1, 0)
    y_pass(2, 2, 1)
    y_pass(3, 2, 1)
    later(1, 1, 0)
    later(2, 1, 0)
    for u in range(1, 4):
        y_copy(u, near(1)[0], me, 0).wait_recv()
    y_copy(0, near(2)[0], me, 1).wait_recv()
    finish(1, 1)
    finish(1, 0)
    for u in range(4):
        y_copy(u, near(3)[0], me, 2).wait_recv()
    for h, p, grads_of in ((0, 0, (0, 1)), (1, 1, (1,)), (1, 0, (0,))):
        e_copy(h, p, me).wait_recv()
        settle(j ^ (2 + h), grads_of, ybr[h, :, piece(h, p, 0)[1]].astype(F32))
    for c in sends:
        c.wait_send()
    for k in range(NZ):
        zq_each(lambda c: c.wait_send(), band(NZ - 1 - k), False)
    for u in range(2):
        a_own(u, lambda c: c.wait_send())
        pl.when(inner)(lambda: a_onward(u, lambda c: c.wait_send()))
    for s in range(NZ - 1):
        b, side, fed, peer = hop(s)
        for h, p in ((0, 0), (1, 0), (1, 1)):
            for i in range(2):
                c_copy(side, b, h, p, i, peer).wait_send()
    for d in range(1, NZ):
        d_copy(far(d)[0], z).wait_send()
    for zb in range(NZ):
        for d in range(1, NZ):
            s_copy(zb, far(d)[0], z, far(d)[2]).wait_send()


def deliver_kernel(parts, *refs):
    n = len(parts)
    moves, k = [], 0
    for src, dst, p in zip(refs[:n], refs[n:2 * n], parts):
        step = src.shape[0] // p
        for i in range(p):
            at = pl.ds(i * step, step)
            moves.append(pltpu.make_async_copy(src.at[at], dst.at[at], refs[2 * n].at[k]))
            k += 1
    for a in moves:
        a.start()
    for a in moves:
        a.wait()


def deliver(*arrays):
    parts = [4, 1, 1]
    return pl.pallas_call(
        functools.partial(deliver_kernel, parts),
        out_shape=[jax.ShapeDtypeStruct(a.shape, a.dtype) for a in arrays],
        in_specs=[pl.BlockSpec(memory_space=pltpu.VMEM)] * len(arrays),
        out_specs=[pl.BlockSpec(memory_space=pl.ANY)] * len(arrays),
        scratch_shapes=[pltpu.SemaphoreType.DMA((sum(parts),))],
        compiler_params=pltpu.CompilerParams(vmem_limit_bytes=1 << 20),
    )(*arrays)


def plane_shards(T, text_queries, text_grads, vision_keys, video_value_rows, vision, lengths, frame_range):
    R, QW = text_queries.shape
    rows, kv_width = vision_keys.shape
    G = kv_width // HEAD_WIDTH
    M = QW // kv_width
    NZ = T // G
    DW = vision.shape[1]
    FB = DW // T
    NK, RZ, JW = G * rows, G * R, M * HEAD_WIDTH
    NR = T * R * M
    cfg = dict(G=G, NZ=NZ, M=M, R=R, FR=rows // FRAME_DEV, NC=4, rows=rows, NK=NK, NR=NR, JW=JW, FB=FB, RZ=RZ,
               NS=lengths.shape[0])
    anyspec = pl.BlockSpec(memory_space=pl.ANY)
    vm = pl.BlockSpec(memory_space=pltpu.VMEM)
    V = pltpu.VMEM
    D = pltpu.SemaphoreType.DMA
    W2 = 2 * HEAD_WIDTH
    pairs = []
    for a, b in (((2, G),) * 2, ((2, 2, NZ), (2, NZ)), ((2, G),) * 2, ((3, NZ),) * 2, ((3, NZ),) * 2, ((NZ, NZ),) * 2, ((2,),) * 2,
                 ((NZ,),) * 2, ((2, 2, NZ), (2, NZ)), ((3, 4),) * 2, ((NZ, 6), (2, NZ, 6)), ((3,),) * 2):
        pairs += [D(a), D(b)]
    q_grad, kw, vw = pl.pallas_call(
        functools.partial(plane_kernel, cfg),
        out_shape=(
            V((T * R, QW), BF16),
            V((FB, kv_width), F32),
            V((FB, kv_width), F32),
        ),
        in_specs=[anyspec] * 7,
        out_specs=(vm,) * 3,
        scratch_shapes=[
            V((T * R, JW), BF16), V((T * R, JW), BF16),
            V((NR, HEAD_WIDTH), BF16), V((NR, HEAD_WIDTH), BF16),
            V((NK, HEAD_WIDTH), BF16), V((NK, HEAD_WIDTH), BF16),
            V((NZ, NK, 2 * FB), BF16),
            V((NK, NR), F32), V((NK, NR), F32),
            V((8, NR), F32), V((NZ, 8, NR), F32), V((8, NR), F32), V((8, NR), jnp.int32),
            V((NK, W2), BF16), V((2, NK, HEAD_WIDTH), BF16),
            V((HEAD_WIDTH, M * RZ), F32), V((T * R, JW), BF16),
            V((NZ, RZ, JW), BF16),
            V((G, 8, NR), F32), V((HEAD_WIDTH, NK), BF16),
            pltpu.SMEM(lengths.shape, jnp.int32), pltpu.SMEM(frame_range.shape[::-1], jnp.int32),
            V((2 * NZ, 2 * FB, W2), F32), V((2, NZ, 2 * FB, W2), BF16), V((2, NZ, 2, 2 * FB, W2), BF16),
            V((2, FB, W2), BF16), V((2, FB, W2), BF16),
            D((6,)), D((NZ, 2)),
        ] + pairs,
        compiler_params=pltpu.CompilerParams(
            collective_id=0, has_side_effects=True, vmem_limit_bytes=67043328 - T * R * QW * 2 - 8 * FB * kv_width - (1 << 18)
        ),
    )(text_queries, text_grads, vision_keys, video_value_rows, vision, lengths, frame_range.T)
    return deliver(*[pltpu.with_memory_space_constraint(a, pltpu.VMEM) for a in (q_grad, kw, vw)])


def solution(mesh):
    return jax.shard_map(
        functools.partial(shards, mesh.shape["tok"], mesh.shape["head"]),
        mesh=mesh,
        in_specs=(
            P("tok", "head"),
            P("tok", "head"),
            P("tok", "head"),
            P("tok", "head"),
            P("tok", None),
            P(),
            P(),
        ),
        out_specs=(P(None, "head"), P("tok", "head"), P("tok", "head")),
        check_vma=False,
    )
```

```python
import functools

import jax
import jax.numpy as jnp
from jax import lax
from jax.experimental import pallas as pl
from jax.experimental.pallas import tpu as pltpu
from jax.sharding import PartitionSpec as P

HEAD_WIDTH = 128
FRAME_DEV = 4
NEG_FILL = -1e30
NT = (((1,), (1,)), ((), ()))
TN = (((0,), (0,)), ((), ()))
F32 = jnp.float32
BF16 = jnp.bfloat16


def dot(a, b, dims=(((1,), (0,)), ((), ()))):
    return lax.dot_general(a, b, dims, preferred_element_type=F32)


def kernel(cfg, q_in, g_in, k_in, v_in, x_in, bounds, q_out, kw_out, vw_out,
           qb, gb, kb, vb, vis, ebuf, dpb, stat, stin, coef, kv, dqt, dqs, dqin, dqall, part, rsb,
           loc, qs, qr, gs, gr, ks, kr, vs, vr, xs, xr, ss, sr, kvs, kvr, ds, dr, as_, ar, ys, yr, rs, rr, fs, fr):
    T, G, NZ = cfg["T"], cfg["G"], cfg["NZ"]
    blk, rows, NK, NR, FR = cfg["blk"], cfg["rows"], cfg["NK"], cfg["NR"], cfg["FR"]
    W, NV, FB = cfg["W"], cfg["NV"], cfg["FB"]
    H = cfg["H"]
    RB = cfg["RB"]
    scale = HEAD_WIDTH ** (-0.5)
    me = lax.axis_index("tok")
    z, j0 = me // G, me % G

    def remote(src, dst, s, r, peer):
        return pltpu.make_async_remote_copy(
            src_ref=src, dst_ref=dst, send_sem=s, recv_sem=r,
            device_id={"tok": peer}, device_id_type=pl.DeviceIdType.MESH)

    def m128(i, n):
        return pl.ds(pl.multiple_of(i * n, n), n)

    barrier = pltpu.get_barrier_semaphore()
    for d in range(1, T):
        pl.semaphore_signal(barrier, inc=1, device_id={"tok": lax.rem(me + d, T)}, device_id_type=pl.DeviceIdType.MESH)
    twin = lax.axis_index("head")
    if H > 1:
        twin = 1 - twin
        pl.semaphore_signal(barrier, inc=1, device_id={"head": twin}, device_id_type=pl.DeviceIdType.MESH)
    pl.semaphore_wait(barrier, T - 1 + (H > 1))

    def tpeer(d):
        return lax.rem(me + d, T), lax.rem(me + T - d, T)

    def gpeer(d):
        a, b = (j0 ^ d, j0 ^ d) if G & (G - 1) == 0 else (lax.rem(j0 + d, G), lax.rem(j0 + G - d, G))
        return a, b, z * G + a, z * G + b

    def zpeer(d):
        a, b = lax.rem(z + d, NZ), lax.rem(z + NZ - d, NZ)
        return a, b, a * G + j0, b * G + j0

    sends = []

    def send(c):
        c.start()
        sends.append(c)

    def q_copy(t_to, t_from):
        return (remote(q_in.at[lax.rem(t_to, G)], qb.at[m128(t_from, blk)], qs.at[t_to], qr.at[t_from], t_to),
                remote(g_in.at[lax.rem(t_to, G)], gb.at[m128(t_from, blk)], gs.at[t_to], gr.at[t_from], t_to))

    def k_copy(j_to, j_from, peer):
        return (remote(k_in.at[:, m128(j_to, 128)], kb.at[m128(j_from, rows)], ks.at[j_to], kr.at[j_from], peer),
                remote(v_in.at[:, m128(j_to, 128)], vb.at[m128(j_from, rows)], vs.at[j_to], vr.at[j_from], peer))

    WH = W // H
    half = lax.axis_index("head") * WH if H > 1 else 0

    def x_copy(b, j_to, j_from, peer):
        cols = pl.ds(pl.multiple_of((b * G + j_to) * W + half, WH), WH)
        dst = vis.at[b, m128(j_from, rows), pl.ds(pl.multiple_of(half, WH), WH)]
        return remote(x_in.at[:, cols], dst, xs.at[j_to, b], xr.at[j_from, b], peer)

    def f_copy(b, j_from, mine):
        at = half if mine else WH - half
        here = vis.at[b, m128(j_from, rows), pl.ds(pl.multiple_of(at, WH), WH)]
        return pltpu.make_async_remote_copy(
            src_ref=here, dst_ref=here, send_sem=fs.at[j_from, b], recv_sem=fr.at[j_from, b],
            device_id={"head": twin}, device_id_type=pl.DeviceIdType.MESH)

    local = [
        pltpu.make_async_copy(q_in.at[j0], qb.at[m128(me, blk)], loc.at[0]),
        pltpu.make_async_copy(g_in.at[j0], gb.at[m128(me, blk)], loc.at[1]),
        pltpu.make_async_copy(k_in.at[:, m128(j0, 128)], kb.at[m128(j0, rows)], loc.at[2]),
        pltpu.make_async_copy(v_in.at[:, m128(j0, 128)], vb.at[m128(j0, rows)], loc.at[3]),
    ]
    local_x = [pltpu.make_async_copy(x_in.at[:, m128(b * G + j0, W)], vis.at[b, m128(j0, rows)], loc.at[4 + b]) for b in range(NV)]
    for c in local:
        c.start()
    def q_sends(zd):
        a, _, _, _ = zpeer(zd)
        for i in range(G):
            to = a * G + (lax.rem(j0 + i, G) if zd else gpeer(i)[0])
            if zd or i:
                for c in q_copy(to, me):
                    send(c)

    q_sends(0)
    for d in range(1, G):
        a, _, peer, _ = gpeer(d)
        for c in k_copy(a, j0, peer):
            send(c)
    for d in range(1, NZ):
        q_sends(d)
    for c in local_x:
        c.start()
    for c in local:
        c.wait()
    for d in range(1, G):
        _, b, _, _ = gpeer(d)
        for c in k_copy(j0, b, me):
            c.wait_recv()

    def q_wait(zd):
        _, b, _, _ = zpeer(zd)
        for i in range(G):
            if zd or i:
                frm = b * G + (i if zd else gpeer(i)[1])
                for c in q_copy(me, frm):
                    c.wait_recv()

    n_frames = NK // FR
    frame0 = z * n_frames
    stat[0:1, :] = jnp.full((1, NR), NEG_FILL, F32)
    stat[1:8, :] = jnp.zeros((7, NR), F32)

    def totals(cols, width):
        first, end = bounds[0:1, cols], bounds[1:2, cols]
        UN = 2 if n_frames % 2 == 0 else 1

        def scored(i, top):
            for u in range(UN):
                f = i * UN + u
                ok = (first <= frame0 + f) & (frame0 + f < end)
                s = jnp.where(ok, dot(kb[m128(f, FR), :], qb[cols, :], NT) * scale, NEG_FILL)
                ebuf[m128(f, FR), cols] = s
                top = jnp.maximum(top, jnp.max(s, axis=0, keepdims=True))
            return top

        top = lax.fori_loop(0, n_frames // UN, scored, jnp.full((1, width), NEG_FILL, F32))

        def summed(i, carry):
            total, dotted = carry
            for u in range(UN):
                f = i * UN + u
                dp = dot(vb[m128(f, FR), :], gb[cols, :], NT)
                e = jnp.exp(ebuf[m128(f, FR), cols] - top)
                ebuf[m128(f, FR), cols] = e
                dpb[m128(f, FR), cols] = dp
                total += jnp.sum(e, axis=0, keepdims=True)
                dotted += jnp.sum(e * dp, axis=0, keepdims=True)
            return total, dotted

        zero = jnp.zeros((1, width), F32)
        total, dotted = lax.fori_loop(0, n_frames // UN, summed, (zero, zero))
        stat[0:1, cols] = top
        stat[1:2, cols] = total
        stat[2:3, cols] = dotted

    def x_sends():
        for d in range(1, G):
            a, _, peer, _ = gpeer(d)
            for b in range(NV):
                send(x_copy(b, a, j0, peer))

    by_z = (NR // NZ) % 128 == 0
    for d in range(NZ):
        q_wait(d)
        if d == NZ - 1:
            x_sends()
        if by_z:
            totals(m128(zpeer(d)[1], NR // NZ), NR // NZ)
    if not by_z:
        for r in range(0, NR, RB):
            totals(pl.ds(r, RB), RB)

    def s_copy(z_to, z_from, peer):
        return remote(stat, stin.at[z_from], ss.at[z_to], sr.at[z_from], peer)

    for d in range(1, NZ):
        a, _, peer, _ = zpeer(d)
        send(s_copy(a, z, peer))
    stin[z] = stat[...]
    for d in range(1, NZ):
        _, b, _, _ = zpeer(d)
        s_copy(z, b, me).wait_recv()
    top = stat[0:1, :]
    for i in range(NZ):
        top = jnp.maximum(top, stin[i, 0:1, :])
    total = jnp.zeros((1, NR), F32)
    dotted = jnp.zeros((1, NR), F32)
    for i in range(NZ):
        w = jnp.exp(stin[i, 0:1, :] - top)
        total += w * stin[i, 1:2, :]
        dotted += w * stin[i, 2:3, :]
    coef[0:1, :] = jnp.exp(stat[0:1, :] - top) / total
    coef[1:2, :] = dotted / total
    dqt[...] = jnp.zeros_like(dqt)

    NC = cfg["NC"]
    CH = NK // NC

    def kv_copy(c, j_to, j_from, peer):
        here = kv.at[j_from, pl.ds(c * CH, CH)]
        return remote(here, here, kvs.at[j_to, c], kvr.at[j_from, c], peer)

    for c in range(NC):
        @pl.loop(c * (CH // FR), (c + 1) * (CH // FR))
        def _(f):
            kt = kb[m128(f, FR), :].astype(F32).T.astype(BF16)
            dk = jnp.zeros((FR, HEAD_WIDTH), F32)
            dv = jnp.zeros((FR, HEAD_WIDTH), F32)
            for r in range(0, NR, RB):
                cols = pl.ds(r, RB)
                p = ebuf[m128(f, FR), cols] * coef[0:1, cols]
                t = (p * (dpb[m128(f, FR), cols] - coef[1:2, cols])).astype(BF16)
                dv += dot(p.astype(BF16), gb[cols, :])
                dk += dot(t, qb[cols, :])
                dqt[:, cols] += dot(kt, t)
            kv[j0, m128(f, FR), 0:HEAD_WIDTH] = (scale * dk).astype(BF16)
            kv[j0, m128(f, FR), HEAD_WIDTH:2 * HEAD_WIDTH] = dv.astype(BF16)

        for d in range(1, G - 1):
            a, _, peer, _ = gpeer(d)
            kv_copy(c, a, j0, peer).start()
        if H > 1 and c == NC // 2:
            for d in range(1, G):
                _, b, _, _ = gpeer(d)
                for i in range(NV):
                    x_copy(i, j0, b, me).wait_recv()
                    send(f_copy(i, b, True))

    for r in range(0, NR, 128):
        dqs[pl.ds(r, 128), :] = (scale * dqt[:, pl.ds(r, 128)].T).astype(BF16)
    QR = NR // NZ

    def d_copy(z_to, z_from, peer):
        return remote(dqs.at[m128(z_to, QR)], dqin.at[z_from], ds.at[z_to], dr.at[z_from], peer)

    def a_copy(z_to, z_from, peer):
        here = dqall.at[j0, m128(z_from, QR)]
        return remote(here, here, as_.at[z_to], ar.at[z_from], peer)

    def y_copy(j_to, j_from, peer):
        here = dqall.at[j_from]
        return remote(here, here, ys.at[j_to], yr.at[j_from], peer)

    def r_copy(j, z_to, z_from, peer):
        return remote(part.at[j, m128(z_to, FB)], rsb.at[z_from, j], rs.at[j, z_to], rr.at[j, z_from], peer)

    for d in range(1, NZ):
        a, _, peer, _ = zpeer(d)
        send(d_copy(a, z, peer))
    for c in local_x:
        c.wait()
    for d in range(1, G):
        _, b, _, _ = gpeer(d)
        for i in range(NV):
            (f_copy(i, b, False) if H > 1 else x_copy(i, j0, b, me)).wait_recv()

    def weigh(j):
        @pl.loop(0, NV)
        def _(b):
            part[j, m128(b, W), :] = dot(vis[b], kv[j], TN).astype(BF16)
        for d in range(1, NZ):
            a, _, peer, _ = zpeer(d)
            send(r_copy(j, a, z, peer))

    weigh(j0)
    mine = dqs[m128(z, QR), :].astype(F32)
    for d in range(1, NZ):
        _, b, _, _ = zpeer(d)
        d_copy(z, b, me).wait_recv()
        mine += dqin[b].astype(F32)
    dqall[j0, m128(z, QR), :] = mine.astype(BF16)
    for d in range(1, NZ):
        a, _, peer, _ = zpeer(d)
        send(a_copy(a, z, peer))

    def spread():
        for d in range(1, NZ):
            _, b, _, _ = zpeer(d)
            a_copy(z, b, me).wait_recv()
        for d in range(1, G):
            a, _, peer, _ = gpeer(d)
            send(y_copy(a, j0, peer))

    for d in range(1, G - 1):
        a, _, peer, _ = gpeer(d)
        for c in range(NC):
            kv_copy(c, a, j0, peer).wait_send()
    if G > 1:
        a, _, peer, _ = gpeer(G - 1)
        for c in range(NC):
            send(kv_copy(c, a, j0, peer))
    if G == 1:
        spread()
    for d in range(1, G):
        _, b, _, _ = gpeer(d)
        for c in range(NC):
            kv_copy(c, j0, b, me).wait_recv()
        weigh(b)
        if d == min(2, G - 1):
            spread()
    for d in range(1, G):
        _, b, _, _ = gpeer(d)
        y_copy(j0, b, me).wait_recv()
    out_copy = pltpu.make_async_copy(dqall, q_out, loc.at[0])
    out_copy.start()

    for d in range(1, NZ):
        _, b, _, _ = zpeer(d)
        for j in range(G):
            r_copy(j, z, b, me).wait_recv()
    for j in range(G):
        acc = part[j, m128(z, FB), :].astype(F32)
        for d in range(1, NZ):
            _, b, _, _ = zpeer(d)
            acc += rsb[b, j].astype(F32)
        kw_out[:, pl.ds(j * HEAD_WIDTH, HEAD_WIDTH)] = acc[:, 0:HEAD_WIDTH]
        vw_out[:, pl.ds(j * HEAD_WIDTH, HEAD_WIDTH)] = acc[:, HEAD_WIDTH:]
    out_copy.wait()
    for c in sends:
        c.wait_send()


def shards(T, cores, text_queries, text_grads, vision_keys, video_value_rows, vision, lengths, frame_range):
    R, QW = text_queries.shape
    rows, kv_width = vision_keys.shape
    G = kv_width // HEAD_WIDTH
    if cores == 2 and G == 4 and T == G * G and vision.shape[1] % (T * 128) == 0 and HEAD_WIDTH % (G * R) == 0 and 2 * vision.shape[1] == T * rows:
        return plane_shards(T, text_queries, text_grads, vision_keys, video_value_rows, vision, lengths, frame_range)
    M = QW // kv_width
    NZ = T // G
    DW = vision.shape[1]
    blk, NK, NR = M * R, G * rows, T * M * R
    FB = DW // T
    W = FB if FB % 128 == 0 else 256
    NV = DW // (G * W)
    FR = rows // FRAME_DEV
    NC = 4 if NK >= 16 * FR else 1
    cfg = dict(T=T, G=G, NZ=NZ, blk=blk, rows=rows, NK=NK, NR=NR, FR=FR, W=W, NV=NV, FB=FB, NC=NC, RB=min(NR, 512),
               H=2 if cores == 2 and G > 1 and W % 256 == 0 else 1)

    text_len = R * T
    row_ids = jnp.arange(text_len, dtype=jnp.int32)
    segment_ends = jnp.cumsum(lengths)
    segment = jnp.sum((row_ids[:, None] >= segment_ends[None, :]).astype(jnp.int32), axis=1)
    segment_pick = (
        segment[:, None] == jnp.arange(lengths.shape[0], dtype=jnp.int32)[None, :]
    ).astype(jnp.int32)
    bounds = jnp.sum(segment_pick[None] * frame_range.T[:, None, :], axis=2)
    bounds = jnp.broadcast_to(bounds.reshape(2, T, 1, R), (2, T, M, R)).reshape(2, NR)

    def split(a):
        return a.reshape(R, G, M, HEAD_WIDTH).transpose(1, 2, 0, 3).reshape(G, blk, HEAD_WIDTH)

    anyspec = pl.BlockSpec(memory_space=pl.ANY)
    vm = pl.BlockSpec(memory_space=pltpu.VMEM)
    V = pltpu.VMEM
    D = pltpu.SemaphoreType.DMA
    sem_pairs = []
    for shape in ((T,), (T,), (G,), (G,), (G, NV), (NZ,), (G, NC), (NZ,), (NZ,), (G,), (G, NZ), (G, NV)):
        sem_pairs += [D(shape), D(shape)]
    q_grad, kw, vw = pl.pallas_call(
        functools.partial(kernel, cfg),
        out_shape=(
            jax.ShapeDtypeStruct((G, NR, HEAD_WIDTH), BF16),
            jax.ShapeDtypeStruct((FB, kv_width), F32),
            jax.ShapeDtypeStruct((FB, kv_width), F32),
        ),
        in_specs=[anyspec] * 5 + [vm],
        out_specs=(anyspec, vm, vm),
        scratch_shapes=[
            V((NR, HEAD_WIDTH), BF16), V((NR, HEAD_WIDTH), BF16),
            V((NK, HEAD_WIDTH), BF16), V((NK, HEAD_WIDTH), BF16),
            V((NV, NK, W), BF16),
            V((NK, NR), F32), V((NK, NR), F32),
            V((8, NR), F32), V((NZ, 8, NR), F32), V((8, NR), F32),
            V((G, NK, 2 * HEAD_WIDTH), BF16),
            V((HEAD_WIDTH, NR), F32), V((NR, HEAD_WIDTH), BF16),
            V((NZ, NR // NZ, HEAD_WIDTH), BF16), V((G, NR, HEAD_WIDTH), BF16),
            V((G, DW // G, 2 * HEAD_WIDTH), BF16),
            V((NZ, G, FB, 2 * HEAD_WIDTH), BF16),
            D((4 + NV,)),
        ] + sem_pairs,
        compiler_params=pltpu.CompilerParams(
            collective_id=0, has_side_effects=True, vmem_limit_bytes=67043328
        ),
    )(split(text_queries), split(text_grads), vision_keys, video_value_rows, vision, bounds)
    q_grad = q_grad.reshape(G, T, M, R, HEAD_WIDTH).transpose(1, 3, 0, 2, 4).reshape(text_len, QW)
    return q_grad, kw, vw


def plane_kernel(cfg, q_in, g_in, k_in, v_in, x_in, lens_in, frames_in, q_out, kw_out, vw_out,
                 qraw, graw, qb, gb, kb, vb, vis, ebuf, dpb, stat, stin, coef, lim, kv, kvn, dqt, dqs, dqin,
                 gst, ktb, lens, frames, tmp, part, rin, ybs, ybr, loc, lx, qs, qr, zs, zr, ks, kr, xs, xr, fs, fr, ss, sr, kvs, kvr,
                 ds, dr, as_, ar, ys, yr, cs, cr, es, er):
    G, NZ, M, R, FR, NC = cfg["G"], cfg["NZ"], cfg["M"], cfg["R"], cfg["FR"], cfg["NC"]
    rows, NK, NR, JW, FB, RZ = cfg["rows"], cfg["NK"], cfg["NR"], cfg["JW"], cfg["FB"], cfg["RZ"]
    D = HEAD_WIDTH
    ZB = M * RZ
    scale = D ** (-0.5)
    me = lax.axis_index("tok")
    core = lax.axis_index("head")
    z, j = me // G, me % G
    y, x = j // 2, j % 2

    def m128(i, n):
        return pl.ds(pl.multiple_of(i * n, n), n)

    def remote(src, dst, s, r, peer):
        return pltpu.make_async_remote_copy(
            src_ref=src, dst_ref=dst, send_sem=s, recv_sem=r,
            device_id={"tok": peer}, device_id_type=pl.DeviceIdType.MESH)

    def near(d):
        return j ^ d, z * G + (j ^ d)

    def far(d):
        a, b = lax.rem(z + d, NZ), lax.rem(z + NZ - d, NZ)
        return a, b, a * G + j, b * G + j

    mirror = 2 * z > NZ - 1
    zz = jnp.where(mirror, NZ - 1 - z, z)

    def band(s):
        u = s - (NZ - 1 - 2 * zz)
        k, odd = u // 2, u % 2
        b = jnp.where(u < 0, NZ - 1 - s, k + odd * (2 * zz - 2 * k))
        return jnp.where(mirror, NZ - 1 - b, b)

    barrier = pltpu.get_barrier_semaphore()
    for d in range(1, G):
        pl.semaphore_signal(barrier, inc=1, device_id={"tok": near(d)[1]}, device_id_type=pl.DeviceIdType.MESH)
    for d in range(1, NZ):
        pl.semaphore_signal(barrier, inc=1, device_id={"tok": far(d)[2]}, device_id_type=pl.DeviceIdType.MESH)
    pl.semaphore_signal(barrier, inc=1, device_id={"head": 1 - core}, device_id_type=pl.DeviceIdType.MESH)
    pl.semaphore_wait(barrier, G + NZ - 1)

    sends = []

    def send(c):
        c.start()
        sends.append(c)

    def own_rows(t):
        return m128(t, R)

    def q_copy(d, t_from, peer, j_to):
        cols = m128(j_to, JW)
        return (remote(q_in.at[:, cols], qraw.at[own_rows(t_from)], qs.at[0, d], qr.at[0, d], peer),
                remote(g_in.at[:, cols], graw.at[own_rows(t_from)], qs.at[1, d], qr.at[1, d], peer))

    low, high = z > 0, z < NZ - 1
    inner = low & high

    def zq_copy(side, a, b):
        here = (qraw, graw)[a].at[m128(b, RZ)]
        return remote(here, here, zs.at[side, a, b], zr.at[a, b], (z + 1 - 2 * side) * G + j)

    def zq_each(act, b, into, which=(0, 1)):
        for a in which:
            if into:
                zq_copy(0, a, b).wait_recv()

            @pl.when(high & (b <= z))
            def _():
                act(zq_copy(0, a, b))

            @pl.when(low & (b >= z))
            def _():
                act(zq_copy(1, a, b))

    def k_copy(d, j_to, j_from, peer):
        return (remote(k_in.at[:, m128(j_to, D)], kb.at[m128(j_from, rows)], ks.at[0, d], kr.at[0, d], peer),
                remote(v_in.at[:, m128(j_to, D)], vb.at[m128(j_from, rows)], ks.at[1, d], kr.at[1, d], peer))

    def lane_half(mine):
        return m128(core if mine else 1 - core, FB)

    def x_copy(kind, b, x_to, j_from, peer):
        cols = m128(b * G + core * 2 + x_to, FB)
        dst = vis.at[b, m128(j_from, rows), lane_half(True)]
        return remote(x_in.at[:, cols], dst, xs.at[kind, b], xr.at[kind, b], peer)

    def pass_copy(b, j_from, peer):
        here = vis.at[b, m128(j_from, rows), lane_half(True)]
        return remote(here, here, xs.at[2, b], xr.at[2, b], peer)

    def f_copy(kind, b, mine):
        here = vis.at[b, m128(j ^ (kind + 1), rows), lane_half(mine)]
        return pltpu.make_async_remote_copy(
            src_ref=here, dst_ref=here, send_sem=fs.at[kind, b], recv_sem=fr.at[kind, b],
            device_id={"head": 1 - core}, device_id_type=pl.DeviceIdType.MESH)

    local = [
        pltpu.make_async_copy(q_in.at[:, m128(j, JW)], qraw.at[own_rows(me)], loc.at[0]),
        pltpu.make_async_copy(g_in.at[:, m128(j, JW)], graw.at[own_rows(me)], loc.at[1]),
        pltpu.make_async_copy(k_in.at[:, m128(j, D)], kb.at[m128(j, rows)], loc.at[2]),
        pltpu.make_async_copy(v_in.at[:, m128(j, D)], vb.at[m128(j, rows)], loc.at[3]),
        pltpu.make_async_copy(lens_in, lens, loc.at[4]),
        pltpu.make_async_copy(frames_in, frames, loc.at[5]),
    ]
    for c in local:
        c.start()
    for d in range(G - 1, 0, -1):
        for c in q_copy(d, me, near(d)[1], near(d)[0]):
            send(c)
    for d in range(1, G):
        for c in k_copy(d, near(d)[0], j, near(d)[1]):
            send(c)
    local_x = []
    for b in range(NZ):
        for h in range(2):
            local_x.append(pltpu.make_async_copy(
                x_in.at[:, m128(b * G + 2 * h + x, FB)], vis.at[b, m128(j, rows), pl.ds(h * FB, FB)], lx.at[b, h]))

    for c in local[4:]:
        c.wait()
    col = lax.broadcasted_iota(jnp.int32, (1, NR), 1)
    text = (col // ZB) * RZ + col % RZ
    seg = jnp.zeros((1, NR), jnp.int32)
    end = jnp.int32(0)
    NS = cfg["NS"]
    for i in range(NS):
        end = end + lens[i]
        seg += (text >= end).astype(jnp.int32)
    first, last = jnp.zeros((1, NR), jnp.int32), jnp.zeros((1, NR), jnp.int32)
    for i in range(NS):
        first = jnp.where(seg == i, frames[0, i], first)
        last = jnp.where(seg == i, frames[1, i], last)
    lim[0:1, :] = first
    lim[1:2, :] = last
    stat[0:8, :] = jnp.zeros((8, NR), F32)

    for c in local[:2]:
        c.wait()
    for d in range(1, G):
        for c in q_copy(d, z * G + near(d)[0], me, j):
            c.wait_recv()
    zq_each(lambda c: c.start(), z, False)
    for s in range(NZ):
        send(x_copy(0, band(s), 1 - x, j, near(1)[1]))
        if s < NZ // 2:
            send(x_copy(1, band(s), x, j, near(2)[1]))
    for c in local_x:
        c.start()
    for c in local[2:4]:
        c.wait()

    n_frames = rows // FR

    def tokens(g, f):
        return m128(g * n_frames + f, FR)

    def scored(g, zb):
        cols = m128(zb, ZB)
        lo, hi = lim[0:1, cols], lim[1:2, cols]
        base = z * G * n_frames + g * n_frames
        top = jnp.full((1, ZB), NEG_FILL, F32)
        for f in range(n_frames):
            ok = (lo <= base + f) & (base + f < hi)
            sc = jnp.where(ok, dot(kb[tokens(g, f), :], qb[cols, :], NT) * scale, NEG_FILL)
            ebuf[tokens(g, f), cols] = sc
            top = jnp.maximum(top, jnp.max(sc, axis=0, keepdims=True))
        gst[g, 0:1, cols] = top

    def summed(g, zb):
        cols = m128(zb, ZB)
        top = gst[g, 0:1, cols]
        total = jnp.zeros((1, ZB), F32)
        dotted = jnp.zeros((1, ZB), F32)
        for f in range(n_frames):
            dp = dot(vb[tokens(g, f), :], gb[cols, :], NT)
            e = jnp.exp(ebuf[tokens(g, f), cols] - top)
            ebuf[tokens(g, f), cols] = e
            dpb[tokens(g, f), cols] = dp
            total += jnp.sum(e, axis=0, keepdims=True)
            dotted += jnp.sum(e * dp, axis=0, keepdims=True)
        gst[g, 1:2, cols] = total
        gst[g, 2:3, cols] = dotted

    def s_copy(zb, z_to, z_from, peer):
        cols = m128(zb, ZB)
        return remote(stat.at[:, cols], stin.at[z_from, :, cols], ss.at[zb, z_to], sr.at[zb, z_from], peer)

    def plane_totals(zb):
        cols = m128(zb, ZB)
        top = gst[0, 0:1, cols]
        for g in range(1, G):
            top = jnp.maximum(top, gst[g, 0:1, cols])
        total = jnp.zeros((1, ZB), F32)
        dotted = jnp.zeros((1, ZB), F32)
        for g in range(G):
            w = jnp.exp(gst[g, 0:1, cols] - top)
            total += w * gst[g, 1:2, cols]
            dotted += w * gst[g, 2:3, cols]
        stat[0:1, cols] = top
        stat[1:2, cols] = total
        stat[2:3, cols] = dotted
        for d in range(1, NZ):
            s_copy(zb, far(d)[0], z, far(d)[2]).start()

    def landed(s):
        b = band(s)
        x_copy(0, b, x, near(1)[0], me).wait_recv()
        send(pass_copy(b, near(1)[0], near(2)[1]))
        if s < NZ // 2:
            send(x_copy(1, band(s + NZ // 2), x, j, near(2)[1]))
        send(f_copy(0, b, True))

    have_g, have_z = {0}, set()

    def arrive(k, which=(0, 1)):
        zq_each(lambda c: c.start(), band(NZ - 1 - k), True, which)

    def head_rows(zb, which=(0, 1)):
        for a in which:
            raw, buf = (qraw, graw)[a], (qb, gb)[a]
            for m in range(M):
                buf[m128(zb * M + m, RZ), :] = raw[m128(zb, RZ), m * D:(m + 1) * D]

    def block(d, k):
        zb = band(NZ - 1 - k)
        if d not in have_g:
            have_g.add(d)
            for c in k_copy(d, j, near(d)[0], me):
                c.wait_recv()
        if k not in have_z:
            have_z.add(k)
            if k:
                pl.when(jnp.logical_not(inner))(lambda: arrive(k))
            head_rows(zb)
        scored(j ^ d, zb)
        summed(j ^ d, zb)

    def last_block(k, waits):
        zb = band(NZ - 1 - k)
        for a, work in ((0, scored), (1, summed)):
            if waits:
                arrive(k, (a,))
            head_rows(zb, (a,))
            for d in range(G):
                work(j ^ d, zb)
        plane_totals(zb)

    block(0, 0)
    block(1, 0)

    @pl.when(inner)
    def _():
        arrive(1)
        arrive(2)
    for d, k in ((2, 0), (0, 1), (1, 1), (2, 1)):
        block(d, k)

    @pl.when(inner)
    def _():
        arrive(3)
    block(3, 0)
    plane_totals(band(NZ - 1))
    block(3, 1)
    plane_totals(band(NZ - 2))
    for d in range(G):
        block(d, 2)
    plane_totals(band(NZ - 3))
    landed(0)
    pl.when(inner)(lambda: last_block(3, False))
    pl.when(jnp.logical_not(inner))(lambda: last_block(3, True))

    CH = NK // NC

    def kv_copy(p, peer):
        return remote(kv.at[:, pl.ds(p * D, D)], kvn.at[p], kvs.at[p], kvr.at[p], peer)

    def d_copy(z_to, z_from):
        return remote(dqs.at[m128(z_to, RZ)], dqin.at[z_from], ds.at[z_to], dr.at[z_from], z_to * G + j)

    def coefs(zb):
        cols = m128(zb, ZB)
        for d in range(1, NZ):
            s_copy(zb, z, far(d)[1], me).wait_recv()
        top = stat[0:1, cols]
        for d in range(1, NZ):
            top = jnp.maximum(top, stin[far(d)[1], 0:1, cols])
        w = jnp.exp(stat[0:1, cols] - top)
        total, dotted = w * stat[1:2, cols], w * stat[2:3, cols]
        for d in range(1, NZ):
            i = far(d)[1]
            w = jnp.exp(stin[i, 0:1, cols] - top)
            total += w * stin[i, 1:2, cols]
            dotted += w * stin[i, 2:3, cols]
        for g in range(G):
            coef[g:g + 1, cols] = jnp.exp(gst[g, 0:1, cols] - top) / total
        coef[G:G + 1, cols] = dotted / total

    brim = jnp.where(2 * z < NZ, 0, NZ - 1)
    core_z = jnp.where(2 * z < NZ, 1, NZ - 2)

    def grads(n, zb):
        cols = m128(zb, ZB)
        coefs(zb)
        dqt[...] = jnp.zeros_like(dqt)

        @pl.loop(0, NC)
        def _(c):
            w, off = coef[pl.ds(c, 1), cols], coef[G:G + 1, cols]
            part_q = None
            for i in range(CH // FR):
                at, tok = pl.ds(i * FR, FR), m128(c * (CH // FR) + i, FR)
                p = ebuf[tok, cols] * w
                t = (p * (dpb[tok, cols] - off)).astype(BF16)
                dv = dot(p.astype(BF16), gb[cols, :])
                dk = dot(t, qb[cols, :])
                dq = dot(ktb[:, tok], t)
                part_q = dq if part_q is None else part_q + dq
                if n:
                    dk += tmp[c, at, 0:D]
                    dv += tmp[c, at, D:2 * D]
                if n < NZ - 1:
                    tmp[c, at, 0:D] = dk
                    tmp[c, at, D:2 * D] = dv
                else:
                    kv[tok, 0:D] = (scale * dk).astype(BF16)
                    kv[tok, D:2 * D] = dv.astype(BF16)
            dqt[...] += part_q

        if n == NZ - 1:
            for p in (1, 0):
                send(kv_copy(p, near(1)[1]))
        for i in range(ZB // D):
            t = (scale * dqt[:, pl.ds(i * D, D)].T).astype(BF16)
            for k in range(D // RZ):
                m = i * (D // RZ) + k
                dqs[m128(zb, RZ), pl.ds(m * D, D)] = t[k * RZ:(k + 1) * RZ, :]

        @pl.when(zb != z)
        def _():
            d_copy(zb, z).start()

    for f in range(NK // FR):
        ktb[:, pl.ds(f * FR, FR)] = kb[pl.ds(f * FR, FR), :].astype(F32).T.astype(BF16)
    grads(0, NZ - 1 - core_z)
    landed(NZ - 3)
    grads(1, core_z)
    grads(2, NZ - 1 - brim)
    landed(NZ - 2)
    grads(3, brim)
    HW = JW // 2

    def jcols(head, off, n):
        return pl.ds(pl.multiple_of(head * JW + off, n), n)

    def half(u):
        return pl.ds(u * HW, HW)

    def a_copy(kind, u, z_to, z_from):
        here = q_out.at[m128(z_from, RZ), jcols(j, u * HW, HW)]
        return remote(here, here, as_.at[kind, u, z_to], ar.at[u, z_from], z_to * G + j)

    def a_own(u, act):
        @pl.when(inner)
        def _():
            for d in range(1, NZ):
                act(a_copy(0, u, far(d)[0], z))

        @pl.when(jnp.logical_not(inner))
        def _():
            act(a_copy(0, u, jnp.where(low, NZ - 2, 1), z))

    def a_onward(u, act):
        act(a_copy(1, u, NZ - 1 - z, brim))
        act(a_copy(1, u, NZ - 1 - brim, brim))

    QW = JW // 4

    def y_copy(u, j_from, peer, kind):
        here = q_out.at[:, jcols(j_from, u * QW, QW)]
        return remote(here, here, ys.at[kind, u], yr.at[kind, u], peer)

    def y_pass(u, frm, to):
        y_copy(u, near(frm)[0], me, frm - 1).wait_recv()
        send(y_copy(u, near(frm)[0], near(to)[1], 2))

    for c in local_x:
        c.wait()

    def piece(h, p, i):
        cols = pl.ds(p * D, D) if h else pl.ds(0, 2 * D)
        return m128(i, FB), cols, (2 + 2 * p + i if h else i)

    def c_copy(side, b, h, p, i, peer):
        at, cols, n = piece(h, p, i)
        return remote(part.at[h, b, at, cols], rin.at[side, b, h, at, cols], cs.at[b, n], cr.at[side, b, n], peer)

    def weigh(s, h, p):
        for i in range(2):
            at, cols, _ = piece(h, p, i)
            tmp[h * NZ + s, at, cols] = dot(vis[band(s), :, i * FB:(i + 1) * FB], kvn[p] if h else kv[...], TN)

    def gather(s):
        b = band(s)
        x_copy(1, b, x, near(2)[0], me).wait_recv()
        send(f_copy(1, b, True))
        pass_copy(b, near(3)[0], me).wait_recv()
        send(f_copy(2, b, True))
        for kind in range(3):
            f_copy(kind, b, False).wait_recv()

    def hop(s):
        b = band(s)
        side = (b < z).astype(jnp.int32)
        return b, side, jnp.where(b > z, low, high), (z + 1 - 2 * side) * G + j

    def first(s, h, p=0):
        weigh(s, h, p)
        b, side, fed, peer = hop(s)

        @pl.when(jnp.logical_not(fed))
        def _():
            for i in (1 - y, y):
                at, cols, _ = piece(h, p, i)
                part[h, b, at, cols] = tmp[h * NZ + s, at, cols].astype(BF16)
                c_copy(side, b, h, p, i, peer).start()

    def later(s, h, p=0):
        b, side, fed, peer = hop(s)

        @pl.when(fed)
        def _():
            for i in (1 - y, y):
                at, cols, _ = piece(h, p, i)
                c_copy(side, b, h, p, i, me).wait_recv()
                part[h, b, at, cols] = (tmp[h * NZ + s, at, cols] + rin[side, b, h, at, cols].astype(F32)).astype(BF16)
                c_copy(side, b, h, p, i, peer).start()

    def e_copy(h, p, peer):
        cols = piece(h, p, 0)[1]
        return remote(ybs.at[h, :, cols], ybr.at[h, :, cols], es.at[h + h * p], er.at[h + h * p], peer)

    def settle(head, grads_of, grad):
        cols = m128(head, D)
        for n, a in enumerate(grads_of):
            (kw_out, vw_out)[a][:, cols] = grad[:, n * D:(n + 1) * D]

    def finish(h, p=0):
        own = h * NZ + NZ - 1
        for i in (1 - y, y):
            at, cols, _ = piece(h, p, i)
            for side, there in ((0, low), (1, high)):
                @pl.when(there)
                def _():
                    c_copy(side, z, h, p, i, me).wait_recv()
                    tmp[own, at, cols] += rin[side, z, h, at, cols].astype(F32)
            if i is y:
                settle(j ^ h, (p,) if h else (0, 1), tmp[own, at, cols])
            else:
                ybs[h, :, cols] = tmp[own, at, cols].astype(BF16)
                send(e_copy(h, p, near(2)[1]))

    def summed_dq():
        mine = dqs[m128(z, RZ), :].astype(F32)
        for d in range(1, NZ):
            d_copy(z, far(d)[1]).wait_recv()
            mine += dqin[far(d)[1]].astype(F32)
        q_out[m128(z, RZ), m128(j, JW)] = mine.astype(BF16)
        for u in range(2):
            a_own(u, lambda c: c.start())

    def relay_dq(u):
        @pl.when(inner)
        def _():
            a_copy(0, u, z, brim).wait_recv()
            a_onward(u, lambda c: c.start())

    def shared_dq():
        for u in range(2):
            for d in range(1, NZ):
                b = far(d)[1]

                @pl.when(jnp.logical_not(inner) | (b != brim))
                def _():
                    a_copy(0, u, z, b).wait_recv()
        for u in range(4):
            send(y_copy(u, j, near(1)[1], 0))
            send(y_copy((u + 1) % 4, j, near(2)[1], 1))

    gather(0)
    first(0, 0)
    landed(NZ - 1)
    summed_dq()
    gather(1)
    first(1, 0)
    later(0, 0)
    relay_dq(0)
    relay_dq(1)
    kv_copy(1, me).wait_recv()
    first(0, 1, 1)
    first(1, 1, 1)
    later(1, 0)
    gather(2)
    first(2, 0)
    early = len(sends)
    shared_dq()
    first(2, 1, 1)
    later(0, 1, 1)
    gather(3)
    kv_copy(0, me).wait_recv()
    for s in range(NZ - 1):
        first(s, 1, 0)
    later(1, 1, 1)
    later(2, 0)
    weigh(3, 0, 0)
    weigh(3, 1, 1)
    weigh(3, 1, 0)

    y_pass(0, 1, 2)
    y_pass(1, 2, 1)
    later(2, 1, 1)
    y_pass(2, 2, 1)
    later(0, 1, 0)
    y_pass(3, 2, 1)
    finish(0)
    later(1, 1, 0)
    later(2, 1, 0)
    for c in sends[:early]:
        c.wait_send()
    for k in range(NZ):
        zq_each(lambda c: c.wait_send(), band(NZ - 1 - k), False)
    for d in range(1, NZ):
        d_copy(far(d)[0], z).wait_send()
    for zb in range(NZ):
        for d in range(1, NZ):
            s_copy(zb, far(d)[0], z, far(d)[2]).wait_send()
    finish(1, 1)
    finish(1, 0)
    for u in range(1, 4):
        y_copy(u, near(1)[0], me, 0).wait_recv()
    y_copy(0, near(2)[0], me, 1).wait_recv()
    for u in range(4):
        y_copy(u, near(3)[0], me, 2).wait_recv()
    for h, p, grads_of in ((0, 0, (0, 1)), (1, 1, (1,)), (1, 0, (0,))):
        e_copy(h, p, me).wait_recv()
        settle(j ^ (2 + h), grads_of, ybr[h, :, piece(h, p, 0)[1]].astype(F32))
    for c in sends[early:]:
        c.wait_send()
    for u in range(2):
        a_own(u, lambda c: c.wait_send())
        pl.when(inner)(lambda: a_onward(u, lambda c: c.wait_send()))
    for s in range(NZ - 1):
        b, side, fed, peer = hop(s)
        for h, p in ((0, 0), (1, 0), (1, 1)):
            for i in range(2):
                c_copy(side, b, h, p, i, peer).wait_send()


def deliver_kernel(parts, *refs):
    n = len(parts)
    moves, k = [], 0
    for src, dst, p in zip(refs[:n], refs[n:2 * n], parts):
        step = src.shape[0] // p
        for i in range(p):
            at = pl.ds(i * step, step)
            moves.append(pltpu.make_async_copy(src.at[at], dst.at[at], refs[2 * n].at[k]))
            k += 1
    for a in moves:
        a.start()
    for a in moves:
        a.wait()


def deliver(*arrays):
    parts = [8, 2, 2]
    return pl.pallas_call(
        functools.partial(deliver_kernel, parts),
        out_shape=[jax.ShapeDtypeStruct(a.shape, a.dtype) for a in arrays],
        in_specs=[pl.BlockSpec(memory_space=pltpu.VMEM)] * len(arrays),
        out_specs=[pl.BlockSpec(memory_space=pl.ANY)] * len(arrays),
        scratch_shapes=[pltpu.SemaphoreType.DMA((sum(parts),))],
        compiler_params=pltpu.CompilerParams(vmem_limit_bytes=1 << 20),
    )(*arrays)


def plane_shards(T, text_queries, text_grads, vision_keys, video_value_rows, vision, lengths, frame_range):
    R, QW = text_queries.shape
    rows, kv_width = vision_keys.shape
    G = kv_width // HEAD_WIDTH
    M = QW // kv_width
    NZ = T // G
    DW = vision.shape[1]
    FB = DW // T
    NK, RZ, JW = G * rows, G * R, M * HEAD_WIDTH
    NR = T * R * M
    cfg = dict(G=G, NZ=NZ, M=M, R=R, FR=rows // FRAME_DEV, NC=4, rows=rows, NK=NK, NR=NR, JW=JW, FB=FB, RZ=RZ,
               NS=lengths.shape[0])
    anyspec = pl.BlockSpec(memory_space=pl.ANY)
    vm = pl.BlockSpec(memory_space=pltpu.VMEM)
    V = pltpu.VMEM
    D = pltpu.SemaphoreType.DMA
    W2 = 2 * HEAD_WIDTH
    pairs = []
    for a, b in (((2, G),) * 2, ((2, 2, NZ), (2, NZ)), ((2, G),) * 2, ((3, NZ),) * 2, ((3, NZ),) * 2, ((NZ, NZ),) * 2, ((2,),) * 2,
                 ((NZ,),) * 2, ((2, 2, NZ), (2, NZ)), ((3, 4),) * 2, ((NZ, 6), (2, NZ, 6)), ((3,),) * 2):
        pairs += [D(a), D(b)]
    q_grad, kw, vw = pl.pallas_call(
        functools.partial(plane_kernel, cfg),
        out_shape=(
            V((T * R, QW), BF16),
            V((FB, kv_width), F32),
            V((FB, kv_width), F32),
        ),
        in_specs=[anyspec] * 7,
        out_specs=(vm,) * 3,
        scratch_shapes=[
            V((T * R, JW), BF16), V((T * R, JW), BF16),
            V((NR, HEAD_WIDTH), BF16), V((NR, HEAD_WIDTH), BF16),
            V((NK, HEAD_WIDTH), BF16), V((NK, HEAD_WIDTH), BF16),
            V((NZ, NK, 2 * FB), BF16),
            V((NK, NR), F32), V((NK, NR), F32),
            V((8, NR), F32), V((NZ, 8, NR), F32), V((8, NR), F32), V((8, NR), jnp.int32),
            V((NK, W2), BF16), V((2, NK, HEAD_WIDTH), BF16),
            V((HEAD_WIDTH, M * RZ), F32), V((T * R, JW), BF16),
            V((NZ, RZ, JW), BF16),
            V((G, 8, NR), F32), V((HEAD_WIDTH, NK), BF16),
            pltpu.SMEM(lengths.shape, jnp.int32), pltpu.SMEM(frame_range.shape[::-1], jnp.int32),
            V((2 * NZ, 2 * FB, W2), F32), V((2, NZ, 2 * FB, W2), BF16), V((2, NZ, 2, 2 * FB, W2), BF16),
            V((2, FB, W2), BF16), V((2, FB, W2), BF16),
            D((6,)), D((NZ, 2)),
        ] + pairs,
        compiler_params=pltpu.CompilerParams(
            collective_id=0, has_side_effects=True, vmem_limit_bytes=67043328 - T * R * QW * 2 - 8 * FB * kv_width - (1 << 18)
        ),
    )(text_queries, text_grads, vision_keys, video_value_rows, vision, lengths, frame_range.T)
    return deliver(*[pltpu.with_memory_space_constraint(a, pltpu.VMEM) for a in (q_grad, kw, vw)])


def solution(mesh):
    return jax.shard_map(
        functools.partial(shards, mesh.shape["tok"], mesh.shape["head"]),
        mesh=mesh,
        in_specs=(
            P("tok", "head"),
            P("tok", "head"),
            P("tok", "head"),
            P("tok", "head"),
            P("tok", None),
            P(),
            P(),
        ),
        out_specs=(P(None, "head"), P("tok", "head"), P("tok", "head")),
        check_vma=False,
    )
```
